256 devices in a mesh: gx: 8 (over z_lo, core), gy: 4 (over y), gz: 8 (over z_hi, x).
Axes of the slice: x: 4, y: 4, z: 8 (z_hi: 2, z_lo: 4; z = z_hi * 4 + z_lo), core: 2. Of those that a mesh axis runs over, the one named last changes fastest.
Arguments:
- raw_weight: float32 [128, 27, 128], P(('gx', 'gy')), may hold values from -6 to 6
- inputs: bfloat16 [64, 64, 128, 128], P('gx', 'gy', 'gz'), may hold values from -6 to 6
- cotangent: bfloat16 [64, 64, 128, 128], P('gx', 'gy', 'gz'), may hold values from -0.099609375 to 0.099609375
Outputs:
- input_grad: bfloat16 [64, 64, 128, 128], P('gx', 'gy', 'gz')
- weight_grad: float32 [128, 27, 128], P(('gx', 'gy'))
The draws below stay inside these ranges and needn't reach their ends.
All inputs are finite; a program needn't handle non-finite values.
Results may differ from the reference program's by a relative error of at most 0.0049.
Values may be sent and summed in bfloat16 or wider, within the bound.
No kernel may reach another device: no remote copies, remote signals or barrier semaphores. Data moves between devices by JAX's collectives and lax.ppermute only.
A program may use at most 64 MiB of HBM per device.

```python
import math
import jax
import jax.numpy as jnp
from jax import lax

C = 128
KK = 27
NX = 64
NY = 64
NZ = 128


def draw_raw_weight(key, part):
    sub_keys = jax.random.split(key, 4)
    row_scale = jnp.exp(jax.random.uniform(sub_keys[0], (C, 1, 1), jnp.float32, math.log(0.1), 0.0))
    col_scale = jnp.exp(jax.random.uniform(sub_keys[1], (1, 1, C), jnp.float32, math.log(0.1), 0.0))
    col_mean = jax.random.uniform(sub_keys[2], (1, 1, C), jnp.float32, -0.5, 0.5)
    base_draw = jnp.clip(jax.random.normal(sub_keys[3], (C, KK, C), jnp.float32), -4.0, 4.0)
    return jnp.clip((base_draw * row_scale + col_mean) * col_scale, -6.0, 6.0)


def steps_of(rng, shape, cuts, smallest, top_value):
    def one(dim, parts):
        steps = jax.random.uniform(jax.random.fold_in(jax.random.fold_in(rng, 6), dim), (parts,), jnp.float32, smallest / len(cuts), top_value / len(cuts))
        return jnp.repeat(jnp.exp(steps), shape[dim] // parts).reshape((-1,) + (1,) * (len(shape) - dim - 1))

    level = one(*cuts[0])
    for cut in cuts[1:]:
        level = level * one(*cut)
    return level


def normal_values(rng, shape, scale, most, shards=(), dtype=jnp.bfloat16):
    array = jax.random.normal(rng, shape, jnp.float32) * scale
    if len(shards) > 0:
        array = steps_of(rng, shape, shards, -0.22, 0.18) * array
    return jnp.clip(array, min=-most, max=most).astype(dtype)


def setup_inputs(seed: int = 0) -> dict:
    key_of = jax.random.split(jax.random.key(seed), 4)
    raw_weight = draw_raw_weight(jax.random.fold_in(key_of[3], 71), 0)
    inputs = normal_values(key_of[1], (NX, NY, NZ, C), 1.0, 6.0, ((0, 8), (1, 4), (2, 8)))
    cotangent = normal_values(key_of[2], (NX, NY, NZ, C), 0.017, 0.099609375, ((0, 8), (1, 4), (2, 8)))
    return dict(raw_weight=raw_weight, inputs=inputs, cotangent=cotangent)


var_eps = 1e-05
norm_eps = 1e-06
clip_norm = 600.0

def tap_view(padded, tap_a, tap_b, tap_c, extent):
    view = padded[2 - tap_a:2 - tap_a + extent[0], 2 - tap_b:2 - tap_b + extent[1], 2 - tap_c:2 - tap_c + extent[2], :]
    return view.reshape(-1, view.shape[-1])

def reference(raw_weight, inputs, cotangent):
    extent = inputs.shape[:3]
    channels = inputs.shape[3]
    fan_count = raw_weight.shape[0] * raw_weight.shape[1]
    sum_first = lax.optimization_barrier(jnp.sum(raw_weight, axis=(0, 1)))
    sum_second = lax.optimization_barrier(jnp.sum(raw_weight * raw_weight, axis=(0, 1)))
    mean_out = sum_first / fan_count
    var_out = sum_second / fan_count - mean_out * mean_out
    inv_std = lax.rsqrt(var_out + var_eps)
    std_float = (raw_weight - mean_out) * inv_std
    std_half = lax.optimization_barrier(std_float.astype(jnp.bfloat16)).astype(jnp.float32)
    padded = jnp.pad(cotangent.astype(jnp.float32), ((1, 1), (1, 1), (1, 1), (0, 0)))
    flat_in = inputs.astype(jnp.float32).reshape(-1, channels)
    dx_total = jnp.zeros((flat_in.shape[0], channels), jnp.float32)
    pieces = []
    for tap_a in range(3):
        for tap_b in range(3):
            for tap_c in range(3):
                tap_index = tap_a * 9 + tap_b * 3 + tap_c
                view = tap_view(padded, tap_a, tap_b, tap_c, extent)
                dx_total = dx_total + jnp.dot(view, std_half[:, tap_index, :].T, precision=lax.Precision.HIGHEST)
                pieces.append(jnp.dot(flat_in.T, view, precision=lax.Precision.HIGHEST))
    input_grad = dx_total.reshape(extent[0], extent[1], extent[2], channels).astype(jnp.bfloat16)
    filter_grad = jnp.stack(pieces, axis=1)
    mean_grad = lax.optimization_barrier(jnp.sum(filter_grad, axis=(0, 1))) / fan_count
    mean_cross = lax.optimization_barrier(jnp.sum(filter_grad * std_float, axis=(0, 1))) / fan_count
    raw_grad = inv_std * (filter_grad - mean_grad - std_float * mean_cross)
    square_sum = jnp.sum(raw_grad * raw_grad)
    scale = jnp.minimum(1.0, clip_norm * lax.rsqrt(square_sum + norm_eps))
    return (input_grad, raw_grad * scale)
```

```python
import jax
import jax.numpy as jnp
from jax import lax
from jax.experimental import pallas as pl
from jax.experimental.pallas import tpu as pltpu
from jax.sharding import PartitionSpec as P


var_eps = 1e-05
norm_eps = 1e-06
clip_norm = 600.0
AXES = ("gx", "gy", "gz")
CORES = 2
VMEM = pltpu.CompilerParams(vmem_limit_bytes=48 * 1024 * 1024)


class Layout:
    def __init__(self, mesh):
        self.gx, self.gy, self.gz = (mesh.shape[a] for a in AXES)
        self.zl = self.gx // CORES
        self.x = self.zl
        self.zh = self.gz // self.x

    def spots(self):
        for zl in range(self.zl):
            for core in range(CORES):
                for y in range(self.gy):
                    for zh in range(self.zh):
                        for x in range(self.x):
                            yield dict(zl=zl, core=core, y=y, zh=zh, x=x)

    def index(self, s):
        return ((s["zl"] * CORES + s["core"]) * self.gy + s["y"]) * self.gz + s["zh"] * self.x + s["x"]

    def send(self, array, target):
        pairs = []
        for s in self.spots():
            t = dict(s)
            t.update(target(s))
            pairs.append((self.index(s), self.index(t)))
        return lax.ppermute(array, AXES, pairs)

    def exchange(self, array, fixed, order):
        groups = {}
        for s in self.spots():
            groups.setdefault(tuple(s[k] for k in fixed), []).append((order(s), self.index(s)))
        groups = [[i for _, i in sorted(g)] for g in groups.values()]
        return lax.all_to_all(array, AXES, 0, 0, tiled=True, axis_index_groups=groups)


def shift(array, axis, step):
    count = lax.axis_size(axis)
    if step > 0:
        pairs = [(i, i + 1) for i in range(count - 1)]
    else:
        pairs = [(i + 1, i) for i in range(count - 1)]
    return lax.ppermute(array, axis, pairs)


def fill_taps(ext_ref, zl_ref, zh_ref, taps_ref):
    ch = ext_ref.shape[-1]

    def row(k, carry):
        mid = ext_ref[k].astype(jnp.float32)
        low = zl_ref[k].astype(jnp.float32)[:, None, :]
        high = zh_ref[k].astype(jnp.float32)[:, None, :]
        up = jnp.concatenate([mid[:, 1:], high], axis=1)
        down = jnp.concatenate([low, mid[:, :-1]], axis=1)
        taps_ref[k, :, :, 0:ch] = up.astype(jnp.bfloat16)
        taps_ref[k, :, :, ch : 2 * ch] = ext_ref[k]
        taps_ref[k, :, :, 2 * ch : 3 * ch] = down.astype(jnp.bfloat16)
        return carry

    lax.fori_loop(0, ext_ref.shape[0], row, 0)


def filter_kernel(core_ref, ext_ref, zl_ref, zh_ref, in_ref, taps_ref, keep_ref, send_ref):
    fill_taps(ext_ref, zl_ref, zh_ref, taps_ref)
    nx, ny, nz, ch = ext_ref.shape[0] - 2, ext_ref.shape[1] - 2, ext_ref.shape[2], ext_ref.shape[3]
    cells = nx * ny * nz
    flat = in_ref[...].T
    core = core_ref[0]
    for a in range(3):
        for b in range(3):
            view = taps_ref[2 - a : 2 - a + nx, 2 - b : 2 - b + ny].reshape(cells, 3 * ch)
            res = jnp.dot(flat, view, preferred_element_type=jnp.float32)
            lanes = pl.ds((a * 3 + b) * 3 * ch, 3 * ch)
            groups = ch // 32
            for g in range(groups):
                first = res[g * 32 : g * 32 + 16]
                second = res[g * 32 + 16 : g * 32 + 32]
                own = jnp.where(core == 0, first, second)
                other = jnp.where(core == 0, second, first)
                keep_ref[g * 16 : g * 16 + 16, lanes] = own
                send_ref[g * 16 : g * 16 + 16, lanes] = other.astype(jnp.bfloat16)


def filter_terms(core, ext, z_low, z_high, flat_in):
    nx, ny, nz, ch = ext.shape[0] - 2, ext.shape[1] - 2, ext.shape[2], ext.shape[3]
    width = 27 * ch
    flops = 2 * nx * ny * nz * ch * width
    return pl.pallas_call(
        filter_kernel,
        out_shape=(
            jax.ShapeDtypeStruct((nx + 2, ny + 2, nz, 3 * ch), jnp.bfloat16),
            jax.ShapeDtypeStruct((ch // 2, width), jnp.float32),
            jax.ShapeDtypeStruct((ch // 2, width), jnp.bfloat16),
        ),
        in_specs=[pl.BlockSpec(memory_space=pltpu.SMEM)] + [pl.BlockSpec(memory_space=pltpu.VMEM)] * 4,
        out_specs=tuple(pl.BlockSpec(memory_space=pltpu.VMEM) for _ in range(3)),
        compiler_params=VMEM,
        cost_estimate=pl.CostEstimate(flops=2 * flops, bytes_accessed=8_000_000, transcendentals=0),
        name="filter_terms",
    )(core, ext, z_low, z_high, flat_in)


def input_kernel(taps_ref, std_ref, out_ref):
    nx, ny, nz, ch = out_ref.shape
    planes = 2
    std = std_ref[...]
    for x in range(0, nx, planes):
        rows = jnp.concatenate(
            [
                taps_ref[x + 2 - a : x + 2 - a + planes, 2 - b : 2 - b + ny].reshape(planes * ny * nz, 3 * ch)
                for a in range(3)
                for b in range(3)
            ],
            axis=1,
        )
        res = lax.dot_general(rows, std, (((1,), (1,)), ((), ())), preferred_element_type=jnp.float32)
        out_ref[x : x + planes] = res.astype(jnp.bfloat16).reshape(planes, ny, nz, ch)


def input_rows(taps, std, shape):
    flops = 2 * shape[0] * shape[1] * shape[2] * shape[3] * std.shape[1]
    return pl.pallas_call(
        input_kernel,
        out_shape=jax.ShapeDtypeStruct(shape, jnp.bfloat16),
        in_specs=[pl.BlockSpec(memory_space=pltpu.VMEM)] * 2,
        out_specs=pl.BlockSpec(memory_space=pltpu.VMEM),
        compiler_params=VMEM,
        cost_estimate=pl.CostEstimate(flops=2 * flops, bytes_accessed=4_000_000, transcendentals=0),
        name="input_rows",
    )(taps, std)


def std_kernel(spot_ref, near_ref, far_ref, std_ref, mean_ref, inv_ref, block_ref):
    slots, rows, wide = near_ref.shape
    ch = inv_ref.shape[1]
    taps = wide // ch - 1
    y, zl, core, x = spot_ref[0], spot_ref[1], spot_ref[2], spot_ref[3]
    blocks = []
    for b in range(2 * slots):
        blocks.append((b // 8, (b // 4) % 2, b % 4))
    count = float(2 * slots * rows * taps)

    def parts(zl_b, core_b, y_b):
        slot = (y_b ^ y) + 4 * (zl_b ^ zl)
        data = jnp.where(core_b == core, near_ref[slot], far_ref[slot]).astype(jnp.float32)
        return data[:, : taps * ch], data[0:1, taps * ch :] + data[1:2, taps * ch :]

    def folded(values):
        total = values[:, 0:ch]
        for t in range(1, taps):
            total = total + values[:, t * ch : (t + 1) * ch]
        return jnp.sum(total, axis=0, keepdims=True)

    total = jnp.zeros((1, ch), jnp.float32)
    for b in blocks:
        values, base = parts(*b)
        total = total + (folded(values) + float(rows * taps) * base)
    mean = total / count
    square = jnp.zeros((1, ch), jnp.float32)
    for b in blocks:
        values, base = parts(*b)
        off = base - mean
        first = values + jnp.concatenate([off] * taps, axis=1)
        square = square + folded(first * first)
    inv = lax.rsqrt(square / count + var_eps)
    mean_ref[...] = mean
    inv_ref[...] = inv
    inv_wide = jnp.concatenate([inv] * taps, axis=1)
    for n, b in enumerate(blocks):
        values, base = parts(*b)
        off = jnp.concatenate([base - mean] * taps, axis=1)
        std_ref[n * rows : (n + 1) * rows, :] = ((values + off) * inv_wide).astype(jnp.bfloat16)
    values, base = parts(x, core, y)
    off = jnp.concatenate([base - mean] * taps, axis=1)
    block_ref[...] = (values + off) * inv_wide


def standardized(spot, near, far, ch):
    slots, rows, wide = near.shape
    width = wide - ch
    return pl.pallas_call(
        std_kernel,
        out_shape=(
            jax.ShapeDtypeStruct((2 * slots * rows, width), jnp.bfloat16),
            jax.ShapeDtypeStruct((1, ch), jnp.float32),
            jax.ShapeDtypeStruct((1, ch), jnp.float32),
            jax.ShapeDtypeStruct((rows, width), jnp.float32),
        ),
        in_specs=[pl.BlockSpec(memory_space=pltpu.SMEM)] + [pl.BlockSpec(memory_space=pltpu.VMEM)] * 2,
        out_specs=tuple(pl.BlockSpec(memory_space=pltpu.VMEM) for _ in range(4)),
        compiler_params=VMEM,
        cost_estimate=pl.CostEstimate(flops=2_000_000_000, bytes_accessed=3_000_000, transcendentals=0),
        name="standardized",
    )(spot, near, far)


def on_device(where, raw_weight, inputs, cotangent):
    nx, ny, nz, ch = inputs.shape
    rows, taps = raw_weight.shape[:2]
    fan_count = ch * taps
    gx, gy, gz = (lax.axis_index(a) for a in AXES)
    core, zl, x = gx % CORES, gx // CORES, gz % where.x
    spot = jnp.stack([gy, zl, core, x]).astype(jnp.int32)

    base = jnp.mean(raw_weight, axis=(0, 1))
    base_high = base.astype(jnp.bfloat16)
    base_low = (base - base_high.astype(jnp.float32)).astype(jnp.bfloat16)
    sent_base = base_high.astype(jnp.float32) + base_low.astype(jnp.float32)
    tail = jnp.concatenate([base_high[None], base_low[None], jnp.zeros((rows - 2, ch), jnp.bfloat16)], 0)
    held = (raw_weight - sent_base).astype(jnp.bfloat16).reshape(rows, taps * ch)
    held = jnp.concatenate([held, tail], axis=1)[None]

    x_low = shift(cotangent[-1:], "gx", 1)
    x_high = shift(cotangent[:1], "gx", -1)
    held = jnp.concatenate([held, where.send(held, lambda s: dict(y=s["y"] ^ 1))], 0)
    deep = jnp.concatenate([x_low, cotangent, x_high], axis=0)
    y_low = shift(deep[:, -1:], "gy", 1)
    y_high = shift(deep[:, :1], "gy", -1)
    held = jnp.concatenate([held, where.send(held, lambda s: dict(y=s["y"] ^ 2))], 0)
    ext = jnp.concatenate([y_low, deep, y_high], axis=1)
    z_low = shift(ext[:, :, -1, :], "gz", 1)
    z_high = shift(ext[:, :, 0, :], "gz", -1)
    held = jnp.concatenate([held, where.send(held, lambda s: dict(zl=s["zl"] ^ 1))], 0)

    tap_views, keep, send = filter_terms(core[None].astype(jnp.int32), ext, z_low, z_high, inputs.reshape(-1, ch))
    held = jnp.concatenate([held, where.send(held, lambda s: dict(zl=s["zl"] ^ 2))], 0)
    other = where.send(send, lambda s: dict(core=1 - s["core"]))
    far = where.send(held, lambda s: dict(core=1 - s["core"]))
    half = (keep + other.astype(jnp.float32)).astype(jnp.bfloat16)
    peers = where.x * where.gy
    parts = where.exchange(
        half.reshape(peers, rows, taps * ch), ("core", "zl", "zh"), lambda s: (s["x"], s["y"])
    )
    part = jnp.sum(parts.astype(jnp.float32), axis=0).astype(jnp.bfloat16)
    deep_count = where.zl * where.zh
    parts = where.exchange(
        jnp.broadcast_to(part[None], (deep_count, *part.shape)), ("core", "x", "y"), lambda s: (s["zh"], s["zl"])
    )
    block_grad = jnp.sum(parts.astype(jnp.float32), axis=0)

    std_half, mean_out, inv_std, block_std = standardized(spot, held, far, ch)
    input_grad = input_rows(tap_views, std_half, inputs.shape)

    filter_grad = where.send(block_grad, lambda s: dict(x=s["zl"], zl=s["x"])).reshape(rows, taps, ch)
    by_tap = block_grad.reshape(rows, taps, ch)
    local = jnp.stack(
        [
            jnp.sum(by_tap, axis=(0, 1)),
            jnp.sum(by_tap * block_std.reshape(rows, taps, ch), axis=(0, 1)),
            jnp.sum(by_tap * by_tap, axis=(0, 1)),
        ]
    )
    everyone = CORES * where.x * where.gy
    sums = where.exchange(
        jnp.broadcast_to(local.reshape(1, 1, 3 * ch), (everyone, 1, 3 * ch)),
        ("zl", "zh"),
        lambda s: (s["core"], s["x"], s["y"]),
    )
    sum_grad, sum_cross, sum_square = jnp.sum(sums, axis=0).reshape(3, ch)
    mean_out, inv_std = mean_out[0], inv_std[0]
    std_float = (raw_weight - mean_out) * inv_std
    mean_grad = sum_grad / fan_count
    mean_cross = sum_cross / fan_count
    raw_grad = inv_std * (filter_grad - mean_grad - std_float * mean_cross)
    per_output = sum_square - 2.0 * mean_grad * sum_grad - 2.0 * mean_cross * sum_cross
    shrink = 1.0 - var_eps * inv_std * inv_std
    per_output = (
        per_output + fan_count * mean_grad * mean_grad + fan_count * mean_cross * mean_cross * shrink
    )
    square_sum = jnp.sum(inv_std * inv_std * per_output)
    scale = jnp.minimum(1.0, clip_norm * lax.rsqrt(square_sum + norm_eps))
    return (input_grad, raw_grad * scale)


def solution(mesh):
    where = Layout(mesh)
    in_specs = (P(("gx", "gy"), None, None), P("gx", "gy", "gz", None), P("gx", "gy", "gz", None))
    out_specs = (P("gx", "gy", "gz", None), P(("gx", "gy"), None, None))

    def body(raw_weight, inputs, cotangent):
        return on_device(where, raw_weight, inputs, cotangent)

    return jax.shard_map(body, mesh=mesh, in_specs=in_specs, out_specs=out_specs, check_vma=False)
```

```python
import jax
import jax.numpy as jnp
from jax import lax
from jax.experimental import pallas as pl
from jax.experimental.pallas import tpu as pltpu
from jax.sharding import PartitionSpec as P


var_eps = 1e-05
norm_eps = 1e-06
clip_norm = 600.0
AXES = ("gx", "gy", "gz")
CORES = 2
TAPS = 27
MIB = 1024 * 1024


def call(kernel, out_shape, args, scalars=0, vmem=8, flops=1_000_000_000):
    spaces = [pltpu.SMEM] * scalars + [pltpu.VMEM] * (len(args) - scalars)
    many = isinstance(out_shape, tuple)
    return pl.pallas_call(
        kernel,
        out_shape=out_shape,
        in_specs=[pl.BlockSpec(memory_space=s) for s in spaces],
        out_specs=tuple(pl.BlockSpec(memory_space=pltpu.VMEM) for _ in out_shape)
        if many
        else pl.BlockSpec(memory_space=pltpu.VMEM),
        compiler_params=pltpu.CompilerParams(vmem_limit_bytes=vmem * MIB),
        cost_estimate=pl.CostEstimate(flops=flops, bytes_accessed=1_000_000, transcendentals=0),
    )(*args)


def of(shape, dtype):
    return jax.ShapeDtypeStruct(shape, dtype)


class Layout:
    def __init__(self, mesh):
        self.gx, self.gy, self.gz = (mesh.shape[a] for a in AXES)
        self.zl = self.gx // CORES
        self.x = self.zl
        self.zh = self.gz // self.x

    def spots(self):
        for zl in range(self.zl):
            for core in range(CORES):
                for y in range(self.gy):
                    for zh in range(self.zh):
                        for x in range(self.x):
                            yield dict(zl=zl, core=core, y=y, zh=zh, x=x)

    def index(self, s):
        return ((s["zl"] * CORES + s["core"]) * self.gy + s["y"]) * self.gz + s["zh"] * self.x + s["x"]

    def send(self, array, target):
        pairs = []
        for s in self.spots():
            t = dict(s)
            t.update(target(s))
            pairs.append((self.index(s), self.index(t)))
        return lax.ppermute(array, AXES, pairs)

    def exchange(self, array, fixed, order):
        groups = {}
        for s in self.spots():
            groups.setdefault(tuple(s[k] for k in fixed), []).append((order(s), self.index(s)))
        groups = [[i for _, i in sorted(g)] for g in groups.values()]
        return lax.all_to_all(array, AXES, 0, 0, tiled=True, axis_index_groups=groups)


def shift(array, axis, step):
    count = lax.axis_size(axis)
    if step > 0:
        pairs = [(i, i + 1) for i in range(count - 1)]
    else:
        pairs = [(i + 1, i) for i in range(count - 1)]
    return lax.ppermute(array, axis, pairs)


def wide(row, taps=TAPS):
    return jnp.concatenate([row] * taps, axis=1)


def fold(values, ch):
    total = values[:, 0:ch]
    for t in range(1, values.shape[1] // ch):
        total = total + values[:, t * ch : (t + 1) * ch]
    return jnp.sum(total, axis=0, keepdims=True)


def base_kernel(raw_ref, held_ref):
    taps, rows, ch = raw_ref.shape
    base = jnp.sum(jnp.sum(raw_ref[...], axis=0), axis=0, keepdims=True) / (taps * rows)
    high = base.astype(jnp.bfloat16)
    low = (base - high.astype(jnp.float32)).astype(jnp.bfloat16)
    base = high.astype(jnp.float32) + low.astype(jnp.float32)
    for t in range(taps):
        held_ref[0, :, t * ch : (t + 1) * ch] = (raw_ref[t] - base).astype(jnp.bfloat16)
    place = lax.broadcasted_iota(jnp.int32, (rows, ch), 0)
    both = jnp.where(place == 0, high.astype(jnp.float32), low.astype(jnp.float32))
    held_ref[0, :, taps * ch :] = both.astype(jnp.bfloat16)


def filter_kernel(core_ref, mid_ref, xl_ref, xh_ref, yl_ref, yh_ref, zl_ref, zh_ref, in_ref, taps_ref, keep_ref, send_ref):
    nx, ny, nz, ch = mid_ref.shape

    def fill(k, rows, j, n):
        mid = rows.astype(jnp.float32)
        low = zl_ref[k, j : j + n].astype(jnp.float32)[:, None, :]
        high = zh_ref[k, j : j + n].astype(jnp.float32)[:, None, :]
        up = jnp.concatenate([mid[:, 1:], high], axis=1)
        down = jnp.concatenate([low, mid[:, :-1]], axis=1)
        taps_ref[k, j : j + n, :, 0:ch] = up.astype(jnp.bfloat16)
        taps_ref[k, j : j + n, :, ch : 2 * ch] = rows
        taps_ref[k, j : j + n, :, 2 * ch : 3 * ch] = down.astype(jnp.bfloat16)

    def plane(k, carry):
        fill(k, yl_ref[k][None], 0, 1)
        fill(k, yh_ref[k][None], ny + 1, 1)
        return carry

    def middle(k, carry):
        fill(k + 1, mid_ref[k], 1, ny)
        return carry

    lax.fori_loop(0, nx, middle, 0)
    fill(0, xl_ref[0], 1, ny)
    fill(nx + 1, xh_ref[0], 1, ny)
    lax.fori_loop(0, nx + 2, plane, 0)
    cells = nx * ny * nz
    flat = in_ref[...].T
    core = core_ref[0]
    for a in range(3):
        for b in range(3):
            view = taps_ref[2 - a : 2 - a + nx, 2 - b : 2 - b + ny].reshape(cells, 3 * ch)
            res = jnp.dot(flat, view, preferred_element_type=jnp.float32)
            lanes = pl.ds((a * 3 + b) * 3 * ch, 3 * ch)
            for g in range(ch // 32):
                first = res[g * 32 : g * 32 + 16]
                second = res[g * 32 + 16 : g * 32 + 32]
                keep_ref[g * 16 : g * 16 + 16, lanes] = jnp.where(core == 0, first, second)
                send_ref[g * 16 : g * 16 + 16, lanes] = jnp.where(core == 0, second, first).astype(jnp.bfloat16)


def pair_kernel(keep_ref, other_ref, out_ref):
    rows = out_ref.shape[1]
    for g in range(keep_ref.shape[0] // 16):
        total = keep_ref[g * 16 : g * 16 + 16] + other_ref[g * 16 : g * 16 + 16].astype(jnp.float32)
        for r in range(16 // rows):
            out_ref[g * (16 // rows) + r] = total[r * rows : (r + 1) * rows].astype(jnp.bfloat16)


def peers_kernel(parts_ref, out_ref):
    total = jnp.sum(parts_ref[...].astype(jnp.float32), axis=0).astype(jnp.bfloat16)
    for k in range(out_ref.shape[0]):
        out_ref[k] = total


def block_kernel(parts_ref, std_ref, grad_ref, sums_ref):
    ch = sums_ref.shape[2] // 3
    total = jnp.sum(parts_ref[...].astype(jnp.float32), axis=0)
    grad_ref[...] = total
    three = jnp.concatenate([fold(total, ch), fold(total * std_ref[...], ch), fold(total * total, ch)], axis=1)
    for k in range(sums_ref.shape[0]):
        sums_ref[k] = three


def input_kernel(taps_ref, std_ref, out_ref):
    nx, ny, nz, ch = out_ref.shape
    planes = 2
    std = std_ref[...]
    for x in range(0, nx, planes):
        rows = jnp.concatenate(
            [
                taps_ref[x + 2 - a : x + 2 - a + planes, 2 - b : 2 - b + ny].reshape(planes * ny * nz, 3 * ch)
                for a in range(3)
                for b in range(3)
            ],
            axis=1,
        )
        res = lax.dot_general(rows, std, (((1,), (1,)), ((), ())), preferred_element_type=jnp.float32)
        out_ref[x : x + planes] = res.astype(jnp.bfloat16).reshape(planes, ny, nz, ch)


def std_kernel(spot_ref, near_ref, far_ref, std_ref, mean_ref, inv_ref, block_ref):
    slots, rows, held = near_ref.shape
    ch = inv_ref.shape[1]
    width = held - ch
    taps = width // ch
    y, zl, core, x = spot_ref[0], spot_ref[1], spot_ref[2], spot_ref[3]
    blocks = [(b // 8, (b // 4) % 2, b % 4) for b in range(2 * slots)]
    count = float(2 * slots * rows * taps)

    def parts(zl_b, core_b, y_b):
        slot = (y_b ^ y) + 4 * (zl_b ^ zl)
        data = jnp.where(core_b == core, near_ref[slot], far_ref[slot]).astype(jnp.float32)
        return data[:, :width], data[0:1, width:] + data[1:2, width:]

    total = jnp.zeros((1, ch), jnp.float32)
    for b in blocks:
        values, base = parts(*b)
        total = total + (fold(values, ch) + float(rows * taps) * base)
    mean = total / count
    square = jnp.zeros((1, ch), jnp.float32)
    for b in blocks:
        values, base = parts(*b)
        first = values + wide(base - mean)
        square = square + fold(first * first, ch)
    inv = lax.rsqrt(square / count + var_eps)
    mean_ref[...] = mean
    inv_ref[...] = inv
    inv_wide = wide(inv)
    for n, b in enumerate(blocks):
        values, base = parts(*b)
        std_ref[n * rows : (n + 1) * rows, :] = ((values + wide(base - mean)) * inv_wide).astype(jnp.bfloat16)
    values, base = parts(x, core, y)
    block_ref[...] = (values + wide(base - mean)) * inv_wide


def last_kernel(fan_count, grad_ref, raw_ref, mean_ref, inv_ref, sums_ref, out_ref):
    taps, _, ch = raw_ref.shape
    sums = jnp.sum(sums_ref[...], axis=0)
    sum_grad, sum_cross, sum_square = sums[:, :ch], sums[:, ch : 2 * ch], sums[:, 2 * ch :]
    mean, inv = mean_ref[...], inv_ref[...]
    mean_grad = sum_grad / fan_count
    mean_cross = sum_cross / fan_count
    shrink = 1.0 - var_eps * inv * inv
    per_output = sum_square - 2.0 * mean_grad * sum_grad - 2.0 * mean_cross * sum_cross
    per_output = per_output + fan_count * mean_grad * mean_grad + fan_count * mean_cross * mean_cross * shrink
    square_sum = jnp.sum(inv * inv * per_output, axis=1, keepdims=True)
    scale = jnp.minimum(1.0, clip_norm * lax.rsqrt(square_sum + norm_eps))
    factor = inv * scale
    for t in range(taps):
        std = (raw_ref[t] - mean) * inv
        out_ref[t] = factor * (grad_ref[:, t * ch : (t + 1) * ch] - mean_grad - std * mean_cross)


def on_device(where, raw_weight, inputs, cotangent):
    nx, ny, nz, ch = inputs.shape
    rows, taps = raw_weight.shape[:2]
    width = taps * ch
    bf16, f32 = jnp.bfloat16, jnp.float32
    gx, gy, gz = (lax.axis_index(a).astype(jnp.int32) for a in AXES)
    core, zl, x = gx & 1, gx >> 1, gz & (where.x - 1)
    spot = jnp.stack([gy, zl, core, x])
    raw = jnp.transpose(raw_weight, (1, 0, 2))

    x_low = shift(cotangent[-1:], "gx", 1)
    x_high = shift(cotangent[:1], "gx", -1)
    held = call(base_kernel, of((1, rows, width + ch), bf16), (raw,))
    held = jnp.concatenate([held, where.send(held, lambda s: dict(y=s["y"] ^ 1))], 0)
    y_low = shift(jnp.concatenate([a[:, -1] for a in (x_low, cotangent, x_high)], 0), "gy", 1)
    y_high = shift(jnp.concatenate([a[:, 0] for a in (x_low, cotangent, x_high)], 0), "gy", -1)
    held = jnp.concatenate([held, where.send(held, lambda s: dict(y=s["y"] ^ 2))], 0)

    def face(k):
        deep = jnp.concatenate([a[:, :, k] for a in (x_low, cotangent, x_high)], 0)
        return jnp.concatenate([y_low[:, None, k], deep, y_high[:, None, k]], 1)

    z_low = shift(face(nz - 1), "gz", 1)
    z_high = shift(face(0), "gz", -1)
    held = jnp.concatenate([held, where.send(held, lambda s: dict(zl=s["zl"] ^ 1))], 0)

    flops = 2 * nx * ny * nz * ch * width
    tap_views, keep, send = call(
        filter_kernel,
        (of((nx + 2, ny + 2, nz, 3 * ch), bf16), of((ch // 2, width), f32), of((ch // 2, width), bf16)),
        (core[None], cotangent, x_low, x_high, y_low, y_high, z_low, z_high, inputs.reshape(-1, ch)),
        scalars=1,
        vmem=16,
        flops=2 * flops,
    )
    other = where.send(send, lambda s: dict(core=1 - s["core"]))
    held = jnp.concatenate([held, where.send(held, lambda s: dict(zl=s["zl"] ^ 2))], 0)
    peers = where.x * where.gy
    half = call(pair_kernel, of((peers, rows, width), bf16), (keep, other))
    parts = where.exchange(half, ("core", "zl", "zh"), lambda s: (s["x"], s["y"]))
    far = where.send(held, lambda s: dict(core=1 - s["core"]))
    copies = call(peers_kernel, of((where.zl * where.zh, rows, width), bf16), (parts,))
    parts = where.exchange(copies, ("core", "x", "y"), lambda s: (s["zh"], s["zl"]))

    std_half, mean_out, inv_std, block_std = call(
        std_kernel,
        (of((ch, width), bf16), of((1, ch), f32), of((1, ch), f32), of((rows, width), f32)),
        (spot, held, far),
        scalars=1,
        flops=3_000_000_000,
    )
    everyone = CORES * where.x * where.gy
    block_grad, local = call(block_kernel, (of((rows, width), f32), of((everyone, 1, 3 * ch), f32)), (parts, block_std))
    filter_grad = where.send(block_grad, lambda s: dict(x=s["zl"], zl=s["x"]))
    sums = where.exchange(local, ("zl", "zh"), lambda s: (s["core"], s["x"], s["y"]))
    input_grad = call(input_kernel, of(inputs.shape, bf16), (tap_views, std_half), vmem=16, flops=2 * flops)

    def last(*refs):
        last_kernel(float(ch * taps), *refs)

    grad = call(last, of((taps, rows, ch), f32), (filter_grad, raw, mean_out, inv_std, sums))
    return (input_grad, jnp.transpose(grad, (1, 0, 2)))


def solution(mesh):
    where = Layout(mesh)
    in_specs = (P(("gx", "gy"), None, None), P("gx", "gy", "gz", None), P("gx", "gy", "gz", None))
    out_specs = (P("gx", "gy", "gz", None), P(("gx", "gy"), None, None))

    def body(raw_weight, inputs, cotangent):
        return on_device(where, raw_weight, inputs, cotangent)

    return jax.shard_map(body, mesh=mesh, in_specs=in_specs, out_specs=out_specs, check_vma=False)
```

```python
import functools

import jax
import jax.numpy as jnp
from jax import lax
from jax.experimental import pallas as pl
from jax.experimental.pallas import tpu as pltpu
from jax.sharding import PartitionSpec as P


var_eps = 1e-05
norm_eps = 1e-06
clip_norm = 600.0
AXES = ("gx", "gy", "gz")
CORES = 2
TAPS = 27
MIB = 1024 * 1024


def call(kernel, out_shape, args, vmem=8, flops=1_000_000_000):
    many = isinstance(out_shape, tuple)
    return pl.pallas_call(
        kernel,
        out_shape=out_shape,
        in_specs=[pl.BlockSpec(memory_space=pltpu.VMEM) for _ in args],
        out_specs=tuple(pl.BlockSpec(memory_space=pltpu.VMEM) for _ in out_shape)
        if many
        else pl.BlockSpec(memory_space=pltpu.VMEM),
        compiler_params=pltpu.CompilerParams(vmem_limit_bytes=vmem * MIB),
        cost_estimate=pl.CostEstimate(flops=flops, bytes_accessed=1_000_000, transcendentals=0),
    )(*args)


def of(shape, dtype):
    return jax.ShapeDtypeStruct(shape, dtype)


class Layout:
    def __init__(self, mesh):
        self.gx, self.gy, self.gz = (mesh.shape[a] for a in AXES)
        self.zl = self.gx // CORES
        self.x = self.zl
        self.zh = self.gz // self.x

    def spots(self):
        for zl in range(self.zl):
            for core in range(CORES):
                for y in range(self.gy):
                    for zh in range(self.zh):
                        for x in range(self.x):
                            yield dict(zl=zl, core=core, y=y, zh=zh, x=x)

    def index(self, s):
        return ((s["zl"] * CORES + s["core"]) * self.gy + s["y"]) * self.gz + s["zh"] * self.x + s["x"]

    def send(self, array, target):
        pairs = []
        for s in self.spots():
            t = dict(s)
            t.update(target(s))
            pairs.append((self.index(s), self.index(t)))
        return lax.ppermute(array, AXES, pairs)

    def exchange(self, array, fixed, order):
        groups = {}
        for s in self.spots():
            groups.setdefault(tuple(s[k] for k in fixed), []).append((order(s), self.index(s)))
        groups = [[i for _, i in sorted(g)] for g in groups.values()]
        return lax.all_to_all(array, AXES, 0, 0, tiled=True, axis_index_groups=groups)


def shift(array, axis, step):
    count = lax.axis_size(axis)
    if step > 0:
        pairs = [(i, i + 1) for i in range(count - 1)]
    else:
        pairs = [(i + 1, i) for i in range(count - 1)]
    return lax.ppermute(array, axis, pairs)


def wide(row, taps=TAPS):
    return jnp.concatenate([row] * taps, axis=1)


def fold(values, ch):
    total = values[:, 0:ch]
    for t in range(1, values.shape[1] // ch):
        total = total + values[:, t * ch : (t + 1) * ch]
    return jnp.sum(total, axis=0, keepdims=True)


def base_kernel(raw_ref, held_ref):
    taps, rows, ch = raw_ref.shape
    base = jnp.sum(jnp.sum(raw_ref[...], axis=0), axis=0, keepdims=True) / (taps * rows)
    high = base.astype(jnp.bfloat16)
    low = (base - high.astype(jnp.float32)).astype(jnp.bfloat16)
    base = high.astype(jnp.float32) + low.astype(jnp.float32)
    for t in range(taps):
        held_ref[0, :, t * ch : (t + 1) * ch] = (raw_ref[t] - base).astype(jnp.bfloat16)
    place = lax.broadcasted_iota(jnp.int32, (rows, ch), 0)
    both = jnp.where(place == 0, high.astype(jnp.float32), low.astype(jnp.float32))
    held_ref[0, :, taps * ch :] = both.astype(jnp.bfloat16)


def filter_kernel(mid_ref, xl_ref, xh_ref, yl_ref, yh_ref, zl_ref, zh_ref, in_ref, taps_ref, keep_ref, send_ref):
    nx, ny, nz, ch = mid_ref.shape

    def fill(k, rows, j, n):
        mid = rows.astype(jnp.float32)
        low = zl_ref[k, j : j + n].astype(jnp.float32)[:, None, :]
        high = zh_ref[k, j : j + n].astype(jnp.float32)[:, None, :]
        up = jnp.concatenate([mid[:, 1:], high], axis=1)
        down = jnp.concatenate([low, mid[:, :-1]], axis=1)
        taps_ref[k, j : j + n, :, 0:ch] = up.astype(jnp.bfloat16)
        taps_ref[k, j : j + n, :, ch : 2 * ch] = rows
        taps_ref[k, j : j + n, :, 2 * ch : 3 * ch] = down.astype(jnp.bfloat16)

    def plane(k, carry):
        fill(k, yl_ref[k][None], 0, 1)
        fill(k, yh_ref[k][None], ny + 1, 1)
        return carry

    def middle(k, carry):
        fill(k + 1, mid_ref[k], 1, ny)
        return carry

    lax.fori_loop(0, nx, middle, 0)
    fill(0, xl_ref[0], 1, ny)
    fill(nx + 1, xh_ref[0], 1, ny)
    lax.fori_loop(0, nx + 2, plane, 0)
    cells = nx * ny * nz
    flat = in_ref[...].T
    core = lax.axis_index("gx") % CORES
    for a in range(3):
        for b in range(3):
            view = taps_ref[2 - a : 2 - a + nx, 2 - b : 2 - b + ny].reshape(cells, 3 * ch)
            res = jnp.dot(flat, view, preferred_element_type=jnp.float32)
            lanes = pl.ds((a * 3 + b) * 3 * ch, 3 * ch)
            for g in range(ch // 32):
                first = res[g * 32 : g * 32 + 16]
                second = res[g * 32 + 16 : g * 32 + 32]
                keep_ref[g * 16 : g * 16 + 16, lanes] = jnp.where(core == 0, first, second)
                send_ref[g * 16 : g * 16 + 16, lanes] = jnp.where(core == 0, second, first).astype(jnp.bfloat16)


def pair_kernel(keep_ref, other_ref, out_ref):
    rows = out_ref.shape[1]
    for g in range(keep_ref.shape[0] // 16):
        total = keep_ref[g * 16 : g * 16 + 16] + other_ref[g * 16 : g * 16 + 16].astype(jnp.float32)
        for r in range(16 // rows):
            out_ref[g * (16 // rows) + r] = total[r * rows : (r + 1) * rows].astype(jnp.bfloat16)


def peers_kernel(parts_ref, out_ref):
    total = jnp.sum(parts_ref[...].astype(jnp.float32), axis=0).astype(jnp.bfloat16)
    for k in range(out_ref.shape[0]):
        out_ref[k] = total


def block_kernel(parts_ref, std_ref, grad_ref, sums_ref):
    ch = sums_ref.shape[2] // 3
    total = jnp.sum(parts_ref[...].astype(jnp.float32), axis=0)
    grad_ref[...] = total
    three = jnp.concatenate([fold(total, ch), fold(total * std_ref[...], ch), fold(total * total, ch)], axis=1)
    for k in range(sums_ref.shape[0]):
        sums_ref[k] = three


def input_kernel(taps_ref, std_ref, out_ref):
    nx, ny, nz, ch = out_ref.shape
    planes = 2
    std = std_ref[...]
    for x in range(0, nx, planes):
        rows = jnp.concatenate(
            [
                taps_ref[x + 2 - a : x + 2 - a + planes, 2 - b : 2 - b + ny].reshape(planes * ny * nz, 3 * ch)
                for a in range(3)
                for b in range(3)
            ],
            axis=1,
        )
        res = lax.dot_general(rows, std, (((1,), (1,)), ((), ())), preferred_element_type=jnp.float32)
        out_ref[x : x + planes] = res.astype(jnp.bfloat16).reshape(planes, ny, nz, ch)


def std_kernel(x_count, near_ref, far_ref, std_ref, mean_ref, inv_ref, block_ref):
    slots, rows, held = near_ref.shape
    ch = inv_ref.shape[1]
    width = held - ch
    taps = width // ch
    gx, y, x = lax.axis_index("gx"), lax.axis_index("gy"), lax.axis_index("gz") % x_count
    zl, core = gx // CORES, gx % CORES
    blocks = [(b // 8, (b // 4) % 2, b % 4) for b in range(2 * slots)]
    count = float(2 * slots * rows * taps)

    def parts(zl_b, core_b, y_b):
        slot = (y_b ^ y) + 4 * (zl_b ^ zl)
        data = jnp.where(core_b == core, near_ref[slot], far_ref[slot]).astype(jnp.float32)
        return data[:, :width], data[0:1, width:] + data[1:2, width:]

    total = jnp.zeros((1, ch), jnp.float32)
    for b in blocks:
        values, base = parts(*b)
        total = total + (fold(values, ch) + float(rows * taps) * base)
    mean = total / count
    square = jnp.zeros((1, ch), jnp.float32)
    for b in blocks:
        values, base = parts(*b)
        first = values + wide(base - mean)
        square = square + fold(first * first, ch)
    inv = lax.rsqrt(square / count + var_eps)
    mean_ref[...] = mean
    inv_ref[...] = inv
    inv_wide = wide(inv)
    for n, b in enumerate(blocks):
        values, base = parts(*b)
        std_ref[n * rows : (n + 1) * rows, :] = ((values + wide(base - mean)) * inv_wide).astype(jnp.bfloat16)
    values, base = parts(x, core, y)
    block_ref[...] = (values + wide(base - mean)) * inv_wide


def last_kernel(fan_count, grad_ref, raw_ref, mean_ref, inv_ref, sums_ref, out_ref):
    taps, _, ch = raw_ref.shape
    sums = jnp.sum(sums_ref[...], axis=0)
    sum_grad, sum_cross, sum_square = sums[:, :ch], sums[:, ch : 2 * ch], sums[:, 2 * ch :]
    mean, inv = mean_ref[...], inv_ref[...]
    mean_grad = sum_grad / fan_count
    mean_cross = sum_cross / fan_count
    shrink = 1.0 - var_eps * inv * inv
    per_output = sum_square - 2.0 * mean_grad * sum_grad - 2.0 * mean_cross * sum_cross
    per_output = per_output + fan_count * mean_grad * mean_grad + fan_count * mean_cross * mean_cross * shrink
    square_sum = jnp.sum(inv * inv * per_output, axis=1, keepdims=True)
    scale = jnp.minimum(1.0, clip_norm * lax.rsqrt(square_sum + norm_eps))
    factor = inv * scale
    for t in range(taps):
        std = (raw_ref[t] - mean) * inv
        out_ref[t] = factor * (grad_ref[:, t * ch : (t + 1) * ch] - mean_grad - std * mean_cross)


def on_device(where, raw_weight, inputs, cotangent):
    nx, ny, nz, ch = inputs.shape
    rows, taps = raw_weight.shape[:2]
    width = taps * ch
    bf16, f32 = jnp.bfloat16, jnp.float32
    raw = jnp.transpose(raw_weight, (1, 0, 2))

    def joined(held, got):
        return jnp.concatenate([held, got], 0)

    x_low = shift(cotangent[-1:], "gx", 1)
    x_high = shift(cotangent[:1], "gx", -1)
    held = call(base_kernel, of((1, rows, width + ch), bf16), (raw,))
    held = joined(held, where.send(held, lambda s: dict(y=s["y"] ^ 1)))
    y_low = shift(jnp.concatenate([a[:, -1] for a in (x_low, cotangent, x_high)], 0), "gy", 1)
    y_high = shift(jnp.concatenate([a[:, 0] for a in (x_low, cotangent, x_high)], 0), "gy", -1)
    held = joined(held, where.send(held, lambda s: dict(y=s["y"] ^ 2)))

    def face(k):
        deep = jnp.concatenate([a[:, :, k] for a in (x_low, cotangent, x_high)], 0)
        return jnp.concatenate([y_low[:, None, k], deep, y_high[:, None, k]], 1)

    z_low = shift(face(nz - 1), "gz", 1)
    z_high = shift(face(0), "gz", -1)
    held = joined(held, where.send(held, lambda s: dict(zl=s["zl"] ^ 1)))

    flops = 2 * nx * ny * nz * ch * width
    tap_views, keep, send = call(
        filter_kernel,
        (of((nx + 2, ny + 2, nz, 3 * ch), bf16), of((ch // 2, width), f32), of((ch // 2, width), bf16)),
        (cotangent, x_low, x_high, y_low, y_high, z_low, z_high, inputs.reshape(-1, ch)),
        vmem=16,
        flops=2 * flops,
    )
    other = where.send(send, lambda s: dict(core=1 - s["core"]))
    held = joined(held, where.send(held, lambda s: dict(zl=s["zl"] ^ 2)))
    peers = where.x * where.gy
    half = call(pair_kernel, of((peers, rows, width), bf16), (keep, other))
    parts = where.exchange(half, ("core", "zl", "zh"), lambda s: (s["x"], s["y"]))
    far = where.send(held, lambda s: dict(core=1 - s["core"]))
    std_half, mean_out, inv_std, block_std = call(
        functools.partial(std_kernel, where.x),
        (of((ch, width), bf16), of((1, ch), f32), of((1, ch), f32), of((rows, width), f32)),
        (held, far),
        flops=3_000_000_000,
    )
    parts, inv_std = lax.optimization_barrier((parts, inv_std))
    copies = call(peers_kernel, of((where.zl * where.zh, rows, width), bf16), (parts,))
    parts = where.exchange(copies, ("core", "x", "y"), lambda s: (s["zh"], s["zl"]))
    input_grad = call(input_kernel, of(inputs.shape, bf16), (tap_views, std_half), vmem=16, flops=2 * flops)
    parts, input_grad = lax.optimization_barrier((parts, input_grad))
    everyone = CORES * where.x * where.gy
    block_grad, local = call(block_kernel, (of((rows, width), f32), of((everyone, 1, 3 * ch), f32)), (parts, block_std))
    filter_grad = where.send(block_grad, lambda s: dict(x=s["zl"], zl=s["x"]))
    sums = where.exchange(local, ("zl", "zh"), lambda s: (s["core"], s["x"], s["y"]))

    grad = call(functools.partial(last_kernel, float(ch * taps)), of((taps, rows, ch), f32), (filter_grad, raw, mean_out, inv_std, sums))
    return (input_grad, jnp.transpose(grad, (1, 0, 2)))


def solution(mesh):
    where = Layout(mesh)
    in_specs = (P(("gx", "gy"), None, None), P("gx", "gy", "gz", None), P("gx", "gy", "gz", None))
    out_specs = (P("gx", "gy", "gz", None), P(("gx", "gy"), None, None))

    def body(raw_weight, inputs, cotangent):
        return on_device(where, raw_weight, inputs, cotangent)

    return jax.shard_map(body, mesh=mesh, in_specs=in_specs, out_specs=out_specs, check_vma=False)
```

```python
import functools

import jax
import jax.numpy as jnp
from jax import lax
from jax.experimental import pallas as pl
from jax.experimental.pallas import tpu as pltpu
from jax.sharding import PartitionSpec as P


var_eps = 1e-05
norm_eps = 1e-06
clip_norm = 600.0
AXES = ("gx", "gy", "gz")
CORES = 2
TAPS = 27
MIB = 1024 * 1024


def call(kernel, out_shape, args, vmem=8, flops=1_000_000_000):
    many = isinstance(out_shape, tuple)
    return pl.pallas_call(
        kernel,
        out_shape=out_shape,
        in_specs=[pl.BlockSpec(memory_space=pltpu.VMEM) for _ in args],
        out_specs=tuple(pl.BlockSpec(memory_space=pltpu.VMEM) for _ in out_shape)
        if many
        else pl.BlockSpec(memory_space=pltpu.VMEM),
        compiler_params=pltpu.CompilerParams(vmem_limit_bytes=vmem * MIB),
        cost_estimate=pl.CostEstimate(flops=flops, bytes_accessed=1_000_000, transcendentals=0),
    )(*args)


def of(shape, dtype):
    return jax.ShapeDtypeStruct(shape, dtype)


class Layout:
    def __init__(self, mesh):
        self.gx, self.gy, self.gz = (mesh.shape[a] for a in AXES)
        self.zl = self.gx // CORES
        self.x = self.zl
        self.zh = self.gz // self.x

    def spots(self):
        for zl in range(self.zl):
            for core in range(CORES):
                for y in range(self.gy):
                    for zh in range(self.zh):
                        for x in range(self.x):
                            yield dict(zl=zl, core=core, y=y, zh=zh, x=x)

    def index(self, s):
        return ((s["zl"] * CORES + s["core"]) * self.gy + s["y"]) * self.gz + s["zh"] * self.x + s["x"]

    def send(self, array, target):
        pairs = []
        for s in self.spots():
            t = dict(s)
            t.update(target(s))
            pairs.append((self.index(s), self.index(t)))
        return lax.ppermute(array, AXES, pairs)

    def exchange(self, array, fixed, order):
        groups = {}
        for s in self.spots():
            groups.setdefault(tuple(s[k] for k in fixed), []).append((order(s), self.index(s)))
        groups = [[i for _, i in sorted(g)] for g in groups.values()]
        return lax.all_to_all(array, AXES, 0, 0, tiled=True, axis_index_groups=groups)


def swapped(first, second, axis):
    count = lax.axis_size(axis)

    def pairs(start):
        ends = [(i, i + 1) for i in range(start, count - 1, 2)]
        return ends + [(j, i) for i, j in ends]

    return lax.ppermute(first, axis, pairs(0)), lax.ppermute(second, axis, pairs(1))


def is_odd(axis):
    return lax.axis_index(axis) % 2 == 1


def wide(row, taps=TAPS):
    return jnp.concatenate([row] * taps, axis=1)


def fold(values, ch):
    total = values[:, 0:ch]
    for t in range(1, values.shape[1] // ch):
        total = total + values[:, t * ch : (t + 1) * ch]
    return jnp.sum(total, axis=0, keepdims=True)


def faces_kernel(mid_ref, first_ref, second_ref):
    last = mid_ref.shape[0] - 1
    odd = is_odd("gx")
    first_ref[0] = mid_ref[jnp.where(odd, 0, last)]
    second_ref[0] = mid_ref[jnp.where(odd, last, 0)]


def base_kernel(raw_ref, mid_ref, held_ref, zl_ref, zh_ref):
    taps, rows, ch = raw_ref.shape
    base = jnp.sum(jnp.sum(raw_ref[...], axis=0), axis=0, keepdims=True) / (taps * rows)
    high = base.astype(jnp.bfloat16)
    low = (base - high.astype(jnp.float32)).astype(jnp.bfloat16)
    base = high.astype(jnp.float32) + low.astype(jnp.float32)
    for t in range(taps):
        held_ref[0, :, t * ch : (t + 1) * ch] = (raw_ref[t] - base).astype(jnp.bfloat16)
    place = lax.broadcasted_iota(jnp.int32, (rows, ch), 0)
    both = jnp.where(place == 0, high.astype(jnp.float32), low.astype(jnp.float32))
    held_ref[0, :, taps * ch :] = both.astype(jnp.bfloat16)
    nz = mid_ref.shape[2]
    for k in range(mid_ref.shape[0]):
        mid = mid_ref[k].astype(jnp.float32)
        zl_ref[k] = mid[:, 0].astype(jnp.bfloat16)
        zh_ref[k] = mid[:, nz - 1].astype(jnp.bfloat16)


def picked(odd, first, second):
    return jnp.where(odd, first, second), jnp.where(odd, second, first)


def height_kernel(mid_ref, xa_ref, xb_ref, first_ref, second_ref):
    nx, ny = mid_ref.shape[:2]
    x_odd, odd = is_odd("gx"), is_odd("gy")
    for out_ref, j in ((first_ref, jnp.where(odd, 0, ny - 1)), (second_ref, jnp.where(odd, ny - 1, 0))):
        low, high = picked(x_odd, xa_ref[0, j], xb_ref[0, j])
        out_ref[0] = low
        out_ref[nx + 1] = high
        for k in range(nx):
            out_ref[k + 1] = mid_ref[k, j]


def width_kernel(zl_ref, zh_ref, xa_ref, xb_ref, ya_ref, yb_ref, first_ref, second_ref):
    nz = ya_ref.shape[1]
    x_odd, y_odd, odd = is_odd("gx"), is_odd("gy"), is_odd("gz")

    def face(k, own):
        x_low, x_high = picked(x_odd, xa_ref[0].astype(jnp.float32)[:, k], xb_ref[0].astype(jnp.float32)[:, k])
        y_low, y_high = picked(y_odd, ya_ref[...].astype(jnp.float32)[:, k], yb_ref[...].astype(jnp.float32)[:, k])
        deep = jnp.concatenate([x_low[None], own.astype(jnp.float32), x_high[None]], axis=0)
        return jnp.concatenate([y_low[:, None], deep, y_high[:, None]], axis=1)

    low, high = face(0, zl_ref[...]), face(nz - 1, zh_ref[...])
    first_ref[...] = jnp.where(odd, low, high).astype(jnp.bfloat16)
    second_ref[...] = jnp.where(odd, high, low).astype(jnp.bfloat16)


def filter_kernel(mid_ref, xa_ref, xb_ref, ya_ref, yb_ref, za_ref, zb_ref, in_ref, taps_ref, keep_ref, send_ref):
    nx, ny, nz, ch = mid_ref.shape
    x_odd, y_odd, z_odd = is_odd("gx"), is_odd("gy"), is_odd("gz")

    def fill(k, rows, j, n):
        mid = rows.astype(jnp.float32)
        low, high = picked(z_odd, za_ref[k, j : j + n], zb_ref[k, j : j + n])
        low = low.astype(jnp.float32)[:, None, :]
        high = high.astype(jnp.float32)[:, None, :]
        up = jnp.concatenate([mid[:, 1:], high], axis=1)
        down = jnp.concatenate([low, mid[:, :-1]], axis=1)
        taps_ref[k, j : j + n, :, 0:ch] = up.astype(jnp.bfloat16)
        taps_ref[k, j : j + n, :, ch : 2 * ch] = rows
        taps_ref[k, j : j + n, :, 2 * ch : 3 * ch] = down.astype(jnp.bfloat16)

    def plane(k, carry):
        low, high = picked(y_odd, ya_ref[k], yb_ref[k])
        fill(k, low[None], 0, 1)
        fill(k, high[None], ny + 1, 1)
        return carry

    def middle(k, carry):
        fill(k + 1, mid_ref[k], 1, ny)
        return carry

    lax.fori_loop(0, nx, middle, 0)
    low, high = picked(x_odd, xa_ref[0], xb_ref[0])
    fill(0, low, 1, ny)
    fill(nx + 1, high, 1, ny)
    lax.fori_loop(0, nx + 2, plane, 0)
    cells = nx * ny * nz
    flat = in_ref[...].T
    core = lax.axis_index("gx") % CORES
    for a in range(3):
        for b in range(3):
            view = taps_ref[2 - a : 2 - a + nx, 2 - b : 2 - b + ny].reshape(cells, 3 * ch)
            res = jnp.dot(flat, view, preferred_element_type=jnp.float32)
            lanes = pl.ds((a * 3 + b) * 3 * ch, 3 * ch)
            for g in range(ch // 32):
                first = res[g * 32 : g * 32 + 16]
                second = res[g * 32 + 16 : g * 32 + 32]
                keep_ref[g * 16 : g * 16 + 16, lanes] = jnp.where(core == 0, first, second)
                send_ref[g * 16 : g * 16 + 16, lanes] = jnp.where(core == 0, second, first).astype(jnp.bfloat16)


def pair_kernel(keep_ref, other_ref, out_ref):
    rows = out_ref.shape[1]
    for g in range(keep_ref.shape[0] // 16):
        total = keep_ref[g * 16 : g * 16 + 16] + other_ref[g * 16 : g * 16 + 16].astype(jnp.float32)
        for r in range(16 // rows):
            out_ref[g * (16 // rows) + r] = total[r * rows : (r + 1) * rows].astype(jnp.bfloat16)


def peers_kernel(parts_ref, out_ref):
    total = jnp.sum(parts_ref[...].astype(jnp.float32), axis=0).astype(jnp.bfloat16)
    for k in range(out_ref.shape[0]):
        out_ref[k] = total


def block_kernel(parts_ref, std_ref, grad_ref, sums_ref):
    ch = sums_ref.shape[2] // 3
    total = jnp.sum(parts_ref[...].astype(jnp.float32), axis=0)
    grad_ref[...] = total
    three = jnp.concatenate([fold(total, ch), fold(total * std_ref[...], ch), fold(total * total, ch)], axis=1)
    for k in range(sums_ref.shape[0]):
        sums_ref[k] = three


def input_kernel(taps_ref, std_ref, out_ref):
    nx, ny, nz, ch = out_ref.shape
    planes = 2
    std = std_ref[...]
    for x in range(0, nx, planes):
        rows = jnp.concatenate(
            [
                taps_ref[x + 2 - a : x + 2 - a + planes, 2 - b : 2 - b + ny].reshape(planes * ny * nz, 3 * ch)
                for a in range(3)
                for b in range(3)
            ],
            axis=1,
        )
        res = lax.dot_general(rows, std, (((1,), (1,)), ((), ())), preferred_element_type=jnp.float32)
        out_ref[x : x + planes] = res.astype(jnp.bfloat16).reshape(planes, ny, nz, ch)


def std_kernel(x_count, near_ref, far_ref, std_ref, mean_ref, inv_ref, block_ref):
    slots, rows, held = near_ref.shape
    ch = inv_ref.shape[1]
    width = held - ch
    taps = width // ch
    gx, y, x = lax.axis_index("gx"), lax.axis_index("gy"), lax.axis_index("gz") % x_count
    zl, core = gx // CORES, gx % CORES
    blocks = [(b // 8, (b // 4) % 2, b % 4) for b in range(2 * slots)]
    count = float(2 * slots * rows * taps)

    def parts(zl_b, core_b, y_b):
        slot = (y_b ^ y) + 4 * (zl_b ^ zl)
        data = jnp.where(core_b == core, near_ref[slot], far_ref[slot]).astype(jnp.float32)
        return data[:, :width], data[0:1, width:] + data[1:2, width:]

    total = jnp.zeros((1, ch), jnp.float32)
    for b in blocks:
        values, base = parts(*b)
        total = total + (fold(values, ch) + float(rows * taps) * base)
    mean = total / count
    square = jnp.zeros((1, ch), jnp.float32)
    for b in blocks:
        values, base = parts(*b)
        first = values + wide(base - mean)
        square = square + fold(first * first, ch)
    inv = lax.rsqrt(square / count + var_eps)
    mean_ref[...] = mean
    inv_ref[...] = inv
    inv_wide = wide(inv)
    for n, b in enumerate(blocks):
        values, base = parts(*b)
        std_ref[n * rows : (n + 1) * rows, :] = ((values + wide(base - mean)) * inv_wide).astype(jnp.bfloat16)
    values, base = parts(x, core, y)
    block_ref[...] = (values + wide(base - mean)) * inv_wide


def last_kernel(fan_count, grad_ref, raw_ref, mean_ref, inv_ref, sums_ref, out_ref):
    taps, _, ch = raw_ref.shape
    sums = jnp.sum(sums_ref[...], axis=0)
    sum_grad, sum_cross, sum_square = sums[:, :ch], sums[:, ch : 2 * ch], sums[:, 2 * ch :]
    mean, inv = mean_ref[...], inv_ref[...]
    mean_grad = sum_grad / fan_count
    mean_cross = sum_cross / fan_count
    shrink = 1.0 - var_eps * inv * inv
    per_output = sum_square - 2.0 * mean_grad * sum_grad - 2.0 * mean_cross * sum_cross
    per_output = per_output + fan_count * mean_grad * mean_grad + fan_count * mean_cross * mean_cross * shrink
    square_sum = jnp.sum(inv * inv * per_output, axis=1, keepdims=True)
    scale = jnp.minimum(1.0, clip_norm * lax.rsqrt(square_sum + norm_eps))
    factor = inv * scale
    for t in range(taps):
        std = (raw_ref[t] - mean) * inv
        out_ref[t] = factor * (grad_ref[:, t * ch : (t + 1) * ch] - mean_grad - std * mean_cross)


def on_device(where, raw_weight, inputs, cotangent):
    nx, ny, nz, ch = inputs.shape
    rows, taps = raw_weight.shape[:2]
    width = taps * ch
    bf16, f32 = jnp.bfloat16, jnp.float32
    raw = jnp.transpose(raw_weight, (1, 0, 2))

    def joined(held, got):
        return jnp.concatenate([held, got], 0)

    def both(shape):
        return (of(shape, bf16), of(shape, bf16))

    faces = call(faces_kernel, both((1, ny, nz, ch)), (cotangent,))
    x_halo = swapped(*faces, "gx")
    held, *width_faces = call(base_kernel, (of((1, rows, width + ch), bf16), *both((nx, ny, ch))), (raw, cotangent))
    held = joined(held, where.send(held, lambda s: dict(y=s["y"] ^ 1)))
    faces = call(height_kernel, both((nx + 2, nz, ch)), (cotangent, *x_halo))
    y_halo = swapped(*faces, "gy")
    held = joined(held, where.send(held, lambda s: dict(y=s["y"] ^ 2)))
    faces = call(width_kernel, both((nx + 2, ny + 2, ch)), (*width_faces, *x_halo, *y_halo))
    z_halo = swapped(*faces, "gz")
    held = joined(held, where.send(held, lambda s: dict(zl=s["zl"] ^ 1)))

    flops = 2 * nx * ny * nz * ch * width
    tap_views, keep, send = call(
        filter_kernel,
        (of((nx + 2, ny + 2, nz, 3 * ch), bf16), of((ch // 2, width), f32), of((ch // 2, width), bf16)),
        (cotangent, *x_halo, *y_halo, *z_halo, inputs.reshape(-1, ch)),
        vmem=16,
        flops=2 * flops,
    )
    other = where.send(send, lambda s: dict(core=1 - s["core"]))
    held = joined(held, where.send(held, lambda s: dict(zl=s["zl"] ^ 2)))
    peers = where.x * where.gy
    half = call(pair_kernel, of((peers, rows, width), bf16), (keep, other))
    parts = where.exchange(half, ("core", "zl", "zh"), lambda s: (s["x"], s["y"]))
    far = where.send(held, lambda s: dict(core=1 - s["core"]))
    std_half, mean_out, inv_std, block_std = call(
        functools.partial(std_kernel, where.x),
        (of((ch, width), bf16), of((1, ch), f32), of((1, ch), f32), of((rows, width), f32)),
        (held, far),
        flops=3_000_000_000,
    )
    parts, inv_std = lax.optimization_barrier((parts, inv_std))
    copies = call(peers_kernel, of((where.zl * where.zh, rows, width), bf16), (parts,))
    parts = where.exchange(copies, ("core", "x", "y"), lambda s: (s["zh"], s["zl"]))
    input_grad = call(input_kernel, of(inputs.shape, bf16), (tap_views, std_half), vmem=16, flops=2 * flops)
    parts, input_grad = lax.optimization_barrier((parts, input_grad))
    everyone = CORES * where.x * where.gy
    block_grad, local = call(block_kernel, (of((rows, width), f32), of((everyone, 1, 3 * ch), f32)), (parts, block_std))
    filter_grad = where.send(block_grad, lambda s: dict(x=s["zl"], zl=s["x"]))
    sums = where.exchange(local, ("zl", "zh"), lambda s: (s["core"], s["x"], s["y"]))

    grad = call(functools.partial(last_kernel, float(ch * taps)), of((taps, rows, ch), f32), (filter_grad, raw, mean_out, inv_std, sums))
    return (input_grad, jnp.transpose(grad, (1, 0, 2)))


def solution(mesh):
    where = Layout(mesh)
    in_specs = (P(("gx", "gy"), None, None), P("gx", "gy", "gz", None), P("gx", "gy", "gz", None))
    out_specs = (P("gx", "gy", "gz", None), P(("gx", "gy"), None, None))

    def body(raw_weight, inputs, cotangent):
        return on_device(where, raw_weight, inputs, cotangent)

    return jax.shard_map(body, mesh=mesh, in_specs=in_specs, out_specs=out_specs, check_vma=False)
```

```python
import functools

import jax
import jax.numpy as jnp
from jax import lax
from jax.experimental import pallas as pl
from jax.experimental.pallas import tpu as pltpu
from jax.sharding import PartitionSpec as P


var_eps = 1e-05
norm_eps = 1e-06
clip_norm = 600.0
AXES = ("gx", "gy", "gz")
CORES = 2
TAPS = 27
MIB = 1024 * 1024


def call(kernel, out_shape, args, vmem=8, flops=1_000_000_000):
    many = isinstance(out_shape, tuple)
    return pl.pallas_call(
        kernel,
        out_shape=out_shape,
        in_specs=[pl.BlockSpec(memory_space=pltpu.VMEM) for _ in args],
        out_specs=tuple(pl.BlockSpec(memory_space=pltpu.VMEM) for _ in out_shape)
        if many
        else pl.BlockSpec(memory_space=pltpu.VMEM),
        compiler_params=pltpu.CompilerParams(vmem_limit_bytes=vmem * MIB),
        cost_estimate=pl.CostEstimate(flops=flops, bytes_accessed=1_000_000, transcendentals=0),
    )(*args)


def of(shape, dtype):
    return jax.ShapeDtypeStruct(shape, dtype)


class Layout:
    def __init__(self, mesh):
        self.gx, self.gy, self.gz = (mesh.shape[a] for a in AXES)
        self.zl = self.gx // CORES
        self.x = self.zl
        self.zh = self.gz // self.x

    def spots(self):
        for zl in range(self.zl):
            for core in range(CORES):
                for y in range(self.gy):
                    for zh in range(self.zh):
                        for x in range(self.x):
                            yield dict(zl=zl, core=core, y=y, zh=zh, x=x)

    def index(self, s):
        return ((s["zl"] * CORES + s["core"]) * self.gy + s["y"]) * self.gz + s["zh"] * self.x + s["x"]

    def send(self, array, target):
        pairs = []
        for s in self.spots():
            t = dict(s)
            t.update(target(s))
            pairs.append((self.index(s), self.index(t)))
        return lax.ppermute(array, AXES, pairs)

    def pass_on(self, array, step):
        pairs = []
        for s in self.spots():
            if s["x"] == s["zl"]:
                pairs.append((self.index(s), self.index(dict(s, x=(s["x"] + step) % self.x))))
        return lax.ppermute(array, AXES, pairs)

    def exchange(self, array, fixed, order):
        groups = {}
        for s in self.spots():
            groups.setdefault(tuple(s[k] for k in fixed), []).append((order(s), self.index(s)))
        groups = [[i for _, i in sorted(g)] for g in groups.values()]
        return lax.all_to_all(array, AXES, 0, 0, tiled=True, axis_index_groups=groups)


def swapped(first, second, axis):
    count = lax.axis_size(axis)

    def pairs(start):
        ends = [(i, i + 1) for i in range(start, count - 1, 2)]
        return ends + [(j, i) for i, j in ends]

    return lax.ppermute(first, axis, pairs(0)), lax.ppermute(second, axis, pairs(1))


def is_odd(axis):
    return lax.axis_index(axis) % 2 == 1


def wide(row, taps=TAPS):
    return jnp.concatenate([row] * taps, axis=1)


def fold(values, ch):
    total = values[:, 0:ch]
    for t in range(1, values.shape[1] // ch):
        total = total + values[:, t * ch : (t + 1) * ch]
    return jnp.sum(total, axis=0, keepdims=True)


def picked(odd, first, second):
    return jnp.where(odd, first, second), jnp.where(odd, second, first)


def width_kernel(mid_ref, first_ref, second_ref):
    nx, _, nz, _ = mid_ref.shape
    odd = is_odd("gz")
    for k in range(nx):
        mid = mid_ref[k].astype(jnp.float32)
        low, high = mid[:, 0], mid[:, nz - 1]
        first_ref[k] = jnp.where(odd, low, high).astype(jnp.bfloat16)
        second_ref[k] = jnp.where(odd, high, low).astype(jnp.bfloat16)


def height_kernel(mid_ref, za_ref, zb_ref, first_ref, second_ref):
    nx, ny, nz, _ = mid_ref.shape
    odd = is_odd("gy")
    low, high = picked(is_odd("gz"), za_ref[...].astype(jnp.float32), zb_ref[...].astype(jnp.float32))
    ends = [jnp.concatenate([low[:, None, j], high[:, None, j]], axis=1) for j in (0, ny - 1)]
    first_end, last_end = (e.astype(jnp.bfloat16) for e in ends)
    for k in range(nx):
        first_ref[k, :nz] = mid_ref[k, jnp.where(odd, 0, ny - 1)]
        second_ref[k, :nz] = mid_ref[k, jnp.where(odd, ny - 1, 0)]
    first_ref[:, nz:] = jnp.where(odd, first_end, last_end)
    second_ref[:, nz:] = jnp.where(odd, last_end, first_end)


def depth_kernel(mid_ref, za_ref, zb_ref, ya_ref, yb_ref, first_ref, second_ref):
    nx, ny, nz, _ = mid_ref.shape
    z_odd, y_odd, odd = is_odd("gz"), is_odd("gy"), is_odd("gx")
    for out_ref, k in ((first_ref, jnp.where(odd, 0, nx - 1)), (second_ref, jnp.where(odd, nx - 1, 0))):
        low, high = picked(z_odd, za_ref[k].astype(jnp.float32), zb_ref[k].astype(jnp.float32))
        out_ref[1 : ny + 1, :nz] = mid_ref[k]
        out_ref[1 : ny + 1, nz:] = jnp.concatenate([low[:, None], high[:, None]], axis=1).astype(jnp.bfloat16)
        low, high = picked(y_odd, ya_ref[k], yb_ref[k])
        out_ref[0] = low
        out_ref[ny + 1] = high


def base_kernel(raw_ref, held_ref):
    taps, rows, ch = raw_ref.shape
    base = jnp.sum(jnp.sum(raw_ref[...], axis=0), axis=0, keepdims=True) / (taps * rows)
    high = base.astype(jnp.bfloat16)
    low = (base - high.astype(jnp.float32)).astype(jnp.bfloat16)
    base = high.astype(jnp.float32) + low.astype(jnp.float32)
    for t in range(taps):
        held_ref[0, :, t * ch : (t + 1) * ch] = (raw_ref[t] - base).astype(jnp.bfloat16)
    place = lax.broadcasted_iota(jnp.int32, (rows, ch), 0)
    both = jnp.where(place == 0, high.astype(jnp.float32), low.astype(jnp.float32))
    held_ref[0, :, taps * ch :] = both.astype(jnp.bfloat16)


def join_kernel(*refs):
    place = 0
    for piece in refs[:-1]:
        refs[-1][place : place + piece.shape[0]] = piece[...]
        place += piece.shape[0]


def filter_kernel(mid_ref, za_ref, zb_ref, ya_ref, yb_ref, xa_ref, xb_ref, in_ref, taps_ref, keep_ref, send_ref):
    nx, ny, nz, ch = mid_ref.shape
    x_odd, y_odd, z_odd = is_odd("gx"), is_odd("gy"), is_odd("gz")

    def fill(k, j, rows, low, high):
        n = rows.shape[0]
        mid = rows.astype(jnp.float32)
        up = jnp.concatenate([mid[:, 1:], high], axis=1)
        down = jnp.concatenate([low, mid[:, :-1]], axis=1)
        taps_ref[k, j : j + n, :, 0:ch] = up.astype(jnp.bfloat16)
        taps_ref[k, j : j + n, :, ch : 2 * ch] = rows
        taps_ref[k, j : j + n, :, 2 * ch : 3 * ch] = down.astype(jnp.bfloat16)

    def fill_face(k, j, rows):
        ends = rows[:, nz:].astype(jnp.float32)
        fill(k, j, rows[:, :nz], ends[:, 0:1], ends[:, 1:2])

    def plane(k, carry):
        low, high = picked(z_odd, za_ref[k].astype(jnp.float32), zb_ref[k].astype(jnp.float32))
        fill(k + 1, 1, mid_ref[k], low[:, None], high[:, None])
        low, high = picked(y_odd, ya_ref[k], yb_ref[k])
        fill_face(k + 1, 0, low[None])
        fill_face(k + 1, ny + 1, high[None])
        return carry

    lax.fori_loop(0, nx, plane, 0)
    low, high = picked(x_odd, xa_ref[...], xb_ref[...])
    fill_face(0, 0, low)
    fill_face(nx + 1, 0, high)
    cells = nx * ny * nz
    flat = in_ref[...].T
    core = lax.axis_index("gx") % CORES
    for a in range(3):
        for b in range(3):
            view = taps_ref[2 - a : 2 - a + nx, 2 - b : 2 - b + ny].reshape(cells, 3 * ch)
            res = jnp.dot(flat, view, preferred_element_type=jnp.float32)
            lanes = pl.ds((a * 3 + b) * 3 * ch, 3 * ch)
            for g in range(ch // 32):
                first = res[g * 32 : g * 32 + 16]
                second = res[g * 32 + 16 : g * 32 + 32]
                keep_ref[g * 16 : g * 16 + 16, lanes] = jnp.where(core == 0, first, second)
                send_ref[g * 16 : g * 16 + 16, lanes] = jnp.where(core == 0, second, first).astype(jnp.bfloat16)


def pair_kernel(keep_ref, other_ref, out_ref):
    rows = out_ref.shape[1]
    for g in range(keep_ref.shape[0] // 16):
        total = keep_ref[g * 16 : g * 16 + 16] + other_ref[g * 16 : g * 16 + 16].astype(jnp.float32)
        for r in range(16 // rows):
            out_ref[g * (16 // rows) + r] = total[r * rows : (r + 1) * rows].astype(jnp.bfloat16)


def peers_kernel(parts_ref, out_ref):
    total = jnp.sum(parts_ref[...].astype(jnp.float32), axis=0).astype(jnp.bfloat16)
    for k in range(out_ref.shape[0]):
        out_ref[k] = total


def block_kernel(parts_ref, std_ref, grad_ref, sums_ref):
    ch = sums_ref.shape[2] // 3
    total = jnp.sum(parts_ref[...].astype(jnp.float32), axis=0)
    grad_ref[...] = total
    three = jnp.concatenate([fold(total, ch), fold(total * std_ref[...], ch), fold(total * total, ch)], axis=1)
    for k in range(sums_ref.shape[0]):
        sums_ref[k] = three


def input_kernel(taps_ref, std_ref, out_ref):
    nx, ny, nz, ch = out_ref.shape
    planes = 2
    std = std_ref[...]
    for x in range(0, nx, planes):
        rows = jnp.concatenate(
            [
                taps_ref[x + 2 - a : x + 2 - a + planes, 2 - b : 2 - b + ny].reshape(planes * ny * nz, 3 * ch)
                for a in range(3)
                for b in range(3)
            ],
            axis=1,
        )
        res = lax.dot_general(rows, std, (((1,), (1,)), ((), ())), preferred_element_type=jnp.float32)
        out_ref[x : x + planes] = res.astype(jnp.bfloat16).reshape(planes, ny, nz, ch)


def std_kernel(x_count, near_ref, far_ref, std_ref, mean_ref, inv_ref, block_ref):
    slots, rows, held = near_ref.shape
    ch = inv_ref.shape[1]
    width = held - ch
    taps = width // ch
    gx, y, x = lax.axis_index("gx"), lax.axis_index("gy"), lax.axis_index("gz") % x_count
    zl, core = gx // CORES, gx % CORES
    blocks = [(b // 8, (b // 4) % 2, b % 4) for b in range(2 * slots)]
    count = float(2 * slots * rows * taps)

    def parts(zl_b, core_b, y_b):
        slot = (y_b ^ y) + 4 * (zl_b ^ zl)
        data = jnp.where(core_b == core, near_ref[slot], far_ref[slot]).astype(jnp.float32)
        return data[:, :width], data[0:1, width:] + data[1:2, width:]

    total = jnp.zeros((1, ch), jnp.float32)
    for b in blocks:
        values, base = parts(*b)
        total = total + (fold(values, ch) + float(rows * taps) * base)
    mean = total / count
    square = jnp.zeros((1, ch), jnp.float32)
    for b in blocks:
        values, base = parts(*b)
        first = values + wide(base - mean)
        square = square + fold(first * first, ch)
    inv = lax.rsqrt(square / count + var_eps)
    mean_ref[...] = mean
    inv_ref[...] = inv
    inv_wide = wide(inv)
    for n, b in enumerate(blocks):
        values, base = parts(*b)
        std_ref[n * rows : (n + 1) * rows, :] = ((values + wide(base - mean)) * inv_wide).astype(jnp.bfloat16)
    values, base = parts(x, core, y)
    block_ref[...] = (values + wide(base - mean)) * inv_wide


def last_kernel(fan_count, x_count, own_ref, *refs):
    *got_refs, raw_ref, mean_ref, inv_ref, sums_ref, out_ref = refs
    taps, _, ch = raw_ref.shape
    grad = got_refs[0][...]
    for got_ref in got_refs[1:]:
        grad = grad + got_ref[...]
    holder = lax.axis_index("gz") % x_count == lax.axis_index("gx") // CORES
    grad = jnp.where(holder, own_ref[...], grad)
    sums = jnp.sum(sums_ref[...], axis=0)
    sum_grad, sum_cross, sum_square = sums[:, :ch], sums[:, ch : 2 * ch], sums[:, 2 * ch :]
    mean, inv = mean_ref[...], inv_ref[...]
    mean_grad = sum_grad / fan_count
    mean_cross = sum_cross / fan_count
    shrink = 1.0 - var_eps * inv * inv
    per_output = sum_square - 2.0 * mean_grad * sum_grad - 2.0 * mean_cross * sum_cross
    per_output = per_output + fan_count * mean_grad * mean_grad + fan_count * mean_cross * mean_cross * shrink
    square_sum = jnp.sum(inv * inv * per_output, axis=1, keepdims=True)
    scale = jnp.minimum(1.0, clip_norm * lax.rsqrt(square_sum + norm_eps))
    factor = inv * scale
    for t in range(taps):
        std = (raw_ref[t] - mean) * inv
        out_ref[t] = factor * (grad[:, t * ch : (t + 1) * ch] - mean_grad - std * mean_cross)


def on_device(where, raw_weight, inputs, cotangent):
    nx, ny, nz, ch = inputs.shape
    rows, taps = raw_weight.shape[:2]
    width = taps * ch
    bf16, f32 = jnp.bfloat16, jnp.float32
    raw = jnp.transpose(raw_weight, (1, 0, 2))

    def joined(held):
        return jnp.concatenate(held, 0)

    def both(shape):
        return (of(shape, bf16), of(shape, bf16))

    faces = call(width_kernel, both((nx, ny, ch)), (cotangent,))
    z_halo = swapped(*faces, "gz")
    held = [call(base_kernel, of((1, rows, width + ch), bf16), (raw,))]
    held.append(where.send(held[0], lambda s: dict(y=s["y"] ^ 1)))
    held.append(where.send(joined(held), lambda s: dict(y=s["y"] ^ 2)))
    faces = call(height_kernel, both((nx, nz + 2, ch)), (cotangent, *z_halo))
    y_halo = swapped(*faces, "gy")
    held.append(where.send(joined(held), lambda s: dict(zl=s["zl"] ^ 1)))
    faces = call(depth_kernel, both((ny + 2, nz + 2, ch)), (cotangent, *z_halo, *y_halo))
    x_halo = swapped(*faces, "gx")
    held.append(where.send(joined(held), lambda s: dict(zl=s["zl"] ^ 2)))

    flops = 2 * nx * ny * nz * ch * width
    tap_views, keep, send = call(
        filter_kernel,
        (of((nx + 2, ny + 2, nz, 3 * ch), bf16), of((ch // 2, width), f32), of((ch // 2, width), bf16)),
        (cotangent, *z_halo, *y_halo, *x_halo, inputs.reshape(-1, ch)),
        vmem=16,
        flops=2 * flops,
    )
    other = where.send(send, lambda s: dict(core=1 - s["core"]))
    held = call(join_kernel, of((16, rows, width + ch), bf16), held)
    peers = where.x * where.gy
    half = call(pair_kernel, of((peers, rows, width), bf16), (keep, other))
    parts = where.exchange(half, ("core", "zl", "zh"), lambda s: (s["x"], s["y"]))
    far = where.send(held, lambda s: dict(core=1 - s["core"]))
    std_half, mean_out, inv_std, block_std = call(
        functools.partial(std_kernel, where.x),
        (of((ch, width), bf16), of((1, ch), f32), of((1, ch), f32), of((rows, width), f32)),
        (held, far),
        flops=3_000_000_000,
    )
    parts, inv_std = lax.optimization_barrier((parts, inv_std))
    copies = call(peers_kernel, of((where.zl * where.zh, rows, width), bf16), (parts,))
    parts = where.exchange(copies, ("core", "x", "y"), lambda s: (s["zh"], s["zl"]))
    input_grad = call(input_kernel, of(inputs.shape, bf16), (tap_views, std_half), vmem=16, flops=2 * flops)
    parts, input_grad = lax.optimization_barrier((parts, input_grad))
    everyone = CORES * where.x * where.gy
    block_grad, local = call(block_kernel, (of((rows, width), f32), of((everyone, 1, 3 * ch), f32)), (parts, block_std))
    passed = [where.pass_on(block_grad, k) for k in range(1, where.x)]
    sums = where.exchange(local, ("zl", "zh"), lambda s: (s["core"], s["x"], s["y"]))

    grad = call(functools.partial(last_kernel, float(ch * taps), where.x), of((taps, rows, ch), f32), (block_grad, *passed, raw, mean_out, inv_std, sums))
    return (input_grad, jnp.transpose(grad, (1, 0, 2)))


def solution(mesh):
    where = Layout(mesh)
    in_specs = (P(("gx", "gy"), None, None), P("gx", "gy", "gz", None), P("gx", "gy", "gz", None))
    out_specs = (P("gx", "gy", "gz", None), P(("gx", "gy"), None, None))

    def body(raw_weight, inputs, cotangent):
        return on_device(where, raw_weight, inputs, cotangent)

    return jax.shard_map(body, mesh=mesh, in_specs=in_specs, out_specs=out_specs, check_vma=False)
```

```python
import functools

import jax
import jax.numpy as jnp
from jax import lax
from jax.experimental import pallas as pl
from jax.experimental.pallas import tpu as pltpu
from jax.sharding import PartitionSpec as P


var_eps = 1e-05
norm_eps = 1e-06
clip_norm = 600.0
AXES = ("gx", "gy", "gz")
CORES = 2
TAPS = 27
MIB = 1024 * 1024


def call(kernel, out_shape, args, vmem=8, flops=1_000_000_000):
    many = isinstance(out_shape, tuple)
    return pl.pallas_call(
        kernel,
        out_shape=out_shape,
        in_specs=[pl.BlockSpec(memory_space=pltpu.VMEM) for _ in args],
        out_specs=tuple(pl.BlockSpec(memory_space=pltpu.VMEM) for _ in out_shape)
        if many
        else pl.BlockSpec(memory_space=pltpu.VMEM),
        compiler_params=pltpu.CompilerParams(vmem_limit_bytes=vmem * MIB),
        cost_estimate=pl.CostEstimate(flops=flops, bytes_accessed=1_000_000, transcendentals=0),
    )(*args)


def of(shape, dtype):
    return jax.ShapeDtypeStruct(shape, dtype)


class Layout:
    def __init__(self, mesh):
        self.gx, self.gy, self.gz = (mesh.shape[a] for a in AXES)
        self.zl = self.gx // CORES
        self.x = self.zl
        self.zh = self.gz // self.x

    def spots(self):
        for zl in range(self.zl):
            for core in range(CORES):
                for y in range(self.gy):
                    for zh in range(self.zh):
                        for x in range(self.x):
                            yield dict(zl=zl, core=core, y=y, zh=zh, x=x)

    def index(self, s):
        return ((s["zl"] * CORES + s["core"]) * self.gy + s["y"]) * self.gz + s["zh"] * self.x + s["x"]

    def send(self, array, target):
        pairs = []
        for s in self.spots():
            t = dict(s)
            t.update(target(s))
            pairs.append((self.index(s), self.index(t)))
        return lax.ppermute(array, AXES, pairs)

    def exchange(self, array, fixed, order):
        groups = {}
        for s in self.spots():
            groups.setdefault(tuple(s[k] for k in fixed), []).append((order(s), self.index(s)))
        groups = [[i for _, i in sorted(g)] for g in groups.values()]
        return lax.all_to_all(array, AXES, 0, 0, tiled=True, axis_index_groups=groups)


def swapped(first, second, axis):
    count = lax.axis_size(axis)

    def pairs(start):
        ends = [(i, i + 1) for i in range(start, count - 1, 2)]
        return ends + [(j, i) for i, j in ends]

    return lax.ppermute(first, axis, pairs(0)), lax.ppermute(second, axis, pairs(1))


def is_odd(axis):
    return lax.axis_index(axis) % 2 == 1


def wide(row, taps=TAPS):
    return jnp.concatenate([row] * taps, axis=1)


def fold(values, ch):
    total = values[:, 0:ch]
    for t in range(1, values.shape[1] // ch):
        total = total + values[:, t * ch : (t + 1) * ch]
    return jnp.sum(total, axis=0, keepdims=True)


def faces_kernel(mid_ref, first_ref, second_ref):
    last = mid_ref.shape[0] - 1
    odd = is_odd("gx")
    first_ref[0] = mid_ref[jnp.where(odd, 0, last)]
    second_ref[0] = mid_ref[jnp.where(odd, last, 0)]


def base_kernel(raw_ref, mid_ref, held_ref, zl_ref, zh_ref):
    taps, rows, ch = raw_ref.shape
    base = jnp.sum(jnp.sum(raw_ref[...], axis=0), axis=0, keepdims=True) / (taps * rows)
    high = base.astype(jnp.bfloat16)
    low = (base - high.astype(jnp.float32)).astype(jnp.bfloat16)
    base = high.astype(jnp.float32) + low.astype(jnp.float32)
    for t in range(taps):
        held_ref[0, :, t * ch : (t + 1) * ch] = (raw_ref[t] - base).astype(jnp.bfloat16)
    place = lax.broadcasted_iota(jnp.int32, (rows, ch), 0)
    both = jnp.where(place == 0, high.astype(jnp.float32), low.astype(jnp.float32))
    held_ref[0, :, taps * ch :] = both.astype(jnp.bfloat16)
    nz = mid_ref.shape[2]
    for k in range(mid_ref.shape[0]):
        mid = mid_ref[k].astype(jnp.float32)
        zl_ref[k] = mid[:, 0].astype(jnp.bfloat16)
        zh_ref[k] = mid[:, nz - 1].astype(jnp.bfloat16)


def join_kernel(*refs):
    place = 0
    for piece in refs[:-1]:
        refs[-1][place : place + piece.shape[0]] = piece[...]
        place += piece.shape[0]


def picked(odd, first, second):
    return jnp.where(odd, first, second), jnp.where(odd, second, first)


def height_kernel(mid_ref, xa_ref, xb_ref, first_ref, second_ref):
    nx, ny = mid_ref.shape[:2]
    x_odd, odd = is_odd("gx"), is_odd("gy")
    for out_ref, j in ((first_ref, jnp.where(odd, 0, ny - 1)), (second_ref, jnp.where(odd, ny - 1, 0))):
        low, high = picked(x_odd, xa_ref[0, j], xb_ref[0, j])
        out_ref[0] = low
        out_ref[nx + 1] = high
        for k in range(nx):
            out_ref[k + 1] = mid_ref[k, j]


def width_kernel(zl_ref, zh_ref, xa_ref, xb_ref, ya_ref, yb_ref, first_ref, second_ref):
    nz = ya_ref.shape[1]
    x_odd, y_odd, odd = is_odd("gx"), is_odd("gy"), is_odd("gz")

    def face(k, own):
        x_low, x_high = picked(x_odd, xa_ref[0].astype(jnp.float32)[:, k], xb_ref[0].astype(jnp.float32)[:, k])
        y_low, y_high = picked(y_odd, ya_ref[...].astype(jnp.float32)[:, k], yb_ref[...].astype(jnp.float32)[:, k])
        deep = jnp.concatenate([x_low[None], own.astype(jnp.float32), x_high[None]], axis=0)
        return jnp.concatenate([y_low[:, None], deep, y_high[:, None]], axis=1)

    low, high = face(0, zl_ref[...]), face(nz - 1, zh_ref[...])
    first_ref[...] = jnp.where(odd, low, high).astype(jnp.bfloat16)
    second_ref[...] = jnp.where(odd, high, low).astype(jnp.bfloat16)


def filter_kernel(mid_ref, xa_ref, xb_ref, ya_ref, yb_ref, za_ref, zb_ref, in_ref, taps_ref, keep_ref, send_ref):
    nx, ny, nz, ch = mid_ref.shape
    x_odd, y_odd, z_odd = is_odd("gx"), is_odd("gy"), is_odd("gz")

    def fill(k, rows, j, n):
        mid = rows.astype(jnp.float32)
        low, high = picked(z_odd, za_ref[k, j : j + n], zb_ref[k, j : j + n])
        low = low.astype(jnp.float32)[:, None, :]
        high = high.astype(jnp.float32)[:, None, :]
        up = jnp.concatenate([mid[:, 1:], high], axis=1)
        down = jnp.concatenate([low, mid[:, :-1]], axis=1)
        taps_ref[k, j : j + n, :, 0:ch] = up.astype(jnp.bfloat16)
        taps_ref[k, j : j + n, :, ch : 2 * ch] = rows
        taps_ref[k, j : j + n, :, 2 * ch : 3 * ch] = down.astype(jnp.bfloat16)

    def plane(k, carry):
        low, high = picked(y_odd, ya_ref[k], yb_ref[k])
        fill(k, low[None], 0, 1)
        fill(k, high[None], ny + 1, 1)
        return carry

    def middle(k, carry):
        fill(k + 1, mid_ref[k], 1, ny)
        return carry

    lax.fori_loop(0, nx, middle, 0)
    low, high = picked(x_odd, xa_ref[0], xb_ref[0])
    fill(0, low, 1, ny)
    fill(nx + 1, high, 1, ny)
    lax.fori_loop(0, nx + 2, plane, 0)
    cells = nx * ny * nz
    flat = in_ref[...].T
    core = lax.axis_index("gx") % CORES
    for a in range(3):
        for b in range(3):
            view = taps_ref[2 - a : 2 - a + nx, 2 - b : 2 - b + ny].reshape(cells, 3 * ch)
            res = jnp.dot(flat, view, preferred_element_type=jnp.float32)
            lanes = pl.ds((a * 3 + b) * 3 * ch, 3 * ch)
            for g in range(ch // 32):
                first = res[g * 32 : g * 32 + 16]
                second = res[g * 32 + 16 : g * 32 + 32]
                keep_ref[g * 16 : g * 16 + 16, lanes] = jnp.where(core == 0, first, second)
                send_ref[g * 16 : g * 16 + 16, lanes] = jnp.where(core == 0, second, first).astype(jnp.bfloat16)


def pair_kernel(keep_ref, other_ref, out_ref):
    rows = out_ref.shape[1]
    for g in range(keep_ref.shape[0] // 16):
        total = keep_ref[g * 16 : g * 16 + 16] + other_ref[g * 16 : g * 16 + 16].astype(jnp.float32)
        for r in range(16 // rows):
            out_ref[g * (16 // rows) + r] = total[r * rows : (r + 1) * rows].astype(jnp.bfloat16)


def peers_kernel(parts_ref, out_ref):
    total = jnp.sum(parts_ref[...].astype(jnp.float32), axis=0).astype(jnp.bfloat16)
    for k in range(out_ref.shape[0]):
        out_ref[k] = total


def block_kernel(parts_ref, std_ref, grad_ref, sums_ref):
    ch = sums_ref.shape[2] // 3
    total = jnp.sum(parts_ref[...].astype(jnp.float32), axis=0)
    grad_ref[...] = total
    three = jnp.concatenate([fold(total, ch), fold(total * std_ref[...], ch), fold(total * total, ch)], axis=1)
    for k in range(sums_ref.shape[0]):
        sums_ref[k] = three


def input_kernel(taps_ref, std_ref, out_ref):
    nx, ny, nz, ch = out_ref.shape
    planes = 2
    std = std_ref[...]
    for x in range(0, nx, planes):
        rows = jnp.concatenate(
            [
                taps_ref[x + 2 - a : x + 2 - a + planes, 2 - b : 2 - b + ny].reshape(planes * ny * nz, 3 * ch)
                for a in range(3)
                for b in range(3)
            ],
            axis=1,
        )
        res = lax.dot_general(rows, std, (((1,), (1,)), ((), ())), preferred_element_type=jnp.float32)
        out_ref[x : x + planes] = res.astype(jnp.bfloat16).reshape(planes, ny, nz, ch)


def std_kernel(x_count, near_ref, far_ref, std_ref, mean_ref, inv_ref, block_ref):
    slots, rows, held = near_ref.shape
    ch = inv_ref.shape[1]
    width = held - ch
    taps = width // ch
    gx, y, x = lax.axis_index("gx"), lax.axis_index("gy"), lax.axis_index("gz") % x_count
    zl, core = gx // CORES, gx % CORES
    blocks = [(b // 8, (b // 4) % 2, b % 4) for b in range(2 * slots)]
    count = float(2 * slots * rows * taps)

    def parts(zl_b, core_b, y_b):
        slot = (y_b ^ y) + 4 * (zl_b ^ zl)
        data = jnp.where(core_b == core, near_ref[slot], far_ref[slot]).astype(jnp.float32)
        return data[:, :width], data[0:1, width:] + data[1:2, width:]

    total = jnp.zeros((1, ch), jnp.float32)
    for b in blocks:
        values, base = parts(*b)
        total = total + (fold(values, ch) + float(rows * taps) * base)
    mean = total / count
    square = jnp.zeros((1, ch), jnp.float32)
    for b in blocks:
        values, base = parts(*b)
        first = values + wide(base - mean)
        square = square + fold(first * first, ch)
    inv = lax.rsqrt(square / count + var_eps)
    mean_ref[...] = mean
    inv_ref[...] = inv
    inv_wide = wide(inv)
    for n, b in enumerate(blocks):
        values, base = parts(*b)
        std_ref[n * rows : (n + 1) * rows, :] = ((values + wide(base - mean)) * inv_wide).astype(jnp.bfloat16)
    values, base = parts(x, core, y)
    block_ref[...] = (values + wide(base - mean)) * inv_wide


def last_kernel(fan_count, grad_ref, raw_ref, mean_ref, inv_ref, sums_ref, out_ref):
    taps, _, ch = raw_ref.shape
    sums = jnp.sum(sums_ref[...], axis=0)
    sum_grad, sum_cross, sum_square = sums[:, :ch], sums[:, ch : 2 * ch], sums[:, 2 * ch :]
    mean, inv = mean_ref[...], inv_ref[...]
    mean_grad = sum_grad / fan_count
    mean_cross = sum_cross / fan_count
    shrink = 1.0 - var_eps * inv * inv
    per_output = sum_square - 2.0 * mean_grad * sum_grad - 2.0 * mean_cross * sum_cross
    per_output = per_output + fan_count * mean_grad * mean_grad + fan_count * mean_cross * mean_cross * shrink
    square_sum = jnp.sum(inv * inv * per_output, axis=1, keepdims=True)
    scale = jnp.minimum(1.0, clip_norm * lax.rsqrt(square_sum + norm_eps))
    factor = inv * scale
    for t in range(taps):
        std = (raw_ref[t] - mean) * inv
        out_ref[t] = factor * (grad_ref[:, t * ch : (t + 1) * ch] - mean_grad - std * mean_cross)


def on_device(where, raw_weight, inputs, cotangent):
    nx, ny, nz, ch = inputs.shape
    rows, taps = raw_weight.shape[:2]
    width = taps * ch
    bf16, f32 = jnp.bfloat16, jnp.float32
    raw = jnp.transpose(raw_weight, (1, 0, 2))

    def joined(held):
        return jnp.concatenate(held, 0)

    def both(shape):
        return (of(shape, bf16), of(shape, bf16))

    faces = call(faces_kernel, both((1, ny, nz, ch)), (cotangent,))
    x_halo = swapped(*faces, "gx")
    block, *width_faces = call(base_kernel, (of((1, rows, width + ch), bf16), *both((nx, ny, ch))), (raw, cotangent))
    held = [block, where.send(block, lambda s: dict(y=s["y"] ^ 1))]
    faces = call(height_kernel, both((nx + 2, nz, ch)), (cotangent, *x_halo))
    y_halo = swapped(*faces, "gy")
    held.append(where.send(joined(held), lambda s: dict(y=s["y"] ^ 2)))
    faces = call(width_kernel, both((nx + 2, ny + 2, ch)), (*width_faces, *x_halo, *y_halo))
    z_halo = swapped(*faces, "gz")
    held.append(where.send(joined(held), lambda s: dict(zl=s["zl"] ^ 1)))
    held.append(where.send(joined(held), lambda s: dict(zl=s["zl"] ^ 2)))

    flops = 2 * nx * ny * nz * ch * width
    tap_views, keep, send = call(
        filter_kernel,
        (of((nx + 2, ny + 2, nz, 3 * ch), bf16), of((ch // 2, width), f32), of((ch // 2, width), bf16)),
        (cotangent, *x_halo, *y_halo, *z_halo, inputs.reshape(-1, ch)),
        vmem=16,
        flops=2 * flops,
    )
    other = where.send(send, lambda s: dict(core=1 - s["core"]))
    held = call(join_kernel, of((16, rows, width + ch), bf16), held)
    peers = where.x * where.gy
    half = call(pair_kernel, of((peers, rows, width), bf16), (keep, other))
    parts = where.exchange(half, ("core", "zl", "zh"), lambda s: (s["x"], s["y"]))
    far = where.send(held, lambda s: dict(core=1 - s["core"]))
    std_half, mean_out, inv_std, block_std = call(
        functools.partial(std_kernel, where.x),
        (of((ch, width), bf16), of((1, ch), f32), of((1, ch), f32), of((rows, width), f32)),
        (held, far),
        flops=3_000_000_000,
    )
    input_grad = call(input_kernel, of(inputs.shape, bf16), (tap_views, std_half), vmem=16, flops=2 * flops)
    parts, input_grad = lax.optimization_barrier((parts, input_grad))
    copies = call(peers_kernel, of((where.zl * where.zh, rows, width), bf16), (parts,))
    parts = where.exchange(copies, ("core", "x", "y"), lambda s: (s["zh"], s["zl"]))
    everyone = CORES * where.x * where.gy
    block_grad, local = call(block_kernel, (of((rows, width), f32), of((everyone, 1, 3 * ch), f32)), (parts, block_std))
    filter_grad = where.send(block_grad, lambda s: dict(x=s["zl"], zl=s["x"]))
    sums = where.exchange(local, ("zl", "zh"), lambda s: (s["core"], s["x"], s["y"]))

    grad = call(functools.partial(last_kernel, float(ch * taps)), of((taps, rows, ch), f32), (filter_grad, raw, mean_out, inv_std, sums))
    return (input_grad, jnp.transpose(grad, (1, 0, 2)))


def solution(mesh):
    where = Layout(mesh)
    in_specs = (P(("gx", "gy"), None, None), P("gx", "gy", "gz", None), P("gx", "gy", "gz", None))
    out_specs = (P("gx", "gy", "gz", None), P(("gx", "gy"), None, None))

    def body(raw_weight, inputs, cotangent):
        return on_device(where, raw_weight, inputs, cotangent)

    return jax.shard_map(body, mesh=mesh, in_specs=in_specs, out_specs=out_specs, check_vma=False)
```

```python
import functools

import jax
import jax.numpy as jnp
from jax import lax
from jax.experimental import pallas as pl
from jax.experimental.pallas import tpu as pltpu
from jax.sharding import PartitionSpec as P


var_eps = 1e-05
norm_eps = 1e-06
clip_norm = 600.0
AXES = ("gx", "gy", "gz")
CORES = 2
TAPS = 27
MIB = 1024 * 1024


def call(kernel, out_shape, args, vmem=8, flops=1_000_000_000, scratch=()):
    many = isinstance(out_shape, tuple)
    return pl.pallas_call(
        kernel,
        out_shape=out_shape,
        in_specs=[pl.BlockSpec(memory_space=pltpu.VMEM) for _ in args],
        out_specs=tuple(pl.BlockSpec(memory_space=pltpu.VMEM) for _ in out_shape)
        if many
        else pl.BlockSpec(memory_space=pltpu.VMEM),
        scratch_shapes=scratch,
        compiler_params=pltpu.CompilerParams(vmem_limit_bytes=vmem * MIB),
        cost_estimate=pl.CostEstimate(flops=flops, bytes_accessed=1_000_000, transcendentals=0),
    )(*args)


def of(shape, dtype):
    return jax.ShapeDtypeStruct(shape, dtype)


class Layout:
    def __init__(self, mesh):
        self.gx, self.gy, self.gz = (mesh.shape[a] for a in AXES)
        self.zl = self.gx // CORES
        self.x = self.zl
        self.zh = self.gz // self.x

    def spots(self):
        for zl in range(self.zl):
            for core in range(CORES):
                for y in range(self.gy):
                    for zh in range(self.zh):
                        for x in range(self.x):
                            yield dict(zl=zl, core=core, y=y, zh=zh, x=x)

    def index(self, s):
        return ((s["zl"] * CORES + s["core"]) * self.gy + s["y"]) * self.gz + s["zh"] * self.x + s["x"]

    def send(self, array, target):
        pairs = []
        for s in self.spots():
            t = dict(s)
            t.update(target(s))
            pairs.append((self.index(s), self.index(t)))
        return lax.ppermute(array, AXES, pairs)

    def exchange(self, array, fixed, order):
        groups = {}
        for s in self.spots():
            groups.setdefault(tuple(s[k] for k in fixed), []).append((order(s), self.index(s)))
        groups = [[i for _, i in sorted(g)] for g in groups.values()]
        return lax.all_to_all(array, AXES, 0, 0, tiled=True, axis_index_groups=groups)


def swapped(first, second, axis):
    count = lax.axis_size(axis)

    def pairs(start):
        ends = [(i, i + 1) for i in range(start, count - 1, 2)]
        return ends + [(j, i) for i, j in ends]

    return lax.ppermute(first, axis, pairs(0)), lax.ppermute(second, axis, pairs(1))


def is_odd(axis):
    return lax.axis_index(axis) % 2 == 1


def wide(row, taps=TAPS):
    return jnp.concatenate([row] * taps, axis=1)


def fold(values, ch):
    total = values[:, 0:ch]
    for t in range(1, values.shape[1] // ch):
        total = total + values[:, t * ch : (t + 1) * ch]
    return jnp.sum(total, axis=0, keepdims=True)


def faces_kernel(mid_ref, first_ref, second_ref):
    last = mid_ref.shape[0] - 1
    odd = is_odd("gx")
    first_ref[0] = mid_ref[jnp.where(odd, 0, last)]
    second_ref[0] = mid_ref[jnp.where(odd, last, 0)]


def base_kernel(raw_ref, mid_ref, held_ref, zl_ref, zh_ref):
    taps, rows, ch = raw_ref.shape
    base = jnp.sum(jnp.sum(raw_ref[...], axis=0), axis=0, keepdims=True) / (taps * rows)
    high = base.astype(jnp.bfloat16)
    low = (base - high.astype(jnp.float32)).astype(jnp.bfloat16)
    base = high.astype(jnp.float32) + low.astype(jnp.float32)
    for t in range(taps):
        held_ref[0, :, t * ch : (t + 1) * ch] = (raw_ref[t] - base).astype(jnp.bfloat16)
    place = lax.broadcasted_iota(jnp.int32, (rows, ch), 0)
    both = jnp.where(place == 0, high.astype(jnp.float32), low.astype(jnp.float32))
    held_ref[0, :, taps * ch :] = both.astype(jnp.bfloat16)
    nz = mid_ref.shape[2]
    for k in range(mid_ref.shape[0]):
        mid = mid_ref[k].astype(jnp.float32)
        zl_ref[k] = mid[:, 0].astype(jnp.bfloat16)
        zh_ref[k] = mid[:, nz - 1].astype(jnp.bfloat16)


def join_kernel(*refs):
    place = 0
    for piece in refs[:-1]:
        refs[-1][place : place + piece.shape[0]] = piece[...]
        place += piece.shape[0]


def picked(odd, first, second):
    return jnp.where(odd, first, second), jnp.where(odd, second, first)


def height_kernel(mid_ref, xa_ref, xb_ref, first_ref, second_ref):
    nx, ny = mid_ref.shape[:2]
    x_odd, odd = is_odd("gx"), is_odd("gy")
    for out_ref, j in ((first_ref, jnp.where(odd, 0, ny - 1)), (second_ref, jnp.where(odd, ny - 1, 0))):
        low, high = picked(x_odd, xa_ref[0, j], xb_ref[0, j])
        out_ref[0] = low
        out_ref[nx + 1] = high
        for k in range(nx):
            out_ref[k + 1] = mid_ref[k, j]


def width_kernel(zl_ref, zh_ref, xa_ref, xb_ref, ya_ref, yb_ref, first_ref, second_ref):
    nz = ya_ref.shape[1]
    x_odd, y_odd, odd = is_odd("gx"), is_odd("gy"), is_odd("gz")

    def face(k, own):
        x_low, x_high = picked(x_odd, xa_ref[0].astype(jnp.float32)[:, k], xb_ref[0].astype(jnp.float32)[:, k])
        y_low, y_high = picked(y_odd, ya_ref[...].astype(jnp.float32)[:, k], yb_ref[...].astype(jnp.float32)[:, k])
        deep = jnp.concatenate([x_low[None], own.astype(jnp.float32), x_high[None]], axis=0)
        return jnp.concatenate([y_low[:, None], deep, y_high[:, None]], axis=1)

    low, high = face(0, zl_ref[...]), face(nz - 1, zh_ref[...])
    first_ref[...] = jnp.where(odd, low, high).astype(jnp.bfloat16)
    second_ref[...] = jnp.where(odd, high, low).astype(jnp.bfloat16)


def fill_taps(taps_ref, mid_ref, xa_ref, xb_ref, ya_ref, yb_ref, z_halo):
    nx, ny, _, ch = mid_ref.shape
    x_odd, y_odd, z_odd = is_odd("gx"), is_odd("gy"), is_odd("gz")

    def fill(k, rows, j, n):
        mid = rows.astype(jnp.float32)
        if z_halo:
            low, high = picked(z_odd, z_halo[0][k, j : j + n], z_halo[1][k, j : j + n])
            low = low.astype(jnp.float32)[:, None, :]
            high = high.astype(jnp.float32)[:, None, :]
        else:
            low = high = jnp.zeros((n, 1, ch), jnp.float32)
        up = jnp.concatenate([mid[:, 1:], high], axis=1)
        down = jnp.concatenate([low, mid[:, :-1]], axis=1)
        taps_ref[k, j : j + n, :, 0:ch] = up.astype(jnp.bfloat16)
        taps_ref[k, j : j + n, :, ch : 2 * ch] = rows
        taps_ref[k, j : j + n, :, 2 * ch : 3 * ch] = down.astype(jnp.bfloat16)

    def plane(k, carry):
        low, high = picked(y_odd, ya_ref[k], yb_ref[k])
        fill(k, low[None], 0, 1)
        fill(k, high[None], ny + 1, 1)
        return carry

    def middle(k, carry):
        fill(k + 1, mid_ref[k], 1, ny)
        return carry

    lax.fori_loop(0, nx, middle, 0)
    low, high = picked(x_odd, xa_ref[0], xb_ref[0])
    fill(0, low, 1, ny)
    fill(nx + 1, high, 1, ny)
    lax.fori_loop(0, nx + 2, plane, 0)


def filter_kernel(mid_ref, xa_ref, xb_ref, ya_ref, yb_ref, in_ref, total_ref, first_ref, last_ref, taps_ref):
    nx, ny, nz, ch = mid_ref.shape
    fill_taps(taps_ref, mid_ref, xa_ref, xb_ref, ya_ref, yb_ref, None)
    cells = nx * ny * nz
    flat = in_ref[...].reshape(cells, ch).T
    for a in range(3):
        for b in range(3):
            view = taps_ref[2 - a : 2 - a + nx, 2 - b : 2 - b + ny].reshape(cells, 3 * ch)
            lanes = pl.ds((a * 3 + b) * 3 * ch, 3 * ch)
            total_ref[:, lanes] = jnp.dot(flat, view, preferred_element_type=jnp.float32)
    for out_ref, j in ((first_ref, 0), (last_ref, nz - 1)):
        ends = [in_ref[k].astype(jnp.float32)[:, j] for k in range(nx)]
        out_ref[...] = jnp.concatenate(ends, axis=0).T.astype(jnp.bfloat16)


def finish_kernel(total_ref, first_ref, last_ref, za_ref, zb_ref, keep_ref, send_ref):
    ch = total_ref.shape[0]
    nx, ny = za_ref.shape[0] - 2, za_ref.shape[1] - 2
    core = lax.axis_index("gx") % CORES
    low, high = picked(is_odd("gz"), za_ref[...].astype(jnp.float32), zb_ref[...].astype(jnp.float32))

    def shifted(face):
        return jnp.concatenate([face[:, 2 - b : 2 - b + ny] for b in range(3)], axis=2).astype(jnp.bfloat16)

    low, high = shifted(low), shifted(high)
    for a in range(3):
        rows = slice(2 - a, 2 - a + nx)
        above = jnp.dot(last_ref[...], high[rows].reshape(nx * ny, 3 * ch), preferred_element_type=jnp.float32)
        below = jnp.dot(first_ref[...], low[rows].reshape(nx * ny, 3 * ch), preferred_element_type=jnp.float32)
        for b in range(3):
            for c in range(3):
                lanes = pl.ds(((a * 3 + b) * 3 + c) * ch, ch)
                res = total_ref[:, lanes]
                if c == 0:
                    res = res + above[:, b * ch : (b + 1) * ch]
                if c == 2:
                    res = res + below[:, b * ch : (b + 1) * ch]
                for g in range(ch // 32):
                    first = res[g * 32 : g * 32 + 16]
                    second = res[g * 32 + 16 : g * 32 + 32]
                    keep_ref[g * 16 : g * 16 + 16, lanes] = jnp.where(core == 0, first, second)
                    other = jnp.where(core == 0, second, first)
                    send_ref[g * 16 : g * 16 + 16, lanes] = other.astype(jnp.bfloat16)


def pair_kernel(keep_ref, other_ref, out_ref):
    rows = out_ref.shape[1]
    for g in range(keep_ref.shape[0] // 16):
        total = keep_ref[g * 16 : g * 16 + 16] + other_ref[g * 16 : g * 16 + 16].astype(jnp.float32)
        for r in range(16 // rows):
            out_ref[g * (16 // rows) + r] = total[r * rows : (r + 1) * rows].astype(jnp.bfloat16)


def peers_kernel(parts_ref, out_ref):
    total = jnp.sum(parts_ref[...].astype(jnp.float32), axis=0).astype(jnp.bfloat16)
    for k in range(out_ref.shape[0]):
        out_ref[k] = total


def block_kernel(parts_ref, std_ref, grad_ref, sums_ref):
    ch = sums_ref.shape[2] // 3
    total = jnp.sum(parts_ref[...].astype(jnp.float32), axis=0)
    grad_ref[...] = total
    three = jnp.concatenate([fold(total, ch), fold(total * std_ref[...], ch), fold(total * total, ch)], axis=1)
    for k in range(sums_ref.shape[0]):
        sums_ref[k] = three


def input_kernel(mid_ref, xa_ref, xb_ref, ya_ref, yb_ref, za_ref, zb_ref, std_ref, out_ref, taps_ref):
    nx, ny, nz, ch = out_ref.shape
    fill_taps(taps_ref, mid_ref, xa_ref, xb_ref, ya_ref, yb_ref, (za_ref, zb_ref))
    planes = 2
    std = std_ref[...]
    for x in range(0, nx, planes):
        rows = jnp.concatenate(
            [
                taps_ref[x + 2 - a : x + 2 - a + planes, 2 - b : 2 - b + ny].reshape(planes * ny * nz, 3 * ch)
                for a in range(3)
                for b in range(3)
            ],
            axis=1,
        )
        res = lax.dot_general(rows, std, (((1,), (1,)), ((), ())), preferred_element_type=jnp.float32)
        out_ref[x : x + planes] = res.astype(jnp.bfloat16).reshape(planes, ny, nz, ch)


def std_kernel(x_count, near_ref, far_ref, std_ref, mean_ref, inv_ref, block_ref):
    slots, rows, held = near_ref.shape
    ch = inv_ref.shape[1]
    width = held - ch
    taps = width // ch
    gx, y, x = lax.axis_index("gx"), lax.axis_index("gy"), lax.axis_index("gz") % x_count
    zl, core = gx // CORES, gx % CORES
    blocks = [(b // 8, (b // 4) % 2, b % 4) for b in range(2 * slots)]
    count = float(2 * slots * rows * taps)

    def parts(zl_b, core_b, y_b):
        slot = (y_b ^ y) + 4 * (zl_b ^ zl)
        data = jnp.where(core_b == core, near_ref[slot], far_ref[slot]).astype(jnp.float32)
        return data[:, :width], data[0:1, width:] + data[1:2, width:]

    total = jnp.zeros((1, ch), jnp.float32)
    for b in blocks:
        values, base = parts(*b)
        total = total + (fold(values, ch) + float(rows * taps) * base)
    mean = total / count
    square = jnp.zeros((1, ch), jnp.float32)
    for b in blocks:
        values, base = parts(*b)
        first = values + wide(base - mean)
        square = square + fold(first * first, ch)
    inv = lax.rsqrt(square / count + var_eps)
    mean_ref[...] = mean
    inv_ref[...] = inv
    inv_wide = wide(inv)
    for n, b in enumerate(blocks):
        values, base = parts(*b)
        std_ref[n * rows : (n + 1) * rows, :] = ((values + wide(base - mean)) * inv_wide).astype(jnp.bfloat16)
    values, base = parts(x, core, y)
    block_ref[...] = (values + wide(base - mean)) * inv_wide


def last_kernel(fan_count, grad_ref, raw_ref, mean_ref, inv_ref, sums_ref, out_ref):
    taps, _, ch = raw_ref.shape
    sums = jnp.sum(sums_ref[...], axis=0)
    sum_grad, sum_cross, sum_square = sums[:, :ch], sums[:, ch : 2 * ch], sums[:, 2 * ch :]
    mean, inv = mean_ref[...], inv_ref[...]
    mean_grad = sum_grad / fan_count
    mean_cross = sum_cross / fan_count
    shrink = 1.0 - var_eps * inv * inv
    per_output = sum_square - 2.0 * mean_grad * sum_grad - 2.0 * mean_cross * sum_cross
    per_output = per_output + fan_count * mean_grad * mean_grad + fan_count * mean_cross * mean_cross * shrink
    square_sum = jnp.sum(inv * inv * per_output, axis=1, keepdims=True)
    scale = jnp.minimum(1.0, clip_norm * lax.rsqrt(square_sum + norm_eps))
    factor = inv * scale
    for t in range(taps):
        std = (raw_ref[t] - mean) * inv
        out_ref[t] = factor * (grad_ref[:, t * ch : (t + 1) * ch] - mean_grad - std * mean_cross)


def on_device(where, raw_weight, inputs, cotangent):
    nx, ny, nz, ch = inputs.shape
    rows, taps = raw_weight.shape[:2]
    width = taps * ch
    bf16, f32 = jnp.bfloat16, jnp.float32
    raw = jnp.transpose(raw_weight, (1, 0, 2))

    def joined(held):
        return jnp.concatenate(held, 0)

    def both(shape):
        return (of(shape, bf16), of(shape, bf16))

    faces = call(faces_kernel, both((1, ny, nz, ch)), (cotangent,))
    x_halo = swapped(*faces, "gx")
    block, *width_faces = call(base_kernel, (of((1, rows, width + ch), bf16), *both((nx, ny, ch))), (raw, cotangent))
    held = [block, where.send(block, lambda s: dict(y=s["y"] ^ 1))]
    faces = call(height_kernel, both((nx + 2, nz, ch)), (cotangent, *x_halo))
    y_halo = swapped(*faces, "gy")
    held.append(where.send(joined(held), lambda s: dict(y=s["y"] ^ 2)))
    faces = call(width_kernel, both((nx + 2, ny + 2, ch)), (*width_faces, *x_halo, *y_halo))
    z_halo = swapped(*faces, "gz")
    held.append(where.send(joined(held), lambda s: dict(zl=s["zl"] ^ 1)))
    held.append(where.send(joined(held), lambda s: dict(zl=s["zl"] ^ 2)))

    flops = 2 * nx * ny * nz * ch * width
    scratch = [pltpu.VMEM((nx + 2, ny + 2, nz, 3 * ch), bf16)]
    total, *ends = call(
        filter_kernel,
        (of((ch, width), f32), of((ch, nx * ny), bf16), of((ch, nx * ny), bf16)),
        (cotangent, *x_halo, *y_halo, inputs),
        vmem=16,
        flops=2 * flops,
        scratch=scratch,
    )
    keep, send = call(finish_kernel, (of((ch // 2, width), f32), of((ch // 2, width), bf16)), (total, *ends, *z_halo))
    other = where.send(send, lambda s: dict(core=1 - s["core"]))
    held = call(join_kernel, of((16, rows, width + ch), bf16), held)
    peers = where.x * where.gy
    half = call(pair_kernel, of((peers, rows, width), bf16), (keep, other))
    parts = where.exchange(half, ("core", "zl", "zh"), lambda s: (s["x"], s["y"]))
    far = where.send(held, lambda s: dict(core=1 - s["core"]))
    std_half, mean_out, inv_std, block_std = call(
        functools.partial(std_kernel, where.x),
        (of((ch, width), bf16), of((1, ch), f32), of((1, ch), f32), of((rows, width), f32)),
        (held, far),
        flops=3_000_000_000,
    )
    parts, inv_std = lax.optimization_barrier((parts, inv_std))
    copies = call(peers_kernel, of((where.zl * where.zh, rows, width), bf16), (parts,))
    parts = where.exchange(copies, ("core", "x", "y"), lambda s: (s["zh"], s["zl"]))
    input_grad = call(
        input_kernel,
        of(inputs.shape, bf16),
        (cotangent, *x_halo, *y_halo, *z_halo, std_half),
        vmem=16,
        flops=2 * flops,
        scratch=scratch,
    )
    parts, input_grad = lax.optimization_barrier((parts, input_grad))
    everyone = CORES * where.x * where.gy
    block_grad, local = call(block_kernel, (of((rows, width), f32), of((everyone, 1, 3 * ch), f32)), (parts, block_std))
    filter_grad = where.send(block_grad, lambda s: dict(x=s["zl"], zl=s["x"]))
    sums = where.exchange(local, ("zl", "zh"), lambda s: (s["core"], s["x"], s["y"]))

    grad = call(functools.partial(last_kernel, float(ch * taps)), of((taps, rows, ch), f32), (filter_grad, raw, mean_out, inv_std, sums))
    return (input_grad, jnp.transpose(grad, (1, 0, 2)))


def solution(mesh):
    where = Layout(mesh)
    in_specs = (P(("gx", "gy"), None, None), P("gx", "gy", "gz", None), P("gx", "gy", "gz", None))
    out_specs = (P("gx", "gy", "gz", None), P(("gx", "gy"), None, None))

    def body(raw_weight, inputs, cotangent):
        return on_device(where, raw_weight, inputs, cotangent)

    return jax.shard_map(body, mesh=mesh, in_specs=in_specs, out_specs=out_specs, check_vma=False)
```

```python
import functools

import jax
import jax.numpy as jnp
from jax import lax
from jax.experimental import pallas as pl
from jax.experimental.pallas import tpu as pltpu
from jax.sharding import PartitionSpec as P


var_eps = 1e-05
norm_eps = 1e-06
clip_norm = 600.0
AXES = ("gx", "gy", "gz")
CORES = 2
TAPS = 27
MIB = 1024 * 1024


def call(kernel, out_shape, args, vmem=8, flops=1_000_000_000, scratch=()):
    many = isinstance(out_shape, tuple)
    return pl.pallas_call(
        kernel,
        out_shape=out_shape,
        in_specs=[pl.BlockSpec(memory_space=pltpu.VMEM) for _ in args],
        out_specs=tuple(pl.BlockSpec(memory_space=pltpu.VMEM) for _ in out_shape)
        if many
        else pl.BlockSpec(memory_space=pltpu.VMEM),
        scratch_shapes=scratch,
        compiler_params=pltpu.CompilerParams(vmem_limit_bytes=vmem * MIB),
        cost_estimate=pl.CostEstimate(flops=flops, bytes_accessed=1_000_000, transcendentals=0),
    )(*args)


def of(shape, dtype):
    return jax.ShapeDtypeStruct(shape, dtype)


class Layout:
    def __init__(self, mesh):
        self.gx, self.gy, self.gz = (mesh.shape[a] for a in AXES)
        self.zl = self.gx // CORES
        self.x = self.zl
        self.zh = self.gz // self.x

    def spots(self):
        for zl in range(self.zl):
            for core in range(CORES):
                for y in range(self.gy):
                    for zh in range(self.zh):
                        for x in range(self.x):
                            yield dict(zl=zl, core=core, y=y, zh=zh, x=x)

    def index(self, s):
        return ((s["zl"] * CORES + s["core"]) * self.gy + s["y"]) * self.gz + s["zh"] * self.x + s["x"]

    def send(self, array, target):
        pairs = []
        for s in self.spots():
            t = dict(s)
            t.update(target(s))
            pairs.append((self.index(s), self.index(t)))
        return lax.ppermute(array, AXES, pairs)

    def exchange(self, array, fixed, order):
        groups = {}
        for s in self.spots():
            groups.setdefault(tuple(s[k] for k in fixed), []).append((order(s), self.index(s)))
        groups = [[i for _, i in sorted(g)] for g in groups.values()]
        return lax.all_to_all(array, AXES, 0, 0, tiled=True, axis_index_groups=groups)


def swapped(first, second, axis):
    count = lax.axis_size(axis)

    def pairs(start):
        ends = [(i, i + 1) for i in range(start, count - 1, 2)]
        return ends + [(j, i) for i, j in ends]

    return lax.ppermute(first, axis, pairs(0)), lax.ppermute(second, axis, pairs(1))


def is_odd(axis):
    return lax.axis_index(axis) % 2 == 1


def wide(row, taps=TAPS):
    return jnp.concatenate([row] * taps, axis=1)


def fold(values, ch):
    total = values[:, 0:ch]
    for t in range(1, values.shape[1] // ch):
        total = total + values[:, t * ch : (t + 1) * ch]
    return jnp.sum(total, axis=0, keepdims=True)


def faces_kernel(mid_ref, first_ref, second_ref):
    last = mid_ref.shape[0] - 1
    odd = is_odd("gx")
    first_ref[0] = mid_ref[jnp.where(odd, 0, last)]
    second_ref[0] = mid_ref[jnp.where(odd, last, 0)]


def base_kernel(raw_ref, mid_ref, in_ref, held_ref, zl_ref, zh_ref, il_ref, ih_ref):
    taps, rows, ch = raw_ref.shape
    base = jnp.sum(jnp.sum(raw_ref[...], axis=0), axis=0, keepdims=True) / (taps * rows)
    high = base.astype(jnp.bfloat16)
    low = (base - high.astype(jnp.float32)).astype(jnp.bfloat16)
    base = high.astype(jnp.float32) + low.astype(jnp.float32)
    for t in range(taps):
        held_ref[0, :, t * ch : (t + 1) * ch] = (raw_ref[t] - base).astype(jnp.bfloat16)
    place = lax.broadcasted_iota(jnp.int32, (rows, ch), 0)
    both = jnp.where(place == 0, high.astype(jnp.float32), low.astype(jnp.float32))
    held_ref[0, :, taps * ch :] = both.astype(jnp.bfloat16)
    for whole_ref, first_ref, last_ref in ((mid_ref, zl_ref, zh_ref), (in_ref, il_ref, ih_ref)):
        for k in range(whole_ref.shape[0]):
            whole = whole_ref[k].astype(jnp.float32)
            first_ref[k] = whole[:, 0].astype(jnp.bfloat16)
            last_ref[k] = whole[:, -1].astype(jnp.bfloat16)


def join_kernel(*refs):
    place = 0
    for piece in refs[:-1]:
        refs[-1][place : place + piece.shape[0]] = piece[...]
        place += piece.shape[0]


def picked(odd, first, second):
    return jnp.where(odd, first, second), jnp.where(odd, second, first)


def height_kernel(mid_ref, xa_ref, xb_ref, il_ref, ih_ref, first_ref, second_ref):
    nx, ny, nz, ch = mid_ref.shape
    x_odd, odd = is_odd("gx"), is_odd("gy")
    first, last = il_ref[...].astype(jnp.float32), ih_ref[...].astype(jnp.float32)
    ends = [jnp.concatenate([first[:, None, j], last[:, None, j]], axis=1) for j in (0, ny - 1)]
    ends = [e.astype(jnp.bfloat16) for e in ends]
    outs = ((first_ref, jnp.where(odd, 0, ny - 1)), (second_ref, jnp.where(odd, ny - 1, 0)))
    for (out_ref, j), end in zip(outs, (picked(odd, *ends))):
        low, high = picked(x_odd, xa_ref[0, j], xb_ref[0, j])
        out_ref[0, :nz] = low
        out_ref[nx + 1, :nz] = high
        for k in (0, nx + 1):
            out_ref[k, nz:] = jnp.zeros((2, ch), jnp.bfloat16)
        for k in range(nx):
            out_ref[k + 1, :nz] = mid_ref[k, j]
        out_ref[1 : nx + 1, nz:] = end


def width_kernel(zl_ref, zh_ref, xa_ref, xb_ref, first_ref, second_ref):
    nx = zl_ref.shape[0]
    nz = xa_ref.shape[2]
    x_odd, odd = is_odd("gx"), is_odd("gz")
    low, high = picked(odd, zl_ref[...], zh_ref[...])
    first_ref[1 : nx + 1] = low
    second_ref[1 : nx + 1] = high
    below, above = picked(x_odd, xa_ref[0].astype(jnp.float32), xb_ref[0].astype(jnp.float32))
    for k, face in ((0, below), (nx + 1, above)):
        low, high = picked(odd, face[:, 0], face[:, nz - 1])
        first_ref[k] = low.astype(jnp.bfloat16)
        second_ref[k] = high.astype(jnp.bfloat16)


def corner_kernel(za_ref, zb_ref, first_ref, second_ref):
    ny = za_ref.shape[1]
    odd = is_odd("gy")
    low, high = picked(is_odd("gz"), za_ref[...].astype(jnp.float32), zb_ref[...].astype(jnp.float32))
    ends = [jnp.concatenate([low[:, None, j], high[:, None, j]], axis=1) for j in (0, ny - 1)]
    first, second = picked(odd, *ends)
    first_ref[...] = first.astype(jnp.bfloat16)
    second_ref[...] = second.astype(jnp.bfloat16)


def fill_taps(taps_ref, mid_ref, xa_ref, xb_ref, ya_ref, yb_ref, z_halo):
    nx, ny, nz, ch = mid_ref.shape
    x_odd, y_odd, z_odd = is_odd("gx"), is_odd("gy"), is_odd("gz")

    def fill(k, j, rows, low, high):
        n = rows.shape[0]
        mid = rows.astype(jnp.float32)
        up = jnp.concatenate([mid[:, 1:], high], axis=1)
        down = jnp.concatenate([low, mid[:, :-1]], axis=1)
        taps_ref[k, j : j + n, :, 0:ch] = up.astype(jnp.bfloat16)
        taps_ref[k, j : j + n, :, ch : 2 * ch] = rows
        taps_ref[k, j : j + n, :, 2 * ch : 3 * ch] = down.astype(jnp.bfloat16)

    def fill_rows(k, rows):
        if z_halo:
            low, high = picked(z_odd, z_halo[0][k].astype(jnp.float32), z_halo[1][k].astype(jnp.float32))
            fill(k, 1, rows, low[:, None], high[:, None])
        else:
            none = jnp.zeros((ny, 1, ch), jnp.float32)
            fill(k, 1, rows, none, none)

    def plane(k, carry):
        pairs = zip((0, ny + 1), picked(y_odd, ya_ref[k, :nz], yb_ref[k, :nz]))
        if z_halo:
            corners = picked(y_odd, z_halo[2][k].astype(jnp.float32), z_halo[3][k].astype(jnp.float32))
            for (j, row), corner in zip(pairs, corners):
                fill(k, j, row[None], corner[None, 0:1], corner[None, 1:2])
        else:
            none = jnp.zeros((1, 1, ch), jnp.float32)
            for j, row in pairs:
                fill(k, j, row[None], none, none)
        return carry

    def middle(k, carry):
        fill_rows(k + 1, mid_ref[k])
        return carry

    lax.fori_loop(0, nx, middle, 0)
    low, high = picked(x_odd, xa_ref[0], xb_ref[0])
    fill_rows(0, low)
    fill_rows(nx + 1, high)
    lax.fori_loop(0, nx + 2, plane, 0)


def filter_kernel(mid_ref, xa_ref, xb_ref, ya_ref, yb_ref, in_ref, il_ref, ih_ref, total_ref, ends_ref, taps_ref):
    nx, ny, nz, ch = mid_ref.shape
    fill_taps(taps_ref, mid_ref, xa_ref, xb_ref, ya_ref, yb_ref, None)
    cells = nx * ny * nz
    flat = in_ref[...].reshape(cells, ch).T
    for a in range(3):
        for b in range(3):
            view = taps_ref[2 - a : 2 - a + nx, 2 - b : 2 - b + ny].reshape(cells, 3 * ch)
            lanes = pl.ds((a * 3 + b) * 3 * ch, 3 * ch)
            total_ref[:, lanes] = jnp.dot(flat, view, preferred_element_type=jnp.float32)
    below, above = picked(is_odd("gy"), ya_ref[1 : nx + 1, nz:], yb_ref[1 : nx + 1, nz:])
    below, above = below.astype(jnp.float32), above.astype(jnp.float32)
    for side, own_ref in enumerate((il_ref, ih_ref)):
        own = own_ref[...].astype(jnp.float32)
        face = jnp.concatenate([below[:, side : side + 1], own, above[:, side : side + 1]], axis=1)
        for b in range(3):
            ends_ref[side, b] = face[:, b : b + ny].reshape(nx * ny, ch).T.astype(jnp.bfloat16)


def finish_kernel(total_ref, ends_ref, za_ref, zb_ref, keep_ref, send_ref):
    ch = total_ref.shape[0]
    nx, ny = za_ref.shape[0] - 2, za_ref.shape[1]
    core = lax.axis_index("gx") % CORES
    crossing = []
    for halo in picked(is_odd("gz"), za_ref[...], zb_ref[...]):
        crossing.append(
            jnp.concatenate([halo[2 - a : 2 - a + nx].reshape(nx * ny, ch) for a in range(3)], axis=1)
        )
    for b in range(3):
        below = jnp.dot(ends_ref[0, b], crossing[0], preferred_element_type=jnp.float32)
        above = jnp.dot(ends_ref[1, b], crossing[1], preferred_element_type=jnp.float32)
        for a in range(3):
            for c in range(3):
                lanes = pl.ds(((a * 3 + b) * 3 + c) * ch, ch)
                res = total_ref[:, lanes]
                if c == 0:
                    res = res + above[:, a * ch : (a + 1) * ch]
                if c == 2:
                    res = res + below[:, a * ch : (a + 1) * ch]
                for g in range(ch // 32):
                    first = res[g * 32 : g * 32 + 16]
                    second = res[g * 32 + 16 : g * 32 + 32]
                    keep_ref[g * 16 : g * 16 + 16, lanes] = jnp.where(core == 0, first, second)
                    other = jnp.where(core == 0, second, first)
                    send_ref[g * 16 : g * 16 + 16, lanes] = other.astype(jnp.bfloat16)


def pair_kernel(keep_ref, other_ref, out_ref):
    rows = out_ref.shape[1]
    for g in range(keep_ref.shape[0] // 16):
        total = keep_ref[g * 16 : g * 16 + 16] + other_ref[g * 16 : g * 16 + 16].astype(jnp.float32)
        for r in range(16 // rows):
            out_ref[g * (16 // rows) + r] = total[r * rows : (r + 1) * rows].astype(jnp.bfloat16)


def peers_kernel(parts_ref, out_ref):
    total = jnp.sum(parts_ref[...].astype(jnp.float32), axis=0).astype(jnp.bfloat16)
    for k in range(out_ref.shape[0]):
        out_ref[k] = total


def block_kernel(parts_ref, std_ref, grad_ref, sums_ref):
    ch = sums_ref.shape[2] // 3
    total = jnp.sum(parts_ref[...].astype(jnp.float32), axis=0)
    grad_ref[...] = total
    three = jnp.concatenate([fold(total, ch), fold(total * std_ref[...], ch), fold(total * total, ch)], axis=1)
    for k in range(sums_ref.shape[0]):
        sums_ref[k] = three


def input_kernel(mid_ref, xa_ref, xb_ref, ya_ref, yb_ref, za_ref, zb_ref, ca_ref, cb_ref, std_ref, out_ref, taps_ref):
    nx, ny, nz, ch = out_ref.shape
    fill_taps(taps_ref, mid_ref, xa_ref, xb_ref, ya_ref, yb_ref, (za_ref, zb_ref, ca_ref, cb_ref))
    planes = 2
    std = std_ref[...]
    for x in range(0, nx, planes):
        rows = jnp.concatenate(
            [
                taps_ref[x + 2 - a : x + 2 - a + planes, 2 - b : 2 - b + ny].reshape(planes * ny * nz, 3 * ch)
                for a in range(3)
                for b in range(3)
            ],
            axis=1,
        )
        res = lax.dot_general(rows, std, (((1,), (1,)), ((), ())), preferred_element_type=jnp.float32)
        out_ref[x : x + planes] = res.astype(jnp.bfloat16).reshape(planes, ny, nz, ch)


def std_kernel(x_count, near_ref, far_ref, std_ref, mean_ref, inv_ref, block_ref):
    slots, rows, held = near_ref.shape
    ch = inv_ref.shape[1]
    width = held - ch
    taps = width // ch
    gx, y, x = lax.axis_index("gx"), lax.axis_index("gy"), lax.axis_index("gz") % x_count
    zl, core = gx // CORES, gx % CORES
    blocks = [(b // 8, (b // 4) % 2, b % 4) for b in range(2 * slots)]
    count = float(2 * slots * rows * taps)

    def parts(zl_b, core_b, y_b):
        slot = (y_b ^ y) + 4 * (zl_b ^ zl)
        data = jnp.where(core_b == core, near_ref[slot], far_ref[slot]).astype(jnp.float32)
        return data[:, :width], data[0:1, width:] + data[1:2, width:]

    total = jnp.zeros((1, ch), jnp.float32)
    for b in blocks:
        values, base = parts(*b)
        total = total + (fold(values, ch) + float(rows * taps) * base)
    mean = total / count
    square = jnp.zeros((1, ch), jnp.float32)
    for b in blocks:
        values, base = parts(*b)
        first = values + wide(base - mean)
        square = square + fold(first * first, ch)
    inv = lax.rsqrt(square / count + var_eps)
    mean_ref[...] = mean
    inv_ref[...] = inv
    inv_wide = wide(inv)
    for n, b in enumerate(blocks):
        values, base = parts(*b)
        std_ref[n * rows : (n + 1) * rows, :] = ((values + wide(base - mean)) * inv_wide).astype(jnp.bfloat16)
    values, base = parts(x, core, y)
    block_ref[...] = (values + wide(base - mean)) * inv_wide


def last_kernel(fan_count, grad_ref, raw_ref, mean_ref, inv_ref, sums_ref, out_ref):
    taps, _, ch = raw_ref.shape
    sums = jnp.sum(sums_ref[...], axis=0)
    sum_grad, sum_cross, sum_square = sums[:, :ch], sums[:, ch : 2 * ch], sums[:, 2 * ch :]
    mean, inv = mean_ref[...], inv_ref[...]
    mean_grad = sum_grad / fan_count
    mean_cross = sum_cross / fan_count
    shrink = 1.0 - var_eps * inv * inv
    per_output = sum_square - 2.0 * mean_grad * sum_grad - 2.0 * mean_cross * sum_cross
    per_output = per_output + fan_count * mean_grad * mean_grad + fan_count * mean_cross * mean_cross * shrink
    square_sum = jnp.sum(inv * inv * per_output, axis=1, keepdims=True)
    scale = jnp.minimum(1.0, clip_norm * lax.rsqrt(square_sum + norm_eps))
    factor = inv * scale
    for t in range(taps):
        std = (raw_ref[t] - mean) * inv
        out_ref[t] = factor * (grad_ref[:, t * ch : (t + 1) * ch] - mean_grad - std * mean_cross)


def on_device(where, raw_weight, inputs, cotangent):
    nx, ny, nz, ch = inputs.shape
    rows, taps = raw_weight.shape[:2]
    width = taps * ch
    bf16, f32 = jnp.bfloat16, jnp.float32
    raw = jnp.transpose(raw_weight, (1, 0, 2))

    def joined(held):
        return jnp.concatenate(held, 0)

    def both(shape):
        return (of(shape, bf16), of(shape, bf16))

    faces = call(faces_kernel, both((1, ny, nz, ch)), (cotangent,))
    x_halo = swapped(*faces, "gx")
    block, *ends = call(
        base_kernel,
        (of((1, rows, width + ch), bf16), *both((nx, ny, ch)), *both((nx, ny, ch))),
        (raw, cotangent, inputs),
    )
    held = [block, where.send(block, lambda s: dict(y=s["y"] ^ 1))]
    faces = call(height_kernel, both((nx + 2, nz + 2, ch)), (cotangent, *x_halo, *ends[2:]))
    y_halo = swapped(*faces, "gy")
    faces = call(width_kernel, both((nx + 2, ny, ch)), (*ends[:2], *x_halo))
    z_halo = swapped(*faces, "gz")
    held.append(where.send(joined(held), lambda s: dict(y=s["y"] ^ 2)))
    held.append(where.send(joined(held), lambda s: dict(zl=s["zl"] ^ 1)))
    held.append(where.send(joined(held), lambda s: dict(zl=s["zl"] ^ 2)))

    flops = 2 * nx * ny * nz * ch * width
    scratch = [pltpu.VMEM((nx + 2, ny + 2, nz, 3 * ch), bf16)]
    total, end_rows = call(
        filter_kernel,
        (of((ch, width), f32), of((2, 3, ch, nx * ny), bf16)),
        (cotangent, *x_halo, *y_halo, inputs, *ends[2:]),
        vmem=16,
        flops=2 * flops,
        scratch=scratch,
    )
    keep, send = call(
        finish_kernel, (of((ch // 2, width), f32), of((ch // 2, width), bf16)), (total, end_rows, *z_halo)
    )
    other = where.send(send, lambda s: dict(core=1 - s["core"]))
    held = call(join_kernel, of((16, rows, width + ch), bf16), held)
    peers = where.x * where.gy
    half = call(pair_kernel, of((peers, rows, width), bf16), (keep, other))
    parts = where.exchange(half, ("core", "zl", "zh"), lambda s: (s["x"], s["y"]))
    far = where.send(held, lambda s: dict(core=1 - s["core"]))
    corners = swapped(*call(corner_kernel, both((nx + 2, 2, ch)), z_halo), "gy")
    std_half, mean_out, inv_std, block_std = call(
        functools.partial(std_kernel, where.x),
        (of((ch, width), bf16), of((1, ch), f32), of((1, ch), f32), of((rows, width), f32)),
        (held, far),
        flops=3_000_000_000,
    )
    parts, inv_std = lax.optimization_barrier((parts, inv_std))
    copies = call(peers_kernel, of((where.zl * where.zh, rows, width), bf16), (parts,))
    parts = where.exchange(copies, ("core", "x", "y"), lambda s: (s["zh"], s["zl"]))
    input_grad = call(
        input_kernel,
        of(inputs.shape, bf16),
        (cotangent, *x_halo, *y_halo, *z_halo, *corners, std_half),
        vmem=16,
        flops=2 * flops,
        scratch=scratch,
    )
    parts, input_grad = lax.optimization_barrier((parts, input_grad))
    everyone = CORES * where.x * where.gy
    block_grad, local = call(block_kernel, (of((rows, width), f32), of((everyone, 1, 3 * ch), f32)), (parts, block_std))
    filter_grad = where.send(block_grad, lambda s: dict(x=s["zl"], zl=s["x"]))
    sums = where.exchange(local, ("zl", "zh"), lambda s: (s["core"], s["x"], s["y"]))

    grad = call(functools.partial(last_kernel, float(ch * taps)), of((taps, rows, ch), f32), (filter_grad, raw, mean_out, inv_std, sums))
    return (input_grad, jnp.transpose(grad, (1, 0, 2)))


def solution(mesh):
    where = Layout(mesh)
    in_specs = (P(("gx", "gy"), None, None), P("gx", "gy", "gz", None), P("gx", "gy", "gz", None))
    out_specs = (P("gx", "gy", "gz", None), P(("gx", "gy"), None, None))

    def body(raw_weight, inputs, cotangent):
        return on_device(where, raw_weight, inputs, cotangent)

    return jax.shard_map(body, mesh=mesh, in_specs=in_specs, out_specs=out_specs, check_vma=False)
```

```python
import functools

import jax
import jax.numpy as jnp
from jax import lax
from jax.experimental import pallas as pl
from jax.experimental.pallas import tpu as pltpu
from jax.sharding import PartitionSpec as P


var_eps = 1e-05
norm_eps = 1e-06
clip_norm = 600.0
AXES = ("gx", "gy", "gz")
CORES = 2
TAPS = 27
MIB = 1024 * 1024


def call(kernel, out_shape, args, vmem=8, flops=1_000_000_000, scratch=()):
    many = isinstance(out_shape, tuple)
    return pl.pallas_call(
        kernel,
        out_shape=out_shape,
        in_specs=[pl.BlockSpec(memory_space=pltpu.VMEM) for _ in args],
        out_specs=tuple(pl.BlockSpec(memory_space=pltpu.VMEM) for _ in out_shape)
        if many
        else pl.BlockSpec(memory_space=pltpu.VMEM),
        scratch_shapes=scratch,
        compiler_params=pltpu.CompilerParams(vmem_limit_bytes=vmem * MIB),
        cost_estimate=pl.CostEstimate(flops=flops, bytes_accessed=1_000_000, transcendentals=0),
    )(*args)


def of(shape, dtype):
    return jax.ShapeDtypeStruct(shape, dtype)


class Layout:
    def __init__(self, mesh):
        self.gx, self.gy, self.gz = (mesh.shape[a] for a in AXES)
        self.zl = self.gx // CORES
        self.x = self.zl
        self.zh = self.gz // self.x

    def spots(self):
        for zl in range(self.zl):
            for core in range(CORES):
                for y in range(self.gy):
                    for zh in range(self.zh):
                        for x in range(self.x):
                            yield dict(zl=zl, core=core, y=y, zh=zh, x=x)

    def index(self, s):
        return ((s["zl"] * CORES + s["core"]) * self.gy + s["y"]) * self.gz + s["zh"] * self.x + s["x"]

    def send(self, array, target):
        pairs = []
        for s in self.spots():
            t = dict(s)
            t.update(target(s))
            pairs.append((self.index(s), self.index(t)))
        return lax.ppermute(array, AXES, pairs)

    def exchange(self, array, fixed, order):
        groups = {}
        for s in self.spots():
            groups.setdefault(tuple(s[k] for k in fixed), []).append((order(s), self.index(s)))
        groups = [[i for _, i in sorted(g)] for g in groups.values()]
        return lax.all_to_all(array, AXES, 0, 0, tiled=True, axis_index_groups=groups)


def swapped(first, second, axis):
    count = lax.axis_size(axis)

    def pairs(start):
        ends = [(i, i + 1) for i in range(start, count - 1, 2)]
        return ends + [(j, i) for i, j in ends]

    first = lax.ppermute(first, axis, pairs(0))
    second = lax.ppermute(second, axis, pairs(1))
    return first, second


def is_odd(axis):
    return lax.axis_index(axis) % 2 == 1


def wide(row, taps=TAPS):
    return jnp.concatenate([row] * taps, axis=1)


def fold(values, ch):
    total = values[:, 0:ch]
    for t in range(1, values.shape[1] // ch):
        total = total + values[:, t * ch : (t + 1) * ch]
    return jnp.sum(total, axis=0, keepdims=True)


def faces_kernel(mid_ref, first_ref, second_ref):
    last = mid_ref.shape[0] - 1
    odd = is_odd("gx")
    first_ref[0] = mid_ref[jnp.where(odd, 0, last)]
    second_ref[0] = mid_ref[jnp.where(odd, last, 0)]


def base_kernel(raw_ref, mid_ref, in_ref, held_ref, zl_ref, zh_ref, il_ref, ih_ref):
    taps, rows, ch = raw_ref.shape
    base = jnp.sum(jnp.sum(raw_ref[...], axis=0), axis=0, keepdims=True) / (taps * rows)
    high = base.astype(jnp.bfloat16)
    low = (base - high.astype(jnp.float32)).astype(jnp.bfloat16)
    base = high.astype(jnp.float32) + low.astype(jnp.float32)
    for t in range(taps):
        held_ref[0, :, t * ch : (t + 1) * ch] = (raw_ref[t] - base).astype(jnp.bfloat16)
    place = lax.broadcasted_iota(jnp.int32, (rows, ch), 0)
    both = jnp.where(place == 0, high.astype(jnp.float32), low.astype(jnp.float32))
    held_ref[0, :, taps * ch :] = both.astype(jnp.bfloat16)
    for whole_ref, first_ref, last_ref in ((mid_ref, zl_ref, zh_ref), (in_ref, il_ref, ih_ref)):
        for k in range(whole_ref.shape[0]):
            whole = whole_ref[k].astype(jnp.float32)
            first_ref[k] = whole[:, 0].astype(jnp.bfloat16)
            last_ref[k] = whole[:, -1].astype(jnp.bfloat16)


def join_kernel(*refs):
    place = 0
    for piece in refs[:-1]:
        refs[-1][place : place + piece.shape[0]] = piece[...]
        place += piece.shape[0]


def picked(odd, first, second):
    return jnp.where(odd, first, second), jnp.where(odd, second, first)


def height_kernel(mid_ref, xa_ref, xb_ref, il_ref, ih_ref, first_ref, second_ref):
    nx, ny, nz, ch = mid_ref.shape
    x_odd, odd = is_odd("gx"), is_odd("gy")
    first, last = il_ref[...].astype(jnp.float32), ih_ref[...].astype(jnp.float32)
    ends = [jnp.concatenate([first[:, None, j], last[:, None, j]], axis=1) for j in (0, ny - 1)]
    ends = [e.astype(jnp.bfloat16) for e in ends]
    outs = ((first_ref, jnp.where(odd, 0, ny - 1)), (second_ref, jnp.where(odd, ny - 1, 0)))
    for (out_ref, j), end in zip(outs, (picked(odd, *ends))):
        low, high = picked(x_odd, xa_ref[0, j], xb_ref[0, j])
        out_ref[0, :nz] = low
        out_ref[nx + 1, :nz] = high
        for k in (0, nx + 1):
            out_ref[k, nz:] = jnp.zeros((2, ch), jnp.bfloat16)
        for k in range(nx):
            out_ref[k + 1, :nz] = mid_ref[k, j]
        out_ref[1 : nx + 1, nz:] = end


def width_kernel(zl_ref, zh_ref, xa_ref, xb_ref, first_ref, second_ref):
    nx = zl_ref.shape[0]
    nz = xa_ref.shape[2]
    x_odd, odd = is_odd("gx"), is_odd("gz")
    low, high = picked(odd, zl_ref[...], zh_ref[...])
    first_ref[1 : nx + 1] = low
    second_ref[1 : nx + 1] = high
    below, above = picked(x_odd, xa_ref[0].astype(jnp.float32), xb_ref[0].astype(jnp.float32))
    for k, face in ((0, below), (nx + 1, above)):
        low, high = picked(odd, face[:, 0], face[:, nz - 1])
        first_ref[k] = low.astype(jnp.bfloat16)
        second_ref[k] = high.astype(jnp.bfloat16)


def corner_kernel(za_ref, zb_ref, first_ref, second_ref):
    ny = za_ref.shape[1]
    odd = is_odd("gy")
    low, high = picked(is_odd("gz"), za_ref[...].astype(jnp.float32), zb_ref[...].astype(jnp.float32))
    ends = [jnp.concatenate([low[:, None, j], high[:, None, j]], axis=1) for j in (0, ny - 1)]
    first, second = picked(odd, *ends)
    first_ref[...] = first.astype(jnp.bfloat16)
    second_ref[...] = second.astype(jnp.bfloat16)


def fill_taps(taps_ref, mid_ref, xa_ref, xb_ref, ya_ref, yb_ref, z_halo):
    nx, ny, nz, ch = mid_ref.shape
    x_odd, y_odd, z_odd = is_odd("gx"), is_odd("gy"), is_odd("gz")

    def fill(k, j, rows, low, high):
        n = rows.shape[0]
        mid = rows.astype(jnp.float32)
        up = jnp.concatenate([mid[:, 1:], high], axis=1)
        down = jnp.concatenate([low, mid[:, :-1]], axis=1)
        taps_ref[k, j : j + n, :, 0:ch] = up.astype(jnp.bfloat16)
        taps_ref[k, j : j + n, :, ch : 2 * ch] = rows
        taps_ref[k, j : j + n, :, 2 * ch : 3 * ch] = down.astype(jnp.bfloat16)

    def fill_rows(k, rows):
        if z_halo:
            low, high = picked(z_odd, z_halo[0][k].astype(jnp.float32), z_halo[1][k].astype(jnp.float32))
            fill(k, 1, rows, low[:, None], high[:, None])
        else:
            none = jnp.zeros((ny, 1, ch), jnp.float32)
            fill(k, 1, rows, none, none)

    def plane(k, carry):
        pairs = zip((0, ny + 1), picked(y_odd, ya_ref[k, :nz], yb_ref[k, :nz]))
        if z_halo:
            corners = picked(y_odd, z_halo[2][k].astype(jnp.float32), z_halo[3][k].astype(jnp.float32))
            for (j, row), corner in zip(pairs, corners):
                fill(k, j, row[None], corner[None, 0:1], corner[None, 1:2])
        else:
            none = jnp.zeros((1, 1, ch), jnp.float32)
            for j, row in pairs:
                fill(k, j, row[None], none, none)
        return carry

    def middle(k, carry):
        fill_rows(k + 1, mid_ref[k])
        return carry

    lax.fori_loop(0, nx, middle, 0)
    low, high = picked(x_odd, xa_ref[0], xb_ref[0])
    fill_rows(0, low)
    fill_rows(nx + 1, high)
    lax.fori_loop(0, nx + 2, plane, 0)


def filter_kernel(mid_ref, xa_ref, xb_ref, ya_ref, yb_ref, in_ref, il_ref, ih_ref, total_ref, ends_ref, taps_ref):
    nx, ny, nz, ch = mid_ref.shape
    fill_taps(taps_ref, mid_ref, xa_ref, xb_ref, ya_ref, yb_ref, None)
    cells = nx * ny * nz
    flat = in_ref[...].reshape(cells, ch).T
    for a in range(3):
        for b in range(3):
            view = taps_ref[2 - a : 2 - a + nx, 2 - b : 2 - b + ny].reshape(cells, 3 * ch)
            lanes = pl.ds((a * 3 + b) * 3 * ch, 3 * ch)
            total_ref[:, lanes] = jnp.dot(flat, view, preferred_element_type=jnp.float32)
    below, above = picked(is_odd("gy"), ya_ref[1 : nx + 1, nz:], yb_ref[1 : nx + 1, nz:])
    below, above = below.astype(jnp.float32), above.astype(jnp.float32)
    for side, own_ref in enumerate((il_ref, ih_ref)):
        own = own_ref[...].astype(jnp.float32)
        face = jnp.concatenate([below[:, side : side + 1], own, above[:, side : side + 1]], axis=1)
        for b in range(3):
            ends_ref[side, b] = face[:, b : b + ny].reshape(nx * ny, ch).T.astype(jnp.bfloat16)


def finish_kernel(total_ref, ends_ref, za_ref, zb_ref, keep_ref, send_ref):
    ch = total_ref.shape[0]
    nx, ny = za_ref.shape[0] - 2, za_ref.shape[1]
    core = lax.axis_index("gx") % CORES
    crossing = []
    for halo in picked(is_odd("gz"), za_ref[...], zb_ref[...]):
        crossing.append(
            jnp.concatenate([halo[2 - a : 2 - a + nx].reshape(nx * ny, ch) for a in range(3)], axis=1)
        )
    for b in range(3):
        below = jnp.dot(ends_ref[0, b], crossing[0], preferred_element_type=jnp.float32)
        above = jnp.dot(ends_ref[1, b], crossing[1], preferred_element_type=jnp.float32)
        for a in range(3):
            for c in range(3):
                lanes = pl.ds(((a * 3 + b) * 3 + c) * ch, ch)
                res = total_ref[:, lanes]
                if c == 0:
                    res = res + above[:, a * ch : (a + 1) * ch]
                if c == 2:
                    res = res + below[:, a * ch : (a + 1) * ch]
                for g in range(ch // 32):
                    first = res[g * 32 : g * 32 + 16]
                    second = res[g * 32 + 16 : g * 32 + 32]
                    keep_ref[g * 16 : g * 16 + 16, lanes] = jnp.where(core == 0, first, second)
                    other = jnp.where(core == 0, second, first)
                    send_ref[g * 16 : g * 16 + 16, lanes] = other.astype(jnp.bfloat16)


def pair_kernel(keep_ref, other_ref, out_ref):
    rows = out_ref.shape[1]
    for g in range(keep_ref.shape[0] // 16):
        total = keep_ref[g * 16 : g * 16 + 16] + other_ref[g * 16 : g * 16 + 16].astype(jnp.float32)
        for r in range(16 // rows):
            out_ref[g * (16 // rows) + r] = total[r * rows : (r + 1) * rows].astype(jnp.bfloat16)


def peers_kernel(parts_ref, out_ref):
    total = jnp.sum(parts_ref[...].astype(jnp.float32), axis=0).astype(jnp.bfloat16)
    for k in range(out_ref.shape[0]):
        out_ref[k] = total


def block_kernel(parts_ref, std_ref, grad_ref, sums_ref):
    ch = sums_ref.shape[2] // 3
    total = jnp.sum(parts_ref[...].astype(jnp.float32), axis=0)
    grad_ref[...] = total
    three = jnp.concatenate([fold(total, ch), fold(total * std_ref[...], ch), fold(total * total, ch)], axis=1)
    for k in range(sums_ref.shape[0]):
        sums_ref[k] = three


def input_kernel(mid_ref, xa_ref, xb_ref, ya_ref, yb_ref, za_ref, zb_ref, ca_ref, cb_ref, std_ref, out_ref, taps_ref):
    nx, ny, nz, ch = out_ref.shape
    fill_taps(taps_ref, mid_ref, xa_ref, xb_ref, ya_ref, yb_ref, (za_ref, zb_ref, ca_ref, cb_ref))
    planes = 2
    std = std_ref[...]
    for x in range(0, nx, planes):
        rows = jnp.concatenate(
            [
                taps_ref[x + 2 - a : x + 2 - a + planes, 2 - b : 2 - b + ny].reshape(planes * ny * nz, 3 * ch)
                for a in range(3)
                for b in range(3)
            ],
            axis=1,
        )
        res = lax.dot_general(rows, std, (((1,), (1,)), ((), ())), preferred_element_type=jnp.float32)
        out_ref[x : x + planes] = res.astype(jnp.bfloat16).reshape(planes, ny, nz, ch)


def std_kernel(x_count, near_ref, far_ref, std_ref, mean_ref, inv_ref, block_ref):
    slots, rows, held = near_ref.shape
    ch = inv_ref.shape[1]
    width = held - ch
    taps = width // ch
    gx, y, x = lax.axis_index("gx"), lax.axis_index("gy"), lax.axis_index("gz") % x_count
    zl, core = gx // CORES, gx % CORES
    blocks = [(b // 8, (b // 4) % 2, b % 4) for b in range(2 * slots)]
    count = float(2 * slots * rows * taps)

    def parts(zl_b, core_b, y_b):
        y_off, z_off = y_b ^ y, zl_b ^ zl
        slot = (y_off >> 1) + 2 * (y_off & 1) + 4 * (z_off >> 1) + 8 * (z_off & 1)
        data = jnp.where(core_b == core, near_ref[slot], far_ref[slot]).astype(jnp.float32)
        return data[:, :width], data[0:1, width:] + data[1:2, width:]

    total = jnp.zeros((1, ch), jnp.float32)
    for b in blocks:
        values, base = parts(*b)
        total = total + (fold(values, ch) + float(rows * taps) * base)
    mean = total / count
    square = jnp.zeros((1, ch), jnp.float32)
    for b in blocks:
        values, base = parts(*b)
        first = values + wide(base - mean)
        square = square + fold(first * first, ch)
    inv = lax.rsqrt(square / count + var_eps)
    mean_ref[...] = mean
    inv_ref[...] = inv
    inv_wide = wide(inv)
    for n, b in enumerate(blocks):
        values, base = parts(*b)
        std_ref[n * rows : (n + 1) * rows, :] = ((values + wide(base - mean)) * inv_wide).astype(jnp.bfloat16)
    values, base = parts(x, core, y)
    block_ref[...] = (values + wide(base - mean)) * inv_wide


def last_kernel(fan_count, x_count, own_ref, *refs):
    *got_refs, raw_ref, mean_ref, inv_ref, sums_ref, out_ref = refs
    taps, _, ch = raw_ref.shape
    steps = (lax.axis_index("gz") - lax.axis_index("gx") // CORES) % x_count
    grad = own_ref[...]
    for k, got_ref in enumerate(got_refs, 1):
        grad = jnp.where(steps == k, got_ref[...], grad)
    sums = jnp.sum(sums_ref[...], axis=0)
    sum_grad, sum_cross, sum_square = sums[:, :ch], sums[:, ch : 2 * ch], sums[:, 2 * ch :]
    mean, inv = mean_ref[...], inv_ref[...]
    mean_grad = sum_grad / fan_count
    mean_cross = sum_cross / fan_count
    shrink = 1.0 - var_eps * inv * inv
    per_output = sum_square - 2.0 * mean_grad * sum_grad - 2.0 * mean_cross * sum_cross
    per_output = per_output + fan_count * mean_grad * mean_grad + fan_count * mean_cross * mean_cross * shrink
    square_sum = jnp.sum(inv * inv * per_output, axis=1, keepdims=True)
    scale = jnp.minimum(1.0, clip_norm * lax.rsqrt(square_sum + norm_eps))
    factor = inv * scale
    for t in range(taps):
        std = (raw_ref[t] - mean) * inv
        out_ref[t] = factor * (grad[:, t * ch : (t + 1) * ch] - mean_grad - std * mean_cross)


def on_device(where, raw_weight, inputs, cotangent):
    nx, ny, nz, ch = inputs.shape
    rows, taps = raw_weight.shape[:2]
    width = taps * ch
    bf16, f32 = jnp.bfloat16, jnp.float32
    raw = jnp.transpose(raw_weight, (1, 0, 2))

    def joined(held):
        return jnp.concatenate(held, 0)

    def both(shape):
        return (of(shape, bf16), of(shape, bf16))

    faces = call(faces_kernel, both((1, ny, nz, ch)), (cotangent,))
    x_halo = swapped(*faces, "gx")
    block, *ends = call(
        base_kernel,
        (of((1, rows, width + ch), bf16), *both((nx, ny, ch)), *both((nx, ny, ch))),
        (raw, cotangent, inputs),
    )
    held = [block, where.send(block, lambda s: dict(y=s["y"] ^ 2))]
    faces = call(height_kernel, both((nx + 2, nz + 2, ch)), (cotangent, *x_halo, *ends[2:]))
    y_halo = swapped(*faces, "gy")
    faces = call(width_kernel, both((nx + 2, ny, ch)), (*ends[:2], *x_halo))
    z_halo = swapped(*faces, "gz")
    held.append(where.send(joined(held), lambda s: dict(y=s["y"] ^ 1)))
    held.append(where.send(joined(held), lambda s: dict(zl=s["zl"] ^ 2)))
    held.append(where.send(joined(held), lambda s: dict(zl=s["zl"] ^ 1)))

    flops = 2 * nx * ny * nz * ch * width
    scratch = [pltpu.VMEM((nx + 2, ny + 2, nz, 3 * ch), bf16)]
    total, end_rows = call(
        filter_kernel,
        (of((ch, width), f32), of((2, 3, ch, nx * ny), bf16)),
        (cotangent, *x_halo, *y_halo, inputs, *ends[2:]),
        vmem=16,
        flops=2 * flops,
        scratch=scratch,
    )
    keep, send = call(
        finish_kernel, (of((ch // 2, width), f32), of((ch // 2, width), bf16)), (total, end_rows, *z_halo)
    )
    other = where.send(send, lambda s: dict(core=1 - s["core"]))
    held = call(join_kernel, of((16, rows, width + ch), bf16), held)
    peers = where.x * where.gy
    half = call(pair_kernel, of((peers, rows, width), bf16), (keep, other))
    parts = where.exchange(half, ("core", "zl", "zh"), lambda s: (s["x"], s["y"]))
    far = where.send(held, lambda s: dict(core=1 - s["core"]))
    corners = swapped(*call(corner_kernel, both((nx + 2, 2, ch)), z_halo), "gy")
    std_half, mean_out, inv_std, block_std = call(
        functools.partial(std_kernel, where.x),
        (of((ch, width), bf16), of((1, ch), f32), of((1, ch), f32), of((rows, width), f32)),
        (held, far),
        flops=3_000_000_000,
    )
    copies = call(peers_kernel, of((where.zl * where.zh, rows, width), bf16), (parts,))
    parts = where.exchange(copies, ("core", "x", "y"), lambda s: (s["zh"], s["zl"]))
    input_grad = call(
        input_kernel,
        of(inputs.shape, bf16),
        (cotangent, *x_halo, *y_halo, *z_halo, *corners, std_half),
        vmem=16,
        flops=2 * flops,
        scratch=scratch,
    )
    parts, input_grad = lax.optimization_barrier((parts, input_grad))
    everyone = CORES * where.x * where.gy
    block_grad, local = call(block_kernel, (of((rows, width), f32), of((everyone, 1, 3 * ch), f32)), (parts, block_std))
    passed = [where.send(block_grad, lambda s, k=k: dict(x=(s["x"] + k) % where.x)) for k in range(1, where.x)]
    sums = where.exchange(local, ("zl", "zh"), lambda s: (s["core"], s["x"], s["y"]))

    grad = call(functools.partial(last_kernel, float(ch * taps), where.x), of((taps, rows, ch), f32), (block_grad, *passed, raw, mean_out, inv_std, sums))
    return (input_grad, jnp.transpose(grad, (1, 0, 2)))


def solution(mesh):
    where = Layout(mesh)
    in_specs = (P(("gx", "gy"), None, None), P("gx", "gy", "gz", None), P("gx", "gy", "gz", None))
    out_specs = (P("gx", "gy", "gz", None), P(("gx", "gy"), None, None))

    def body(raw_weight, inputs, cotangent):
        return on_device(where, raw_weight, inputs, cotangent)

    return jax.shard_map(body, mesh=mesh, in_specs=in_specs, out_specs=out_specs, check_vma=False)
```

```python
import functools

import jax
import jax.numpy as jnp
from jax import lax
from jax.experimental import pallas as pl
from jax.experimental.pallas import tpu as pltpu
from jax.sharding import PartitionSpec as P


var_eps = 1e-05
norm_eps = 1e-06
clip_norm = 600.0
AXES = ("gx", "gy", "gz")
CORES = 2
TAPS = 27
MIB = 1024 * 1024


def call(kernel, out_shape, args, vmem=8, flops=1_000_000_000, scratch=()):
    many = isinstance(out_shape, tuple)
    return pl.pallas_call(
        kernel,
        out_shape=out_shape,
        in_specs=[pl.BlockSpec(memory_space=pltpu.VMEM) for _ in args],
        out_specs=tuple(pl.BlockSpec(memory_space=pltpu.VMEM) for _ in out_shape)
        if many
        else pl.BlockSpec(memory_space=pltpu.VMEM),
        scratch_shapes=scratch,
        compiler_params=pltpu.CompilerParams(vmem_limit_bytes=vmem * MIB),
        cost_estimate=pl.CostEstimate(flops=flops, bytes_accessed=1_000_000, transcendentals=0),
    )(*args)


def of(shape, dtype):
    return jax.ShapeDtypeStruct(shape, dtype)


class Layout:
    def __init__(self, mesh):
        self.gx, self.gy, self.gz = (mesh.shape[a] for a in AXES)
        self.zl = self.gx // CORES
        self.x = self.zl
        self.zh = self.gz // self.x

    def spots(self):
        for zl in range(self.zl):
            for core in range(CORES):
                for y in range(self.gy):
                    for zh in range(self.zh):
                        for x in range(self.x):
                            yield dict(zl=zl, core=core, y=y, zh=zh, x=x)

    def index(self, s):
        return ((s["zl"] * CORES + s["core"]) * self.gy + s["y"]) * self.gz + s["zh"] * self.x + s["x"]

    def send(self, array, target):
        pairs = []
        for s in self.spots():
            t = dict(s)
            t.update(target(s))
            pairs.append((self.index(s), self.index(t)))
        return lax.ppermute(array, AXES, pairs)

    def exchange(self, array, fixed, order):
        groups = {}
        for s in self.spots():
            groups.setdefault(tuple(s[k] for k in fixed), []).append((order(s), self.index(s)))
        groups = [[i for _, i in sorted(g)] for g in groups.values()]
        return lax.all_to_all(array, AXES, 0, 0, tiled=True, axis_index_groups=groups)


def swapped(first, second, axis):
    count = lax.axis_size(axis)

    def pairs(start):
        ends = [(i, i + 1) for i in range(start, count - 1, 2)]
        return ends + [(j, i) for i, j in ends]

    first = lax.ppermute(first, axis, pairs(0))
    second = lax.ppermute(second, axis, pairs(1))
    return first, second


def is_odd(axis):
    return lax.axis_index(axis) % 2 == 1


def wide(row, taps=TAPS):
    return jnp.concatenate([row] * taps, axis=1)


def fold(values, ch):
    total = values[:, 0:ch]
    for t in range(1, values.shape[1] // ch):
        total = total + values[:, t * ch : (t + 1) * ch]
    return jnp.sum(total, axis=0, keepdims=True)


def faces_kernel(mid_ref, first_ref, second_ref):
    last = mid_ref.shape[0] - 1
    odd = is_odd("gx")
    first_ref[0] = mid_ref[jnp.where(odd, 0, last)]
    second_ref[0] = mid_ref[jnp.where(odd, last, 0)]


def base_kernel(raw_ref, mid_ref, in_ref, held_ref, zl_ref, zh_ref, il_ref, ih_ref):
    taps, rows, ch = raw_ref.shape
    base = jnp.sum(jnp.sum(raw_ref[...], axis=0), axis=0, keepdims=True) / (taps * rows)
    high = base.astype(jnp.bfloat16)
    low = (base - high.astype(jnp.float32)).astype(jnp.bfloat16)
    base = high.astype(jnp.float32) + low.astype(jnp.float32)
    for t in range(taps):
        held_ref[0, :, t * ch : (t + 1) * ch] = (raw_ref[t] - base).astype(jnp.bfloat16)
    place = lax.broadcasted_iota(jnp.int32, (rows, ch), 0)
    both = jnp.where(place == 0, high.astype(jnp.float32), low.astype(jnp.float32))
    held_ref[0, :, taps * ch :] = both.astype(jnp.bfloat16)
    for whole_ref, first_ref, last_ref in ((mid_ref, zl_ref, zh_ref), (in_ref, il_ref, ih_ref)):
        for k in range(whole_ref.shape[0]):
            whole = whole_ref[k].astype(jnp.float32)
            first_ref[k] = whole[:, 0].astype(jnp.bfloat16)
            last_ref[k] = whole[:, -1].astype(jnp.bfloat16)


def join_kernel(*refs):
    place = 0
    for piece in refs[:-1]:
        refs[-1][place : place + piece.shape[0]] = piece[...]
        place += piece.shape[0]


def picked(odd, first, second):
    return jnp.where(odd, first, second), jnp.where(odd, second, first)


def height_kernel(mid_ref, xa_ref, xb_ref, il_ref, ih_ref, first_ref, second_ref):
    nx, ny, nz, ch = mid_ref.shape
    x_odd, odd = is_odd("gx"), is_odd("gy")
    first, last = il_ref[...].astype(jnp.float32), ih_ref[...].astype(jnp.float32)
    ends = [jnp.concatenate([first[:, None, j], last[:, None, j]], axis=1) for j in (0, ny - 1)]
    ends = [e.astype(jnp.bfloat16) for e in ends]
    outs = ((first_ref, jnp.where(odd, 0, ny - 1)), (second_ref, jnp.where(odd, ny - 1, 0)))
    for (out_ref, j), end in zip(outs, (picked(odd, *ends))):
        low, high = picked(x_odd, xa_ref[0, j], xb_ref[0, j])
        out_ref[0, :nz] = low
        out_ref[nx + 1, :nz] = high
        for k in (0, nx + 1):
            out_ref[k, nz:] = jnp.zeros((2, ch), jnp.bfloat16)
        for k in range(nx):
            out_ref[k + 1, :nz] = mid_ref[k, j]
        out_ref[1 : nx + 1, nz:] = end


def width_kernel(zl_ref, zh_ref, xa_ref, xb_ref, first_ref, second_ref):
    nx = zl_ref.shape[0]
    nz = xa_ref.shape[2]
    x_odd, odd = is_odd("gx"), is_odd("gz")
    low, high = picked(odd, zl_ref[...], zh_ref[...])
    first_ref[1 : nx + 1] = low
    second_ref[1 : nx + 1] = high
    below, above = picked(x_odd, xa_ref[0].astype(jnp.float32), xb_ref[0].astype(jnp.float32))
    for k, face in ((0, below), (nx + 1, above)):
        low, high = picked(odd, face[:, 0], face[:, nz - 1])
        first_ref[k] = low.astype(jnp.bfloat16)
        second_ref[k] = high.astype(jnp.bfloat16)


def corner_kernel(za_ref, zb_ref, first_ref, second_ref):
    ny = za_ref.shape[1]
    odd = is_odd("gy")
    low, high = picked(is_odd("gz"), za_ref[...].astype(jnp.float32), zb_ref[...].astype(jnp.float32))
    ends = [jnp.concatenate([low[:, None, j], high[:, None, j]], axis=1) for j in (0, ny - 1)]
    first, second = picked(odd, *ends)
    first_ref[...] = first.astype(jnp.bfloat16)
    second_ref[...] = second.astype(jnp.bfloat16)


def fill_taps(taps_ref, mid_ref, xa_ref, xb_ref, ya_ref, yb_ref, z_halo):
    nx, ny, nz, ch = mid_ref.shape
    x_odd, y_odd, z_odd = is_odd("gx"), is_odd("gy"), is_odd("gz")

    def fill(k, j, rows, low, high):
        n = rows.shape[0]
        mid = rows.astype(jnp.float32)
        up = jnp.concatenate([mid[:, 1:], high], axis=1)
        down = jnp.concatenate([low, mid[:, :-1]], axis=1)
        taps_ref[k, j : j + n, :, 0:ch] = up.astype(jnp.bfloat16)
        taps_ref[k, j : j + n, :, ch : 2 * ch] = rows
        taps_ref[k, j : j + n, :, 2 * ch : 3 * ch] = down.astype(jnp.bfloat16)

    def fill_rows(k, rows):
        if z_halo:
            low, high = picked(z_odd, z_halo[0][k].astype(jnp.float32), z_halo[1][k].astype(jnp.float32))
            fill(k, 1, rows, low[:, None], high[:, None])
        else:
            none = jnp.zeros((ny, 1, ch), jnp.float32)
            fill(k, 1, rows, none, none)

    def plane(k, carry):
        pairs = zip((0, ny + 1), picked(y_odd, ya_ref[k, :nz], yb_ref[k, :nz]))
        if z_halo:
            corners = picked(y_odd, z_halo[2][k].astype(jnp.float32), z_halo[3][k].astype(jnp.float32))
            for (j, row), corner in zip(pairs, corners):
                fill(k, j, row[None], corner[None, 0:1], corner[None, 1:2])
        else:
            none = jnp.zeros((1, 1, ch), jnp.float32)
            for j, row in pairs:
                fill(k, j, row[None], none, none)
        return carry

    def middle(k, carry):
        fill_rows(k + 1, mid_ref[k])
        return carry

    lax.fori_loop(0, nx, middle, 0)
    low, high = picked(x_odd, xa_ref[0], xb_ref[0])
    fill_rows(0, low)
    fill_rows(nx + 1, high)
    lax.fori_loop(0, nx + 2, plane, 0)


def filter_kernel(mid_ref, xa_ref, xb_ref, ya_ref, yb_ref, in_ref, il_ref, ih_ref, total_ref, ends_ref, taps_ref):
    nx, ny, nz, ch = mid_ref.shape
    fill_taps(taps_ref, mid_ref, xa_ref, xb_ref, ya_ref, yb_ref, None)
    cells = nx * ny * nz
    flat = in_ref[...].reshape(cells, ch).T
    for a in range(3):
        for b in range(3):
            view = taps_ref[2 - a : 2 - a + nx, 2 - b : 2 - b + ny].reshape(cells, 3 * ch)
            lanes = pl.ds((a * 3 + b) * 3 * ch, 3 * ch)
            total_ref[:, lanes] = jnp.dot(flat, view, preferred_element_type=jnp.float32)
    below, above = picked(is_odd("gy"), ya_ref[1 : nx + 1, nz:], yb_ref[1 : nx + 1, nz:])
    below, above = below.astype(jnp.float32), above.astype(jnp.float32)
    for side, own_ref in enumerate((il_ref, ih_ref)):
        own = own_ref[...].astype(jnp.float32)
        face = jnp.concatenate([below[:, side : side + 1], own, above[:, side : side + 1]], axis=1)
        for b in range(3):
            ends_ref[side, b] = face[:, b : b + ny].reshape(nx * ny, ch).T.astype(jnp.bfloat16)


def finish_kernel(total_ref, ends_ref, za_ref, zb_ref, keep_ref, send_ref):
    ch = total_ref.shape[0]
    nx, ny = za_ref.shape[0] - 2, za_ref.shape[1]
    core = lax.axis_index("gx") % CORES
    crossing = []
    for halo in picked(is_odd("gz"), za_ref[...], zb_ref[...]):
        crossing.append(
            jnp.concatenate([halo[2 - a : 2 - a + nx].reshape(nx * ny, ch) for a in range(3)], axis=1)
        )
    for b in range(3):
        below = jnp.dot(ends_ref[0, b], crossing[0], preferred_element_type=jnp.float32)
        above = jnp.dot(ends_ref[1, b], crossing[1], preferred_element_type=jnp.float32)
        for a in range(3):
            for c in range(3):
                lanes = pl.ds(((a * 3 + b) * 3 + c) * ch, ch)
                res = total_ref[:, lanes]
                if c == 0:
                    res = res + above[:, a * ch : (a + 1) * ch]
                if c == 2:
                    res = res + below[:, a * ch : (a + 1) * ch]
                for g in range(ch // 32):
                    first = res[g * 32 : g * 32 + 16]
                    second = res[g * 32 + 16 : g * 32 + 32]
                    keep_ref[g * 16 : g * 16 + 16, lanes] = jnp.where(core == 0, first, second)
                    other = jnp.where(core == 0, second, first)
                    send_ref[g * 16 : g * 16 + 16, lanes] = other.astype(jnp.bfloat16)


def pair_kernel(keep_ref, other_ref, out_ref):
    rows = out_ref.shape[1]
    for g in range(keep_ref.shape[0] // 16):
        total = keep_ref[g * 16 : g * 16 + 16] + other_ref[g * 16 : g * 16 + 16].astype(jnp.float32)
        for r in range(16 // rows):
            out_ref[g * (16 // rows) + r] = total[r * rows : (r + 1) * rows].astype(jnp.bfloat16)


def peers_kernel(parts_ref, out_ref):
    total = jnp.sum(parts_ref[...].astype(jnp.float32), axis=0).astype(jnp.bfloat16)
    for k in range(out_ref.shape[0]):
        out_ref[k] = total


def block_kernel(parts_ref, std_ref, out_ref):
    rows, width = std_ref.shape
    ch = (out_ref.shape[1] - width) // 3
    total = jnp.sum(parts_ref[...].astype(jnp.float32), axis=0)
    out_ref[:, :width] = total
    sums = jnp.concatenate([fold(total, ch), fold(total * std_ref[...], ch), fold(total * total, ch)], axis=1)
    place = lax.broadcasted_iota(jnp.int32, (rows, 3 * ch), 0)
    out_ref[:, width:] = jnp.where(place == 0, sums, 0.0)


def around_kernel(axis, count, own_ref, *refs):
    *got_refs, out_ref, held_ref = refs
    here = lax.axis_index(axis) % count
    size = out_ref.shape[1]
    for k, ref in enumerate((own_ref, *got_refs)):
        held_ref[(here + count - k) % count] = ref[0:1, ref.shape[1] - size :]
    total = held_ref[0]
    for k in range(1, count):
        total = total + held_ref[k]
    out_ref[...] = total


def input_kernel(mid_ref, xa_ref, xb_ref, ya_ref, yb_ref, za_ref, zb_ref, ca_ref, cb_ref, std_ref, out_ref, taps_ref):
    nx, ny, nz, ch = out_ref.shape
    fill_taps(taps_ref, mid_ref, xa_ref, xb_ref, ya_ref, yb_ref, (za_ref, zb_ref, ca_ref, cb_ref))
    planes = 2
    std = std_ref[...]
    for x in range(0, nx, planes):
        rows = jnp.concatenate(
            [
                taps_ref[x + 2 - a : x + 2 - a + planes, 2 - b : 2 - b + ny].reshape(planes * ny * nz, 3 * ch)
                for a in range(3)
                for b in range(3)
            ],
            axis=1,
        )
        res = lax.dot_general(rows, std, (((1,), (1,)), ((), ())), preferred_element_type=jnp.float32)
        out_ref[x : x + planes] = res.astype(jnp.bfloat16).reshape(planes, ny, nz, ch)


def std_kernel(x_count, near_ref, far_ref, std_ref, mean_ref, inv_ref, block_ref):
    slots, rows, held = near_ref.shape
    ch = inv_ref.shape[1]
    width = held - ch
    taps = width // ch
    gx, y, x = lax.axis_index("gx"), lax.axis_index("gy"), lax.axis_index("gz") % x_count
    zl, core = gx // CORES, gx % CORES
    blocks = [(b // 8, (b // 4) % 2, b % 4) for b in range(2 * slots)]
    count = float(2 * slots * rows * taps)

    def parts(zl_b, core_b, y_b):
        y_off, z_off = y_b ^ y, zl_b ^ zl
        slot = (y_off >> 1) + 2 * (y_off & 1) + 4 * (z_off >> 1) + 8 * (z_off & 1)
        data = jnp.where(core_b == core, near_ref[slot], far_ref[slot]).astype(jnp.float32)
        return data[:, :width], data[0:1, width:] + data[1:2, width:]

    total = jnp.zeros((1, ch), jnp.float32)
    for b in blocks:
        values, base = parts(*b)
        total = total + (fold(values, ch) + float(rows * taps) * base)
    mean = total / count
    square = jnp.zeros((1, ch), jnp.float32)
    for b in blocks:
        values, base = parts(*b)
        first = values + wide(base - mean)
        square = square + fold(first * first, ch)
    inv = lax.rsqrt(square / count + var_eps)
    mean_ref[...] = mean
    inv_ref[...] = inv
    inv_wide = wide(inv)
    for n, b in enumerate(blocks):
        values, base = parts(*b)
        std_ref[n * rows : (n + 1) * rows, :] = ((values + wide(base - mean)) * inv_wide).astype(jnp.bfloat16)
    values, base = parts(x, core, y)
    block_ref[...] = (values + wide(base - mean)) * inv_wide


def last_kernel(fan_count, x_count, own_ref, *refs):
    *got_refs, raw_ref, mean_ref, inv_ref, sums_ref, others_ref, out_ref = refs
    taps, _, ch = raw_ref.shape
    steps = (lax.axis_index("gz") - lax.axis_index("gx") // CORES) % x_count
    grad = own_ref[:, : taps * ch]
    for k, got_ref in enumerate(got_refs, 1):
        grad = jnp.where(steps == k, got_ref[:, : taps * ch], grad)
    sums = sums_ref[...] + others_ref[...]
    sum_grad, sum_cross, sum_square = sums[:, :ch], sums[:, ch : 2 * ch], sums[:, 2 * ch :]
    mean, inv = mean_ref[...], inv_ref[...]
    mean_grad = sum_grad / fan_count
    mean_cross = sum_cross / fan_count
    shrink = 1.0 - var_eps * inv * inv
    per_output = sum_square - 2.0 * mean_grad * sum_grad - 2.0 * mean_cross * sum_cross
    per_output = per_output + fan_count * mean_grad * mean_grad + fan_count * mean_cross * mean_cross * shrink
    square_sum = jnp.sum(inv * inv * per_output, axis=1, keepdims=True)
    scale = jnp.minimum(1.0, clip_norm * lax.rsqrt(square_sum + norm_eps))
    factor = inv * scale
    for t in range(taps):
        std = (raw_ref[t] - mean) * inv
        out_ref[t] = factor * (grad[:, t * ch : (t + 1) * ch] - mean_grad - std * mean_cross)


def on_device(where, raw_weight, inputs, cotangent):
    nx, ny, nz, ch = inputs.shape
    rows, taps = raw_weight.shape[:2]
    width = taps * ch
    bf16, f32 = jnp.bfloat16, jnp.float32
    raw = jnp.transpose(raw_weight, (1, 0, 2))

    def joined(held):
        return jnp.concatenate(held, 0)

    def both(shape):
        return (of(shape, bf16), of(shape, bf16))

    faces = call(faces_kernel, both((1, ny, nz, ch)), (cotangent,))
    x_halo = swapped(*faces, "gx")
    block, *ends = call(
        base_kernel,
        (of((1, rows, width + ch), bf16), *both((nx, ny, ch)), *both((nx, ny, ch))),
        (raw, cotangent, inputs),
    )
    held = [block, where.send(block, lambda s: dict(y=s["y"] ^ 2))]
    faces = call(height_kernel, both((nx + 2, nz + 2, ch)), (cotangent, *x_halo, *ends[2:]))
    y_halo = swapped(*faces, "gy")
    faces = call(width_kernel, both((nx + 2, ny, ch)), (*ends[:2], *x_halo))
    z_halo = swapped(*faces, "gz")
    held.append(where.send(joined(held), lambda s: dict(y=s["y"] ^ 1)))
    held.append(where.send(joined(held), lambda s: dict(zl=s["zl"] ^ 2)))
    held.append(where.send(joined(held), lambda s: dict(zl=s["zl"] ^ 1)))

    flops = 2 * nx * ny * nz * ch * width
    scratch = [pltpu.VMEM((nx + 2, ny + 2, nz, 3 * ch), bf16)]
    total, end_rows = call(
        filter_kernel,
        (of((ch, width), f32), of((2, 3, ch, nx * ny), bf16)),
        (cotangent, *x_halo, *y_halo, inputs, *ends[2:]),
        vmem=16,
        flops=2 * flops,
        scratch=scratch,
    )
    keep, send = call(
        finish_kernel, (of((ch // 2, width), f32), of((ch // 2, width), bf16)), (total, end_rows, *z_halo)
    )
    other = where.send(send, lambda s: dict(core=1 - s["core"]))
    held = call(join_kernel, of((16, rows, width + ch), bf16), held)
    peers = where.x * where.gy
    half = call(pair_kernel, of((peers, rows, width), bf16), (keep, other))
    parts = where.exchange(half, ("core", "zl", "zh"), lambda s: (s["x"], s["y"]))
    far = where.send(held, lambda s: dict(core=1 - s["core"]))
    corners = swapped(*call(corner_kernel, both((nx + 2, 2, ch)), z_halo), "gy")
    std_half, mean_out, inv_std, block_std = call(
        functools.partial(std_kernel, where.x),
        (of((ch, width), bf16), of((1, ch), f32), of((1, ch), f32), of((rows, width), f32)),
        (held, far),
        flops=3_000_000_000,
    )
    copies = call(peers_kernel, of((where.zl * where.zh, rows, width), bf16), (parts,))
    parts = where.exchange(copies, ("core", "x", "y"), lambda s: (s["zh"], s["zl"]))
    input_grad = call(
        input_kernel,
        of(inputs.shape, bf16),
        (cotangent, *x_halo, *y_halo, *z_halo, *corners, std_half),
        vmem=16,
        flops=2 * flops,
        scratch=scratch,
    )
    parts, input_grad = lax.optimization_barrier((parts, input_grad))
    block_grad = call(block_kernel, of((rows, width + 3 * ch), f32), (parts, block_std))
    passed = [where.send(block_grad, lambda s, k=k: dict(x=(s["x"] + k) % where.x)) for k in range(1, where.x)]

    def around(axis, count, arrays):
        kernel = functools.partial(around_kernel, axis, count)
        scratch = [pltpu.VMEM((count, 1, 3 * ch), f32)]
        return call(kernel, of((1, 3 * ch), f32), arrays, scratch=scratch)

    sums = around("gz", where.x, (block_grad, *passed))
    rest = [where.send(sums, lambda s, k=k: dict(y=(s["y"] + k) % where.gy)) for k in range(1, where.gy)]
    sums = around("gy", where.gy, (sums, *rest))
    others = where.send(sums, lambda s: dict(core=1 - s["core"]))
    grad = call(
        functools.partial(last_kernel, float(ch * taps), where.x),
        of((taps, rows, ch), f32),
        (block_grad, *passed, raw, mean_out, inv_std, sums, others),
    )
    return (input_grad, jnp.transpose(grad, (1, 0, 2)))


def solution(mesh):
    where = Layout(mesh)
    in_specs = (P(("gx", "gy"), None, None), P("gx", "gy", "gz", None), P("gx", "gy", "gz", None))
    out_specs = (P("gx", "gy", "gz", None), P(("gx", "gy"), None, None))

    def body(raw_weight, inputs, cotangent):
        return on_device(where, raw_weight, inputs, cotangent)

    return jax.shard_map(body, mesh=mesh, in_specs=in_specs, out_specs=out_specs, check_vma=False)
```

```python
import functools

import jax
import jax.numpy as jnp
from jax import lax
from jax.experimental import pallas as pl
from jax.experimental.pallas import tpu as pltpu
from jax.sharding import PartitionSpec as P


var_eps = 1e-05
norm_eps = 1e-06
clip_norm = 600.0
AXES = ("gx", "gy", "gz")
CORES = 2
TAPS = 27
MIB = 1024 * 1024


def call(kernel, out_shape, args, vmem=8, flops=1_000_000_000, scratch=()):
    many = isinstance(out_shape, tuple)
    return pl.pallas_call(
        kernel,
        out_shape=out_shape,
        in_specs=[pl.BlockSpec(memory_space=pltpu.VMEM) for _ in args],
        out_specs=tuple(pl.BlockSpec(memory_space=pltpu.VMEM) for _ in out_shape)
        if many
        else pl.BlockSpec(memory_space=pltpu.VMEM),
        scratch_shapes=scratch,
        compiler_params=pltpu.CompilerParams(vmem_limit_bytes=vmem * MIB),
        cost_estimate=pl.CostEstimate(flops=flops, bytes_accessed=1_000_000, transcendentals=0),
    )(*args)


def of(shape, dtype):
    return jax.ShapeDtypeStruct(shape, dtype)


class Layout:
    def __init__(self, mesh):
        self.gx, self.gy, self.gz = (mesh.shape[a] for a in AXES)
        self.zl = self.gx // CORES
        self.x = self.zl
        self.zh = self.gz // self.x

    def spots(self):
        for zl in range(self.zl):
            for core in range(CORES):
                for y in range(self.gy):
                    for zh in range(self.zh):
                        for x in range(self.x):
                            yield dict(zl=zl, core=core, y=y, zh=zh, x=x)

    def index(self, s):
        return ((s["zl"] * CORES + s["core"]) * self.gy + s["y"]) * self.gz + s["zh"] * self.x + s["x"]

    def send(self, array, target):
        pairs = []
        for s in self.spots():
            t = dict(s)
            t.update(target(s))
            pairs.append((self.index(s), self.index(t)))
        return lax.ppermute(array, AXES, pairs)

    def exchange(self, array, fixed, order):
        groups = {}
        for s in self.spots():
            groups.setdefault(tuple(s[k] for k in fixed), []).append((order(s), self.index(s)))
        groups = [[i for _, i in sorted(g)] for g in groups.values()]
        return lax.all_to_all(array, AXES, 0, 0, tiled=True, axis_index_groups=groups)


def swapped(first, second, axis):
    count = lax.axis_size(axis)

    def pairs(start):
        ends = [(i, i + 1) for i in range(start, count - 1, 2)]
        return ends + [(j, i) for i, j in ends]

    first = lax.ppermute(first, axis, pairs(0))
    second = lax.ppermute(second, axis, pairs(1))
    return first, second


def is_odd(axis):
    return lax.axis_index(axis) % 2 == 1


def wide(row, taps=TAPS):
    return jnp.concatenate([row] * taps, axis=1)


def fold(values, ch):
    total = values[:, 0:ch]
    for t in range(1, values.shape[1] // ch):
        total = total + values[:, t * ch : (t + 1) * ch]
    return jnp.sum(total, axis=0, keepdims=True)


def faces_kernel(mid_ref, first_ref, second_ref):
    last = mid_ref.shape[0] - 1
    odd = is_odd("gx")
    first_ref[0] = mid_ref[jnp.where(odd, 0, last)]
    second_ref[0] = mid_ref[jnp.where(odd, last, 0)]


def base_kernel(raw_ref, mid_ref, in_ref, held_ref, zl_ref, zh_ref, il_ref, ih_ref):
    taps, rows, ch = raw_ref.shape
    base = jnp.sum(jnp.sum(raw_ref[...], axis=0), axis=0, keepdims=True) / (taps * rows)
    high = base.astype(jnp.bfloat16)
    low = (base - high.astype(jnp.float32)).astype(jnp.bfloat16)
    base = high.astype(jnp.float32) + low.astype(jnp.float32)
    for t in range(taps):
        held_ref[0, :, t * ch : (t + 1) * ch] = (raw_ref[t] - base).astype(jnp.bfloat16)
    place = lax.broadcasted_iota(jnp.int32, (rows, ch), 0)
    both = jnp.where(place == 0, high.astype(jnp.float32), low.astype(jnp.float32))
    held_ref[0, :, taps * ch :] = both.astype(jnp.bfloat16)
    for whole_ref, first_ref, last_ref in ((mid_ref, zl_ref, zh_ref), (in_ref, il_ref, ih_ref)):
        for k in range(whole_ref.shape[0]):
            whole = whole_ref[k].astype(jnp.float32)
            first_ref[k] = whole[:, 0].astype(jnp.bfloat16)
            last_ref[k] = whole[:, -1].astype(jnp.bfloat16)


def join_kernel(*refs):
    place = 0
    for piece in refs[:-1]:
        refs[-1][place : place + piece.shape[0]] = piece[...]
        place += piece.shape[0]


def picked(odd, first, second):
    return jnp.where(odd, first, second), jnp.where(odd, second, first)


def height_kernel(mid_ref, xa_ref, xb_ref, il_ref, ih_ref, first_ref, second_ref):
    nx, ny, nz, ch = mid_ref.shape
    x_odd, odd = is_odd("gx"), is_odd("gy")
    first, last = il_ref[...].astype(jnp.float32), ih_ref[...].astype(jnp.float32)
    ends = [jnp.concatenate([first[:, None, j], last[:, None, j]], axis=1) for j in (0, ny - 1)]
    ends = [e.astype(jnp.bfloat16) for e in ends]
    outs = ((first_ref, jnp.where(odd, 0, ny - 1)), (second_ref, jnp.where(odd, ny - 1, 0)))
    for (out_ref, j), end in zip(outs, (picked(odd, *ends))):
        low, high = picked(x_odd, xa_ref[0, j], xb_ref[0, j])
        out_ref[0, :nz] = low
        out_ref[nx + 1, :nz] = high
        for k in (0, nx + 1):
            out_ref[k, nz:] = jnp.zeros((2, ch), jnp.bfloat16)
        for k in range(nx):
            out_ref[k + 1, :nz] = mid_ref[k, j]
        out_ref[1 : nx + 1, nz:] = end


def width_kernel(zl_ref, zh_ref, xa_ref, xb_ref, first_ref, second_ref):
    nx = zl_ref.shape[0]
    nz = xa_ref.shape[2]
    x_odd, odd = is_odd("gx"), is_odd("gz")
    low, high = picked(odd, zl_ref[...], zh_ref[...])
    first_ref[1 : nx + 1] = low
    second_ref[1 : nx + 1] = high
    below, above = picked(x_odd, xa_ref[0].astype(jnp.float32), xb_ref[0].astype(jnp.float32))
    for k, face in ((0, below), (nx + 1, above)):
        low, high = picked(odd, face[:, 0], face[:, nz - 1])
        first_ref[k] = low.astype(jnp.bfloat16)
        second_ref[k] = high.astype(jnp.bfloat16)


def corner_kernel(za_ref, zb_ref, first_ref, second_ref):
    ny = za_ref.shape[1]
    odd = is_odd("gy")
    low, high = picked(is_odd("gz"), za_ref[...].astype(jnp.float32), zb_ref[...].astype(jnp.float32))
    ends = [jnp.concatenate([low[:, None, j], high[:, None, j]], axis=1) for j in (0, ny - 1)]
    first, second = picked(odd, *ends)
    first_ref[...] = first.astype(jnp.bfloat16)
    second_ref[...] = second.astype(jnp.bfloat16)


def fill_taps(taps_ref, mid_ref, xa_ref, xb_ref, ya_ref, yb_ref, z_halo):
    nx, ny, nz, ch = mid_ref.shape
    x_odd, y_odd, z_odd = is_odd("gx"), is_odd("gy"), is_odd("gz")

    def fill(k, j, rows, low, high):
        n = rows.shape[0]
        mid = rows.astype(jnp.float32)
        up = jnp.concatenate([mid[:, 1:], high], axis=1)
        down = jnp.concatenate([low, mid[:, :-1]], axis=1)
        taps_ref[k, j : j + n, :, 0:ch] = up.astype(jnp.bfloat16)
        taps_ref[k, j : j + n, :, ch : 2 * ch] = rows
        taps_ref[k, j : j + n, :, 2 * ch : 3 * ch] = down.astype(jnp.bfloat16)

    def fill_rows(k, rows):
        if z_halo:
            low, high = picked(z_odd, z_halo[0][k].astype(jnp.float32), z_halo[1][k].astype(jnp.float32))
            fill(k, 1, rows, low[:, None], high[:, None])
        else:
            none = jnp.zeros((ny, 1, ch), jnp.float32)
            fill(k, 1, rows, none, none)

    def plane(k, carry):
        pairs = zip((0, ny + 1), picked(y_odd, ya_ref[k, :nz], yb_ref[k, :nz]))
        if z_halo:
            corners = picked(y_odd, z_halo[2][k].astype(jnp.float32), z_halo[3][k].astype(jnp.float32))
            for (j, row), corner in zip(pairs, corners):
                fill(k, j, row[None], corner[None, 0:1], corner[None, 1:2])
        else:
            none = jnp.zeros((1, 1, ch), jnp.float32)
            for j, row in pairs:
                fill(k, j, row[None], none, none)
        return carry

    def middle(k, carry):
        fill_rows(k + 1, mid_ref[k])
        return carry

    lax.fori_loop(0, nx, middle, 0)
    low, high = picked(x_odd, xa_ref[0], xb_ref[0])
    fill_rows(0, low)
    fill_rows(nx + 1, high)
    lax.fori_loop(0, nx + 2, plane, 0)


def filter_kernel(mid_ref, xa_ref, xb_ref, ya_ref, yb_ref, in_ref, il_ref, ih_ref, total_ref, ends_ref, taps_ref):
    nx, ny, nz, ch = mid_ref.shape
    fill_taps(taps_ref, mid_ref, xa_ref, xb_ref, ya_ref, yb_ref, None)
    cells = nx * ny * nz
    flat = in_ref[...].reshape(cells, ch).T
    for a in range(3):
        views = [taps_ref[2 - a : 2 - a + nx, 2 - b : 2 - b + ny].reshape(cells, 3 * ch) for b in range(3)]
        lanes = pl.ds(a * 9 * ch, 9 * ch)
        total_ref[:, lanes] = jnp.dot(flat, jnp.concatenate(views, axis=1), preferred_element_type=jnp.float32)
    below, above = picked(is_odd("gy"), ya_ref[1 : nx + 1, nz:], yb_ref[1 : nx + 1, nz:])
    below, above = below.astype(jnp.float32), above.astype(jnp.float32)
    for side, own_ref in enumerate((il_ref, ih_ref)):
        own = own_ref[...].astype(jnp.float32)
        face = jnp.concatenate([below[:, side : side + 1], own, above[:, side : side + 1]], axis=1)
        for b in range(3):
            ends_ref[side, b] = face[:, b : b + ny].reshape(nx * ny, ch).T.astype(jnp.bfloat16)


def finish_kernel(total_ref, ends_ref, za_ref, zb_ref, keep_ref, send_ref):
    ch = total_ref.shape[0]
    nx, ny = za_ref.shape[0] - 2, za_ref.shape[1]
    core = lax.axis_index("gx") % CORES
    crossing = []
    for halo in picked(is_odd("gz"), za_ref[...], zb_ref[...]):
        crossing.append(
            jnp.concatenate([halo[2 - a : 2 - a + nx].reshape(nx * ny, ch) for a in range(3)], axis=1)
        )
    for b in range(3):
        below = jnp.dot(ends_ref[0, b], crossing[0], preferred_element_type=jnp.float32)
        above = jnp.dot(ends_ref[1, b], crossing[1], preferred_element_type=jnp.float32)
        for a in range(3):
            for c in range(3):
                lanes = pl.ds(((a * 3 + b) * 3 + c) * ch, ch)
                res = total_ref[:, lanes]
                if c == 0:
                    res = res + above[:, a * ch : (a + 1) * ch]
                if c == 2:
                    res = res + below[:, a * ch : (a + 1) * ch]
                for g in range(ch // 32):
                    first = res[g * 32 : g * 32 + 16]
                    second = res[g * 32 + 16 : g * 32 + 32]
                    keep_ref[g * 16 : g * 16 + 16, lanes] = jnp.where(core == 0, first, second)
                    other = jnp.where(core == 0, second, first)
                    send_ref[g * 16 : g * 16 + 16, lanes] = other.astype(jnp.bfloat16)


def pair_kernel(keep_ref, other_ref, out_ref):
    rows = out_ref.shape[1]
    for g in range(keep_ref.shape[0] // 16):
        total = keep_ref[g * 16 : g * 16 + 16] + other_ref[g * 16 : g * 16 + 16].astype(jnp.float32)
        for r in range(16 // rows):
            out_ref[g * (16 // rows) + r] = total[r * rows : (r + 1) * rows].astype(jnp.bfloat16)


def peers_kernel(parts_ref, out_ref):
    total = jnp.sum(parts_ref[...].astype(jnp.float32), axis=0).astype(jnp.bfloat16)
    for k in range(out_ref.shape[0]):
        out_ref[k] = total


def block_kernel(parts_ref, std_ref, grad_ref, sums_ref):
    ch = sums_ref.shape[2] // 3
    total = jnp.sum(parts_ref[...].astype(jnp.float32), axis=0)
    grad_ref[...] = total
    three = jnp.concatenate([fold(total, ch), fold(total * std_ref[...], ch), fold(total * total, ch)], axis=1)
    for k in range(sums_ref.shape[0]):
        sums_ref[k] = three


def input_kernel(mid_ref, xa_ref, xb_ref, ya_ref, yb_ref, za_ref, zb_ref, ca_ref, cb_ref, std_ref, out_ref, taps_ref):
    nx, ny, nz, ch = out_ref.shape
    fill_taps(taps_ref, mid_ref, xa_ref, xb_ref, ya_ref, yb_ref, (za_ref, zb_ref, ca_ref, cb_ref))
    planes = 2
    std = std_ref[...]
    for x in range(0, nx, planes):
        rows = jnp.concatenate(
            [
                taps_ref[x + 2 - a : x + 2 - a + planes, 2 - b : 2 - b + ny].reshape(planes * ny * nz, 3 * ch)
                for a in range(3)
                for b in range(3)
            ],
            axis=1,
        )
        res = lax.dot_general(rows, std, (((1,), (1,)), ((), ())), preferred_element_type=jnp.float32)
        out_ref[x : x + planes] = res.astype(jnp.bfloat16).reshape(planes, ny, nz, ch)


def std_kernel(x_count, near_ref, far_ref, std_ref, mean_ref, inv_ref, block_ref):
    slots, rows, held = near_ref.shape
    ch = inv_ref.shape[1]
    width = held - ch
    taps = width // ch
    gx, y, x = lax.axis_index("gx"), lax.axis_index("gy"), lax.axis_index("gz") % x_count
    zl, core = gx // CORES, gx % CORES
    blocks = [(b // 8, (b // 4) % 2, b % 4) for b in range(2 * slots)]
    count = float(2 * slots * rows * taps)

    def parts(zl_b, core_b, y_b):
        y_off, z_off = y_b ^ y, zl_b ^ zl
        slot = (y_off >> 1) + 2 * (y_off & 1) + 4 * (z_off >> 1) + 8 * (z_off & 1)
        data = jnp.where(core_b == core, near_ref[slot], far_ref[slot]).astype(jnp.float32)
        return data[:, :width], data[0:1, width:] + data[1:2, width:]

    total = jnp.zeros((1, ch), jnp.float32)
    for b in blocks:
        values, base = parts(*b)
        total = total + (fold(values, ch) + float(rows * taps) * base)
    mean = total / count
    square = jnp.zeros((1, ch), jnp.float32)
    for b in blocks:
        values, base = parts(*b)
        first = values + wide(base - mean)
        square = square + fold(first * first, ch)
    inv = lax.rsqrt(square / count + var_eps)
    mean_ref[...] = mean
    inv_ref[...] = inv
    inv_wide = wide(inv)
    for n, b in enumerate(blocks):
        values, base = parts(*b)
        std_ref[n * rows : (n + 1) * rows, :] = ((values + wide(base - mean)) * inv_wide).astype(jnp.bfloat16)
    values, base = parts(x, core, y)
    block_ref[...] = (values + wide(base - mean)) * inv_wide


def last_kernel(fan_count, x_count, own_ref, *refs):
    *got_refs, raw_ref, mean_ref, inv_ref, sums_ref, out_ref = refs
    taps, _, ch = raw_ref.shape
    steps = (lax.axis_index("gz") - lax.axis_index("gx") // CORES) % x_count
    grad = own_ref[...]
    for k, got_ref in enumerate(got_refs, 1):
        grad = jnp.where(steps == k, got_ref[...], grad)
    sums = jnp.sum(sums_ref[...], axis=0)
    sum_grad, sum_cross, sum_square = sums[:, :ch], sums[:, ch : 2 * ch], sums[:, 2 * ch :]
    mean, inv = mean_ref[...], inv_ref[...]
    mean_grad = sum_grad / fan_count
    mean_cross = sum_cross / fan_count
    shrink = 1.0 - var_eps * inv * inv
    per_output = sum_square - 2.0 * mean_grad * sum_grad - 2.0 * mean_cross * sum_cross
    per_output = per_output + fan_count * mean_grad * mean_grad + fan_count * mean_cross * mean_cross * shrink
    square_sum = jnp.sum(inv * inv * per_output, axis=1, keepdims=True)
    scale = jnp.minimum(1.0, clip_norm * lax.rsqrt(square_sum + norm_eps))
    factor = inv * scale
    for t in range(taps):
        std = (raw_ref[t] - mean) * inv
        out_ref[t] = factor * (grad[:, t * ch : (t + 1) * ch] - mean_grad - std * mean_cross)


def on_device(where, raw_weight, inputs, cotangent):
    nx, ny, nz, ch = inputs.shape
    rows, taps = raw_weight.shape[:2]
    width = taps * ch
    bf16, f32 = jnp.bfloat16, jnp.float32
    raw = jnp.transpose(raw_weight, (1, 0, 2))

    def joined(held):
        return jnp.concatenate(held, 0)

    def both(shape):
        return (of(shape, bf16), of(shape, bf16))

    faces = call(faces_kernel, both((1, ny, nz, ch)), (cotangent,))
    x_halo = swapped(*faces, "gx")
    block, *ends = call(
        base_kernel,
        (of((1, rows, width + ch), bf16), *both((nx, ny, ch)), *both((nx, ny, ch))),
        (raw, cotangent, inputs),
    )
    held = [block, where.send(block, lambda s: dict(y=s["y"] ^ 2))]
    faces = call(height_kernel, both((nx + 2, nz + 2, ch)), (cotangent, *x_halo, *ends[2:]))
    y_halo = swapped(*faces, "gy")
    faces = call(width_kernel, both((nx + 2, ny, ch)), (*ends[:2], *x_halo))
    z_halo = swapped(*faces, "gz")
    held.append(where.send(joined(held), lambda s: dict(y=s["y"] ^ 1)))
    held.append(where.send(joined(held), lambda s: dict(zl=s["zl"] ^ 2)))
    held.append(where.send(joined(held), lambda s: dict(zl=s["zl"] ^ 1)))

    flops = 2 * nx * ny * nz * ch * width
    scratch = [pltpu.VMEM((nx + 2, ny + 2, nz, 3 * ch), bf16)]
    total, end_rows = call(
        filter_kernel,
        (of((ch, width), f32), of((2, 3, ch, nx * ny), bf16)),
        (cotangent, *x_halo, *y_halo, inputs, *ends[2:]),
        vmem=16,
        flops=2 * flops,
        scratch=scratch,
    )
    keep, send = call(
        finish_kernel, (of((ch // 2, width), f32), of((ch // 2, width), bf16)), (total, end_rows, *z_halo)
    )
    other = where.send(send, lambda s: dict(core=1 - s["core"]))
    held = call(join_kernel, of((16, rows, width + ch), bf16), held)
    peers = where.x * where.gy
    half = call(pair_kernel, of((peers, rows, width), bf16), (keep, other))
    parts = where.exchange(half, ("core", "zl", "zh"), lambda s: (s["x"], s["y"]))
    far = where.send(held, lambda s: dict(core=1 - s["core"]))
    corners = swapped(*call(corner_kernel, both((nx + 2, 2, ch)), z_halo), "gy")
    std_half, mean_out, inv_std, block_std = call(
        functools.partial(std_kernel, where.x),
        (of((ch, width), bf16), of((1, ch), f32), of((1, ch), f32), of((rows, width), f32)),
        (held, far),
        flops=3_000_000_000,
    )
    copies = call(peers_kernel, of((where.zl * where.zh, rows, width), bf16), (parts,))
    parts = where.exchange(copies, ("core", "x", "y"), lambda s: (s["zh"], s["zl"]))
    input_grad = call(
        input_kernel,
        of(inputs.shape, bf16),
        (cotangent, *x_halo, *y_halo, *z_halo, *corners, std_half),
        vmem=16,
        flops=2 * flops,
        scratch=scratch,
    )
    parts, input_grad = lax.optimization_barrier((parts, input_grad))
    everyone = CORES * where.x * where.gy
    block_grad, local = call(block_kernel, (of((rows, width), f32), of((everyone, 1, 3 * ch), f32)), (parts, block_std))
    passed = [where.send(block_grad, lambda s, k=k: dict(x=(s["x"] + k) % where.x)) for k in range(1, where.x)]
    sums = where.exchange(local, ("zl", "zh"), lambda s: (s["core"], s["x"], s["y"]))

    grad = call(functools.partial(last_kernel, float(ch * taps), where.x), of((taps, rows, ch), f32), (block_grad, *passed, raw, mean_out, inv_std, sums))
    return (input_grad, jnp.transpose(grad, (1, 0, 2)))


def solution(mesh):
    where = Layout(mesh)
    in_specs = (P(("gx", "gy"), None, None), P("gx", "gy", "gz", None), P("gx", "gy", "gz", None))
    out_specs = (P("gx", "gy", "gz", None), P(("gx", "gy"), None, None))

    def body(raw_weight, inputs, cotangent):
        return on_device(where, raw_weight, inputs, cotangent)

    return jax.shard_map(body, mesh=mesh, in_specs=in_specs, out_specs=out_specs, check_vma=False)
```
